32 devices in a mesh: dp: 4 (over x, core), fsdp: 8 (over z, y).
Axes of the slice: x: 2, y: 2, z: 4, core: 2. Of those that a mesh axis runs over, the one named last changes fastest.
Arguments:
- tokens: bfloat16 [16384, 768], P(('dp', 'fsdp')), may hold values from -6 to 6
- lengths: int32 [32, 6], P(('dp', 'fsdp')), may hold values from 1 to 128, 256 in all within a row
- norm1_gain: bfloat16 [768], P('fsdp'), may hold values from 0.25 to 1.75
- norm1_bias: bfloat16 [768], P('fsdp'), may hold values from -1.75 to 1.75
- query_weight: bfloat16 [768, 768], P('fsdp'), may hold values from -0.21875 to 0.21875
- key_weight: bfloat16 [768, 768], P('fsdp'), may hold values from -0.21875 to 0.21875
- value_weight: bfloat16 [768, 768], P('fsdp'), may hold values from -0.21875 to 0.21875
- output_weight: bfloat16 [768, 768], P('fsdp'), may hold values from -0.625 to 0.625
- norm2_gain: bfloat16 [768], P('fsdp'), may hold values from 0.25 to 1.75
- norm2_bias: bfloat16 [768], P('fsdp'), may hold values from -1.75 to 1.75
- up_weight: bfloat16 [768, 3072], P('fsdp'), may hold values from -0.21875 to 0.21875
- up_bias: bfloat16 [3072], P('fsdp'), may hold values from -3 to 3
- down_weight: bfloat16 [3072, 768], P('fsdp'), may hold values from -0.109375 to 0.109375
- down_bias: bfloat16 [768], P('fsdp'), may hold values from -1.75 to 1.75
- cotangent: bfloat16 [16384, 768], P(('dp', 'fsdp')), may hold values from -6 to 6
Outputs:
- output: bfloat16 [16384, 768], P(('dp', 'fsdp'))
- input_grad: float32 [16384, 768], P(('dp', 'fsdp'))
- norm1_gain_grad: float32 [768], P('fsdp')
- norm1_bias_grad: float32 [768], P('fsdp')
- query_weight_grad: float32 [768, 768], P('fsdp')
- key_weight_grad: float32 [768, 768], P('fsdp')
- value_weight_grad: float32 [768, 768], P('fsdp')
- output_weight_grad: float32 [768, 768], P('fsdp')
- norm2_gain_grad: float32 [768], P('fsdp')
- norm2_bias_grad: float32 [768], P('fsdp')
- up_weight_grad: float32 [768, 3072], P('fsdp')
- up_bias_grad: float32 [3072], P('fsdp')
- down_weight_grad: float32 [3072, 768], P('fsdp')
- down_bias_grad: float32 [768], P('fsdp')
The draws below stay inside these ranges and needn't reach their ends.
Inputs may be any that keep to these rules, and one draw needn't show every extreme that they name: Each row of lengths sums to 256, and its largest entry equals 128.
All inputs are finite; a program needn't handle non-finite values.
Results may differ from the reference program's by a relative error of at most 0.012.
Values may be sent and summed in bfloat16 or wider, within the bound.
No kernel may reach another device: no remote copies, remote signals or barrier semaphores. Data moves between devices by JAX's collectives and lax.ppermute only.
A program may use at most 192 MiB of HBM per device.

```python
import math
import jax
import jax.numpy as jnp
import numpy as np
from jax import lax

D = 768
H = 12
HD = 64
FF = 3072
BLOCK = 16
SLOTS = 6
TOK_DEV = 256
MOST = 128
ROWS_DEV = 512
ROWS = 16384
N_DP = 4
N_FSDP = 8


def spiked(values, stream_key, source, target, parts, factor):
    owner, partner = [(jnp.arange(values.shape[dim]) // (values.shape[dim] // parts)).reshape([-1 if axis == dim else 1 for axis in range(values.ndim)]) for dim in (source, target)]
    chosen = jax.random.permutation(stream_key, parts)[partner]
    strong = (owner == chosen) | (owner == (partner + parts // 2) % parts)
    return jnp.where(strong, factor * values, values)


def shard_levels(rng, dims, pieces, low, high):
    def one(dim, blocks):
        steps = jax.random.uniform(jax.random.fold_in(jax.random.fold_in(rng, 6), dim), (blocks,), jnp.float32, low / len(pieces), high / len(pieces))
        return jnp.repeat(jnp.exp(steps), dims[dim] // blocks).reshape((-1,) + (1,) * (len(dims) - dim - 1))

    level = one(*pieces[0])
    for cut in pieces[1:]:
        level = level * one(*cut)
    return level


def length_profile(count, total, reach, lean):
    portions = [(1 << 20) // math.isqrt(grade ** lean) + 1 for grade in range(2, count + 1)]
    surplus, given = total - reach - (count - 1), [1] * (count - 1)
    while surplus > 0:
        candidates = [i for i in range(count - 1) if given[i] < reach]
        whole, remaining = sum([portions[i] for i in candidates]), surplus
        for i in candidates:
            more = min(reach - given[i], max(1, remaining * portions[i] // whole), surplus)
            given[i] = given[i] + more
            surplus = surplus - more
    return np.array([reach] + given)


def ragged_sizes(stream_key, amount, total, reach, lean):
    if amount == 2:
        one = jax.random.randint(stream_key, (), max(1, total - reach), min(reach, total - 1) + 1)
        return jnp.stack([one, total - one])
    sizes = jnp.asarray(length_profile(amount, total, reach, lean), jnp.int32)
    couples = (amount - 1) // 2
    giver, receiver = sizes[1:1 + 2 * couples:2], sizes[2:2 + 2 * couples:2]
    slack = jnp.minimum(giver - 1, reach - receiver)
    shifted = jax.random.randint(jax.random.fold_in(stream_key, 1), (couples,), 0, 1 << 20) % (slack + 1)
    sizes = sizes.at[1:1 + 2 * couples:2].set(giver - shifted).at[2:2 + 2 * couples:2].set(receiver + shifted)
    return sizes[jax.random.permutation(jax.random.fold_in(stream_key, 2), amount)]


def gaussian(own_key, shape, width, most, shards=(), kind=jnp.bfloat16):
    values = width * jax.random.normal(own_key, shape, jnp.float32)
    if shards:
        values = values * shard_levels(own_key, shape, shards, -0.22, 0.18)
    return jnp.clip(values, -most, most).astype(kind)


def heavy_noise(key, dims, scale, limit, cuts, heavy, kind=jnp.bfloat16):
    drawn = scale * jax.random.normal(key, dims, jnp.float32)
    if cuts:
        drawn = drawn * shard_levels(key, dims, cuts, -0.22, 0.18)
    return jnp.clip(spiked(drawn, jax.random.fold_in(key, 3), *heavy), -limit, limit).astype(kind)


def setup_inputs(seed: int = 0) -> dict:
    key_of = jax.random.split(jax.random.key(seed), 16)
    tokens = gaussian(key_of[0], (ROWS, D), 1.0, 6.0, ((0, 32),))
    lengths = jax.vmap(lambda own: ragged_sizes(own, SLOTS, TOK_DEV, MOST, 2))(jax.random.split(key_of[1], (N_DP * N_FSDP))).reshape((N_DP * N_FSDP, SLOTS)).astype(jnp.int32)
    norm1_gain = jnp.clip(1.0 + 0.15 * jax.random.normal(key_of[2], (D,), jnp.float32), 0.25, 1.75).astype(jnp.bfloat16)
    norm1_bias = gaussian(key_of[3], (D,), 0.3, 1.75, ((0, 8),))
    query_weight = gaussian(key_of[4], (D, D), D ** -0.5, 0.21875, ((0, 8),))
    key_weight = gaussian(key_of[5], (D, D), D ** -0.5, 0.21875, ((0, 8),))
    value_weight = gaussian(key_of[6], (D, D), D ** -0.5, 0.21875, ((0, 8),))
    output_weight = gaussian(key_of[7], (D, D), (D // 8) ** -0.5, 0.625, ((0, 8),))
    norm2_gain = jnp.clip(1.0 + 0.15 * jax.random.normal(key_of[8], (D,), jnp.float32), 0.25, 1.75).astype(jnp.bfloat16)
    norm2_bias = gaussian(key_of[9], (D,), 0.3, 1.75, ((0, 8),))
    up_weight = gaussian(key_of[10], (D, FF), D ** -0.5, 0.21875, ((0, 8),))
    up_bias = gaussian(key_of[11], (FF,), 0.5, 3.0, ((0, 8),))
    down_weight = gaussian(key_of[12], (FF, D), FF ** -0.5, 0.109375, ((0, 8),))
    down_bias = gaussian(key_of[13], (D,), 0.3, 1.75, ((0, 8),))
    cotangent = heavy_noise(key_of[14], (ROWS, D), 1.0, 6.0, ((0, 32),), (0, 1, 32, 2.75))
    return dict(tokens=tokens, lengths=lengths, norm1_gain=norm1_gain, norm1_bias=norm1_bias, query_weight=query_weight, key_weight=key_weight, value_weight=value_weight, output_weight=output_weight, norm2_gain=norm2_gain, norm2_bias=norm2_bias, up_weight=up_weight, up_bias=up_bias, down_weight=down_weight, down_bias=down_bias, cotangent=cotangent)


EPSILON = 1e-05
BASE = 10000.0
NEGATIVE = -1e+30

@jax.custom_vjp
def low(v):
    return lax.optimization_barrier(v.astype(jnp.bfloat16)).astype(jnp.float32)

@jax.custom_vjp
def low_back(v):
    return v

def low_keep(v):
    return (low(v), None)

def low_pass(kept, grad):
    return (grad,)

def back_keep(v):
    return (v, None)

def back_low(kept, grad):
    return (low(grad),)
low.defvjp(low_keep, low_pass)
low_back.defvjp(back_keep, back_low)

def matmul(left, right):
    return jnp.dot(left, right, precision=lax.Precision.HIGHEST, preferred_element_type=jnp.float32)

def layer_norm(values, gain, shift):
    center = values - lax.optimization_barrier(jnp.mean(values, axis=-1, keepdims=True))
    spread = lax.optimization_barrier(jnp.mean(center * center, axis=-1, keepdims=True))
    return center * lax.rsqrt(spread + EPSILON) * gain + shift

def row_layout(length_row, row_count, slot_count):
    doubled = 2 * length_row
    ends_at = jnp.cumsum(doubled, dtype=jnp.int32)
    starts_at = ends_at - doubled
    row_index = jnp.arange(row_count, dtype=jnp.int32)
    member = (row_index[:, None] >= starts_at[None, :]) & (row_index[:, None] < ends_at[None, :])
    slot_ids = jnp.arange(slot_count, dtype=jnp.int32)
    slot_index = lax.optimization_barrier(jnp.sum(jnp.where(member, slot_ids[None, :], 0), axis=1, dtype=jnp.int32))
    start_row = lax.optimization_barrier(jnp.sum(jnp.where(member, starts_at[None, :], 0), axis=1, dtype=jnp.int32))
    seq_length = lax.optimization_barrier(jnp.sum(jnp.where(member, length_row[None, :], 0), axis=1, dtype=jnp.int32))
    local_row = row_index - start_row
    clean_flag = (local_row >= seq_length).astype(jnp.int32)
    position = local_row - clean_flag * seq_length
    return (row_index, slot_index, clean_flag, position)

def allowed_pairs(query_side, key_side, block_size, slot_count):
    query_row, query_slot, query_clean, query_pos = query_side
    key_row, key_slot, key_clean, key_pos = key_side
    query_block = query_pos // block_size
    key_block = key_pos // block_size
    same_seq = query_slot[:, None] == key_slot[None, :]
    key_noisy = key_clean[None, :] == 0
    key_plain = key_clean[None, :] == 1
    noisy_rule = key_noisy & (key_block[None, :] == query_block[:, None]) | key_plain & (key_block[None, :] < query_block[:, None])
    clean_rule = key_plain & (key_block[None, :] <= query_block[:, None])
    rule_held = jnp.where(query_clean[:, None] == 1, clean_rule, noisy_rule)
    padded = query_slot == slot_count - 1
    real_pairs = same_seq & rule_held & jnp.logical_not(padded)[:, None]
    self_pairs = padded[:, None] & (query_row[:, None] == key_row[None, :])
    return real_pairs | self_pairs

def rotary_tables(position, head_dim):
    half_dim = head_dim // 2
    freqs = jnp.exp(jnp.arange(half_dim, dtype=jnp.float32) * (-2.0 * math.log(BASE) / head_dim))
    angles = position.astype(jnp.float32)[:, None] * freqs[None, :]
    return (jnp.cos(angles)[:, None, :], jnp.sin(angles)[:, None, :])

def rotate(values, cosine, sine):
    half_dim = values.shape[-1] // 2
    first = values[..., :half_dim]
    second = values[..., half_dim:]
    return jnp.concatenate([first * cosine - second * sine, second * cosine + first * sine], axis=-1)

def forward(inputs, cosine, sine, allowed, params):
    first_gain, first_shift, query_weight, key_weight, value_weight, output_weight, second_gain, second_shift, up_weight, up_bias, down_weight, down_bias = params
    row_count = inputs.shape[0]
    heads_split = (row_count, H, HD)
    normed = low(layer_norm(inputs, first_gain, first_shift))
    queries = low(rotate(low_back(matmul(normed, query_weight)).reshape(heads_split), cosine, sine))
    key_rows = low(rotate(low_back(matmul(normed, key_weight)).reshape(heads_split), cosine, sine))
    value_rows = low(low_back(matmul(normed, value_weight))).reshape(heads_split)
    raw_scores = low_back(jnp.einsum('qhd,khd->hqk', queries, key_rows, precision=lax.Precision.HIGHEST))
    scores = jnp.where(allowed[None], raw_scores * HD ** (-0.5), NEGATIVE)
    row_max = lax.optimization_barrier(jnp.max(scores, axis=2, keepdims=True))
    exponent = jnp.exp(scores - row_max)
    probs = low(exponent / lax.optimization_barrier(jnp.sum(exponent, axis=2, keepdims=True)))
    mixed = low(low_back(jnp.einsum('hqk,khd->qhd', probs, value_rows, precision=lax.Precision.HIGHEST)))
    mixed = mixed.reshape(row_count, H * HD)
    residual = inputs + low_back(matmul(mixed, output_weight))
    hidden_in = low(layer_norm(residual, second_gain, second_shift))
    pre_act = low_back(matmul(hidden_in, up_weight) + up_bias)
    activated = low(jax.nn.gelu(pre_act, approximate=True))
    return residual + matmul(activated, down_weight) + down_bias

def reference(tokens, lengths, norm1_gain, norm1_bias, query_weight, key_weight, value_weight, output_weight, norm2_gain, norm2_bias, up_weight, up_bias, down_weight, down_bias, cotangent):
    params = (norm1_gain, norm1_bias, query_weight, key_weight, value_weight, output_weight, norm2_gain, norm2_bias, up_weight, up_bias, down_weight, down_bias)
    params = tuple((item.astype(jnp.float32) for item in params))
    groups = N_DP * N_FSDP
    token_groups = tokens.reshape(groups, ROWS_DEV, D)
    grad_groups = cotangent.reshape(groups, ROWS_DEV, D)
    slot_count = lengths.shape[1]

    def one_group(running, group_item):
        group_tokens, group_grad, group_lengths = group_item
        layout = row_layout(group_lengths, ROWS_DEV, slot_count)
        allowed = allowed_pairs(layout, layout, BLOCK, slot_count)
        cosine, sine = rotary_tables(layout[3], HD)

        def run_layer(inputs, weights_in):
            return forward(inputs, cosine, sine, allowed, weights_in)
        result, pull_back = jax.vjp(run_layer, group_tokens.astype(jnp.float32), params)
        input_grad, weight_grads = pull_back(group_grad.astype(jnp.float32))
        running = tuple((total_item + grad_item for total_item, grad_item in zip(running, weight_grads)))
        return (running, (result.astype(jnp.bfloat16), input_grad))
    start_sums = tuple((jnp.zeros(item.shape, jnp.float32) for item in params))
    totals, (outputs, input_grads) = lax.scan(one_group, start_sums, (token_groups, grad_groups, lengths))
    output = outputs.reshape(ROWS, D)
    input_grad = input_grads.reshape(ROWS, D)
    return (output, input_grad, totals[0], totals[1], totals[2], totals[3], totals[4], totals[5], totals[6], totals[7], totals[8], totals[9], totals[10], totals[11])
```

```python
from functools import partial
import math

import jax
import jax.numpy as jnp
from jax import lax
from jax.experimental import pallas as pl
from jax.experimental.pallas import tpu as pltpu
from jax.sharding import PartitionSpec as P

H = 12
HD = 64
BLOCK = 16
EPSILON = 1e-05
BASE = 10000.0
NEGATIVE = -1e30
BF = jnp.bfloat16
F32 = jnp.float32
SMALL = 16
VMEM_LIMIT = 56 * 1024 * 1024


def row_layout(length_row, row_count, slot_count):
    doubled = 2 * length_row
    ends_at = jnp.cumsum(doubled, dtype=jnp.int32)
    starts_at = ends_at - doubled
    row_index = jnp.arange(row_count, dtype=jnp.int32)
    member = (row_index[:, None] >= starts_at[None, :]) & (row_index[:, None] < ends_at[None, :])
    slot_ids = jnp.arange(slot_count, dtype=jnp.int32)
    slot_index = jnp.sum(jnp.where(member, slot_ids[None, :], 0), axis=1, dtype=jnp.int32)
    start_row = jnp.sum(jnp.where(member, starts_at[None, :], 0), axis=1, dtype=jnp.int32)
    seq_length = jnp.sum(jnp.where(member, length_row[None, :], 0), axis=1, dtype=jnp.int32)
    local_row = row_index - start_row
    clean_flag = (local_row >= seq_length).astype(jnp.int32)
    position = local_row - clean_flag * seq_length
    return (row_index, slot_index, clean_flag, position)


def allowed_pairs(query_side, key_side, block_size, slot_count):
    query_row, query_slot, query_clean, query_pos = query_side
    key_row, key_slot, key_clean, key_pos = key_side
    query_block = query_pos // block_size
    key_block = key_pos // block_size
    same_seq = query_slot[:, None] == key_slot[None, :]
    key_noisy = key_clean[None, :] == 0
    key_plain = key_clean[None, :] == 1
    noisy_rule = key_noisy & (key_block[None, :] == query_block[:, None]) | key_plain & (
        key_block[None, :] < query_block[:, None]
    )
    clean_rule = key_plain & (key_block[None, :] <= query_block[:, None])
    rule_held = jnp.where(query_clean[:, None] == 1, clean_rule, noisy_rule)
    padded = query_slot == slot_count - 1
    real_pairs = same_seq & rule_held & jnp.logical_not(padded)[:, None]
    self_pairs = padded[:, None] & (query_row[:, None] == key_row[None, :])
    return real_pairs | self_pairs


def rotary_tables(position):
    half = HD // 2
    lane = jnp.arange(2 * HD, dtype=jnp.int32)
    freqs = jnp.exp((lane % half).astype(F32) * (-2.0 * math.log(BASE) / HD))
    angles = position.astype(F32)[:, None] * freqs[None, :]
    sign = jnp.where(lane % HD < half, -1.0, 1.0)
    return jnp.cos(angles), jnp.sin(angles) * sign[None, :]


def swap(values, axis, mask, size):
    return lax.ppermute(values, axis, [(i, i ^ mask) for i in range(size)])


def dot(a, b):
    return jnp.dot(a, b, preferred_element_type=F32)


def dot_nt(a, b):
    return lax.dot_general(a, b, (((1,), (1,)), ((), ())), preferred_element_type=F32)


def dot_tn(a, b):
    return lax.dot_general(a, b, (((0,), (0,)), ((), ())), preferred_element_type=F32)


def params(**more):
    return pltpu.CompilerParams(vmem_limit_bytes=VMEM_LIMIT, **more)


def cost(flops, moved):
    return pl.CostEstimate(flops=int(flops), bytes_accessed=int(moved), transcendentals=0)


def norm_parts(values):
    center = values - jnp.mean(values, axis=-1, keepdims=True)
    spread = jnp.mean(center * center, axis=-1, keepdims=True)
    inv = lax.rsqrt(spread + EPSILON)
    return center * inv, inv


def norm_back(grad, unit, inv, gain):
    scaled = grad * gain
    first = jnp.mean(scaled, axis=-1, keepdims=True)
    second = jnp.mean(scaled * unit, axis=-1, keepdims=True)
    return inv * (scaled - first - unit * second)


def turn(values, cosine, sine):
    half = HD // 2
    pair = 2 * HD
    lane = lax.broadcasted_iota(jnp.int32, (1, pair), 1)
    low = (lane % HD) < half
    parts = []
    for at in range(0, values.shape[1], pair):
        part = values[:, at : at + pair]
        other = jnp.where(low, pltpu.roll(part, pair - half, 1), pltpu.roll(part, half, 1))
        parts.append(part * cosine + other * sine)
    return parts[0] if len(parts) == 1 else jnp.concatenate(parts, axis=1)


def bits_of(index, masks):
    total = 0
    for bit, mask in enumerate(masks):
        if (index >> bit) & 1:
            total |= mask
    return total


def assemble_kernel(masks, h, idx_ref, a0, a1, a2, a3, b0, b1, b2, b3, out_ref, sems):
    count = 1 << len(masks)
    half = count // 2
    me_d, me_f = idx_ref[0], idx_ref[1]
    copies = []

    def put(src, r, k, colour):
        d = me_d ^ r
        j = me_f ^ k
        copy = pltpu.make_async_copy(src, out_ref.at[d, j, colour], sems.at[len(copies)])
        copy.start()
        copies.append(copy)

    for ref, r in ((a0, 0), (a1, 2), (a2, 1), (a3, 3)):
        for i in range(count):
            put(ref.at[i], r, bits_of(i, masks), 0)
    for ref, r, y in ((b0, 0, 0), (b1, 0, 1), (b2, 1, 0), (b3, 1, 1)):
        for x in range(2):
            for i in range(half):
                put(ref.at[x * half + i], r | (2 * x), bits_of(i, masks) | y, 1)
    for copy in copies:
        copy.wait()


def assemble(idx, pieces, masks, shards, h, width):
    count = 1 << len(masks)
    out = pl.pallas_call(
        partial(assemble_kernel, masks, h),
        out_shape=jax.ShapeDtypeStruct((4, shards, 2, h, width), BF),
        in_specs=[pl.BlockSpec(memory_space=pltpu.SMEM)]
        + [pl.BlockSpec(memory_space=pl.ANY)] * 8,
        out_specs=pl.BlockSpec(memory_space=pltpu.VMEM),
        scratch_shapes=[pltpu.SemaphoreType.DMA((8 * count,))],
        compiler_params=params(),
        cost_estimate=cost(0, 4 * shards * 2 * h * width * 4),
        name="assemble",
    )(idx, *pieces)
    return out.reshape(4, shards * 2 * h, width)


def qkv_kernel(x_ref, small_ref, cos_ref, sin_ref, w_ref, normed_ref, out_ref, keep):
    g = pl.program_id(0)

    @pl.when(g == 0)
    def _():
        unit, _ = norm_parts(x_ref[...].astype(F32))
        normed = (unit * small_ref[0:1, :] + small_ref[1:2, :]).astype(BF)
        keep[...] = normed
        normed_ref[...] = normed

    product = dot(keep[...], w_ref[0])

    @pl.when(g < 2)
    def _():
        out_ref[0] = turn(product, cos_ref[...], sin_ref[...]).astype(BF)

    @pl.when(g == 2)
    def _():
        out_ref[0] = product.astype(BF)


def qkv(x, small, cosine, sine, weights):
    n, d = x.shape
    return pl.pallas_call(
        qkv_kernel,
        grid=(3,),
        out_shape=(jax.ShapeDtypeStruct((n, d), BF), jax.ShapeDtypeStruct((3, n, d), BF)),
        in_specs=[
            pl.BlockSpec((n, d), lambda g: (0, 0)),
            pl.BlockSpec(small.shape, lambda g: (0, 0)),
            pl.BlockSpec(cosine.shape, lambda g: (0, 0)),
            pl.BlockSpec(sine.shape, lambda g: (0, 0)),
            pl.BlockSpec((1, d, d), lambda g: (g, 0, 0)),
        ],
        out_specs=(
            pl.BlockSpec((n, d), lambda g: (0, 0)),
            pl.BlockSpec((1, n, d), lambda g: (g, 0, 0)),
        ),
        scratch_shapes=[pltpu.VMEM((n, d), BF)],
        compiler_params=params(),
        cost_estimate=cost(6 * n * d * d, 2 * (5 * n * d + 3 * d * d)),
        name="qkv",
    )(x, small, cosine, sine, weights)


def head_mask(which):
    lane = lax.broadcasted_iota(jnp.int32, (1, 2 * HD), 1)
    return (lane < HD) if which == 0 else (lane >= HD)


def attend_kernel(q_ref, k_ref, v_ref, bias_ref, mixed_ref, probs_ref):
    q, k, v = q_ref[0], k_ref[0], v_ref[0]
    zero = jnp.zeros((), BF)
    parts = []
    for h in range(2):
        own = jnp.where(head_mask(h), q, zero)
        scores = dot_nt(own, k) * (HD**-0.5) + bias_ref[...]
        top = jnp.max(scores, axis=1, keepdims=True)
        raised = jnp.exp(scores - top)
        total = jnp.sum(raised, axis=1, keepdims=True)
        probs = (raised * (1.0 / total)).astype(BF)
        probs_ref[h] = probs
        parts.append(dot(probs, v))
    mixed_ref[...] = jnp.where(head_mask(0), parts[0], parts[1]).astype(BF)


def attend(three, bias):
    _, n, d = three.shape
    pair = 2 * HD
    return pl.pallas_call(
        attend_kernel,
        grid=(d // pair,),
        out_shape=(
            jax.ShapeDtypeStruct((n, d), BF),
            jax.ShapeDtypeStruct((d // HD, n, n), BF),
        ),
        in_specs=[
            pl.BlockSpec((1, n, pair), lambda p: (0, 0, p)),
            pl.BlockSpec((1, n, pair), lambda p: (1, 0, p)),
            pl.BlockSpec((1, n, pair), lambda p: (2, 0, p)),
            pl.BlockSpec((n, n), lambda p: (0, 0)),
        ],
        out_specs=(
            pl.BlockSpec((n, pair), lambda p: (0, p)),
            pl.BlockSpec((2, n, n), lambda p: (p, 0, 0)),
        ),
        compiler_params=params(),
        cost_estimate=cost(8 * n * n * d, 2 * n * n * (d // HD) + 8 * n * d),
        name="attend",
    )(three, three, three, bias)


def attend_back_kernel(
    q_ref, k_ref, v_ref, probs_ref, grad_ref, mixed_ref, cos_ref, sin_ref, out_ref
):
    q, k, v, grad = q_ref[0], k_ref[0], v_ref[0], grad_ref[...]
    zero = jnp.zeros((), BF)
    product = grad.astype(F32) * mixed_ref[...].astype(F32)
    dq, dk, dv = [], [], []
    for h in range(2):
        mask = head_mask(h)
        inner = jnp.sum(jnp.where(mask, product, 0.0), axis=1, keepdims=True)
        probs = probs_ref[h]
        prob_grad = dot_nt(jnp.where(mask, grad, zero), v)
        score_grad = (probs.astype(F32) * (prob_grad - inner)).astype(BF)
        dq.append(dot(score_grad, k))
        dk.append(dot_tn(score_grad, q))
        dv.append(dot_tn(probs, grad))
    first = head_mask(0)
    scale = HD**-0.5
    cosine, sine = cos_ref[...], sin_ref[...]
    out_ref[0] = turn(jnp.where(first, dq[0], dq[1]) * scale, cosine, -sine).astype(BF)
    out_ref[1] = turn(jnp.where(first, dk[0], dk[1]) * scale, cosine, -sine).astype(BF)
    out_ref[2] = jnp.where(first, dv[0], dv[1]).astype(BF)


def attend_back(three, probs, grad, mixed, cosine, sine):
    _, n, d = three.shape
    pair = 2 * HD
    return pl.pallas_call(
        attend_back_kernel,
        grid=(d // pair,),
        out_shape=jax.ShapeDtypeStruct((3, n, d), BF),
        in_specs=[
            pl.BlockSpec((1, n, pair), lambda p: (0, 0, p)),
            pl.BlockSpec((1, n, pair), lambda p: (1, 0, p)),
            pl.BlockSpec((1, n, pair), lambda p: (2, 0, p)),
            pl.BlockSpec((2, n, n), lambda p: (p, 0, 0)),
            pl.BlockSpec((n, pair), lambda p: (0, p)),
            pl.BlockSpec((n, pair), lambda p: (0, p)),
            pl.BlockSpec(cosine.shape, lambda p: (0, 0)),
            pl.BlockSpec(sine.shape, lambda p: (0, 0)),
        ],
        out_specs=pl.BlockSpec((3, n, pair), lambda p: (0, 0, p)),
        compiler_params=params(),
        cost_estimate=cost(16 * n * n * d, 2 * n * n * (d // HD) + 16 * n * d),
        name="attend_back",
    )(three, three, three, probs, grad, mixed, cosine, sine)


def branch_kernel(x_ref, mixed_ref, w_ref, small_ref, residual_ref, hidden_ref):
    residual = x_ref[...].astype(F32) + dot(mixed_ref[...], w_ref[0])
    residual_ref[...] = residual
    unit, _ = norm_parts(residual)
    hidden_ref[...] = (unit * small_ref[2:3, :] + small_ref[3:4, :]).astype(BF)


def branch(x, mixed, weights, small):
    n, d = x.shape
    rows = n // 2
    return pl.pallas_call(
        branch_kernel,
        grid=(2,),
        out_shape=(jax.ShapeDtypeStruct((n, d), F32), jax.ShapeDtypeStruct((n, d), BF)),
        in_specs=[
            pl.BlockSpec((rows, d), lambda g: (g, 0)),
            pl.BlockSpec((rows, d), lambda g: (g, 0)),
            pl.BlockSpec((1, d, d), lambda g: (3, 0, 0)),
            pl.BlockSpec(small.shape, lambda g: (0, 0)),
        ],
        out_specs=(
            pl.BlockSpec((rows, d), lambda g: (g, 0)),
            pl.BlockSpec((rows, d), lambda g: (g, 0)),
        ),
        compiler_params=params(),
        cost_estimate=cost(2 * n * d * d, 10 * n * d + 2 * d * d),
        name="branch",
    )(x, mixed, weights, small)


def up_kernel(hidden_ref, w_ref, small_ref, act_ref, slope_ref):
    g = pl.program_id(0)
    bias = small_ref[5:6, :]
    for other in range(1, 4):
        bias = jnp.where(g == other, small_ref[5 + other : 6 + other, :], bias)
    v = dot(hidden_ref[...], w_ref[0]) + bias
    c = math.sqrt(2.0 / math.pi)
    square = v * v
    t = jnp.tanh(v * (c + (c * 0.044715) * square))
    half = 0.5 * (1.0 + t)
    act_ref[0] = (v * half).astype(BF)
    slope = half + (0.5 * v) * (1.0 - t * t) * (c + (3.0 * c * 0.044715) * square)
    slope_ref[0] = slope.astype(BF)


def up(hidden, weights, small):
    n, d = hidden.shape
    return pl.pallas_call(
        up_kernel,
        grid=(4,),
        out_shape=(
            jax.ShapeDtypeStruct((4, n, d), BF),
            jax.ShapeDtypeStruct((4, n, d), BF),
        ),
        in_specs=[
            pl.BlockSpec((n, d), lambda g: (0, 0)),
            pl.BlockSpec((1, d, d), lambda g: (g, 0, 0)),
            pl.BlockSpec(small.shape, lambda g: (0, 0)),
        ],
        out_specs=(
            pl.BlockSpec((1, n, d), lambda g: (g, 0, 0)),
            pl.BlockSpec((1, n, d), lambda g: (g, 0, 0)),
        ),
        compiler_params=params(),
        cost_estimate=cost(8 * n * d * d, 18 * n * d + 8 * d * d),
        name="up",
    )(hidden, weights, small)


def weight_grad_kernel(masks, h, shards, idx_ref, x_ref, y_ref, out_ref, keep):
    keep[...] = dot_tn(x_ref[0], y_ref[0]).astype(BF)
    me_f = idx_ref[1]
    for i in range(shards):
        j = me_f ^ bits_of(i, masks)
        for colour in range(2):
            start = pl.multiple_of(j * (2 * h) + colour * h, h & -h)
            out_ref[0, colour, i] = keep[pl.ds(start, h), :]


def weight_grad(idx, xs, ys, x_of, y_of, distances, masks, shards, h):
    _, n, d = xs.shape
    first, step = distances[0], distances[1] - distances[0]

    def chunk(g, idx_ref):
        return idx_ref[0] ^ (first + step * g)

    return pl.pallas_call(
        partial(weight_grad_kernel, masks, h, shards),
        grid_spec=pltpu.PrefetchScalarGridSpec(
            num_scalar_prefetch=1,
            grid=(len(distances),),
            in_specs=[
                pl.BlockSpec((1, n, d), lambda g, i: (x_of(chunk(g, i)), 0, 0)),
                pl.BlockSpec((1, n, d), lambda g, i: (y_of(chunk(g, i)), 0, 0)),
            ],
            out_specs=pl.BlockSpec(
                (1, 2, shards, h, d), lambda g, i: (g, 0, 0, 0, 0)
            ),
            scratch_shapes=[pltpu.VMEM((d, d), BF)],
        ),
        out_shape=jax.ShapeDtypeStruct((len(distances), 2, shards, h, d), BF),
        compiler_params=params(),
        cost_estimate=cost(
            2 * len(distances) * n * d * d, 2 * len(distances) * (2 * n * d + d * d)
        ),
        name="weight_grad",
    )(idx, xs, ys)


def act_grad_kernel(c_ref, down_ref, up_ref, slope_ref, pre_ref, sums_ref, hidden_ref):
    g = pl.program_id(0)
    c = c_ref[...]

    @pl.when(g == 0)
    def _():
        hidden_ref[...] = jnp.zeros_like(hidden_ref)
        sums_ref[...] = jnp.zeros_like(sums_ref)
        sums_ref[4:5, :] = jnp.sum(c.astype(F32), axis=0, keepdims=True)

    pre = (dot_nt(c, down_ref[0]) * slope_ref[0].astype(F32)).astype(BF)
    pre_ref[0] = pre
    sums = jnp.sum(pre.astype(F32), axis=0, keepdims=True)
    row = lax.broadcasted_iota(jnp.int32, (sums_ref.shape[0], 1), 0)
    sums_ref[...] += jnp.where(row == 5 + g, sums, 0.0)
    hidden_ref[...] += dot_nt(pre, up_ref[0])


def act_grad(c, down, up_weights, slope):
    n, d = c.shape
    return pl.pallas_call(
        act_grad_kernel,
        grid=(4,),
        out_shape=(
            jax.ShapeDtypeStruct((4, n, d), BF),
            jax.ShapeDtypeStruct((SMALL, d), F32),
            jax.ShapeDtypeStruct((n, d), F32),
        ),
        in_specs=[
            pl.BlockSpec((n, d), lambda g: (0, 0)),
            pl.BlockSpec((1, d, d), lambda g: (g, 0, 0)),
            pl.BlockSpec((1, d, d), lambda g: (g, 0, 0)),
            pl.BlockSpec((1, n, d), lambda g: (g, 0, 0)),
        ],
        out_specs=(
            pl.BlockSpec((1, n, d), lambda g: (g, 0, 0)),
            pl.BlockSpec((SMALL, d), lambda g: (0, 0)),
            pl.BlockSpec((n, d), lambda g: (0, 0)),
        ),
        compiler_params=params(),
        cost_estimate=cost(16 * n * d * d, 22 * n * d + 16 * d * d),
        name="act_grad",
    )(c, down, up_weights, slope)


def middle_kernel(
    c_ref, hidden_ref, residual_ref, small_ref, w_ref, grad_ref, low_ref, mixed_ref, sums_ref
):
    @pl.when(pl.program_id(0) == 0)
    def _():
        sums_ref[...] = jnp.zeros_like(sums_ref)

    grad = hidden_ref[...]
    unit, inv = norm_parts(residual_ref[...])
    sums_ref[2:3, :] += jnp.sum(grad * unit, axis=0, keepdims=True)
    sums_ref[3:4, :] += jnp.sum(grad, axis=0, keepdims=True)
    full = c_ref[...].astype(F32) + norm_back(grad, unit, inv, small_ref[2:3, :])
    grad_ref[...] = full
    low = full.astype(BF)
    low_ref[...] = low
    mixed_ref[...] = dot_nt(low, w_ref[0]).astype(BF)


def middle(c, hidden_grad, residual, small, weights):
    n, d = c.shape
    rows = n // 2
    return pl.pallas_call(
        middle_kernel,
        grid=(2,),
        out_shape=(
            jax.ShapeDtypeStruct((n, d), F32),
            jax.ShapeDtypeStruct((n, d), BF),
            jax.ShapeDtypeStruct((n, d), BF),
            jax.ShapeDtypeStruct((SMALL, d), F32),
        ),
        in_specs=[
            pl.BlockSpec((rows, d), lambda g: (g, 0)),
            pl.BlockSpec((rows, d), lambda g: (g, 0)),
            pl.BlockSpec((rows, d), lambda g: (g, 0)),
            pl.BlockSpec(small.shape, lambda g: (0, 0)),
            pl.BlockSpec((1, d, d), lambda g: (3, 0, 0)),
        ],
        out_specs=(
            pl.BlockSpec((rows, d), lambda g: (g, 0)),
            pl.BlockSpec((rows, d), lambda g: (g, 0)),
            pl.BlockSpec((rows, d), lambda g: (g, 0)),
            pl.BlockSpec((SMALL, d), lambda g: (0, 0)),
        ),
        compiler_params=params(),
        cost_estimate=cost(2 * n * d * d, 18 * n * d + 2 * d * d),
        name="middle",
    )(c, hidden_grad, residual, small, weights)


def input_kernel(x_ref, three_ref, w_ref, small_ref, grad_ref, out_ref, sums_ref, total):
    g = pl.program_id(0)
    part = dot_nt(three_ref[0], w_ref[0])

    @pl.when(g == 0)
    def _():
        total[...] = part

    @pl.when(g > 0)
    def _():
        total[...] += part

    @pl.when(g == 2)
    def _():
        grad = total[...]
        unit, inv = norm_parts(x_ref[...].astype(F32))
        sums_ref[...] = jnp.zeros_like(sums_ref)
        sums_ref[0:1, :] = jnp.sum(grad * unit, axis=0, keepdims=True)
        sums_ref[1:2, :] = jnp.sum(grad, axis=0, keepdims=True)
        out_ref[...] = grad_ref[...] + norm_back(grad, unit, inv, small_ref[0:1, :])


def input_grads(x, three_grad, weights, small, residual_grad):
    n, d = x.shape
    return pl.pallas_call(
        input_kernel,
        grid=(3,),
        out_shape=(jax.ShapeDtypeStruct((n, d), F32), jax.ShapeDtypeStruct((SMALL, d), F32)),
        in_specs=[
            pl.BlockSpec((n, d), lambda g: (0, 0)),
            pl.BlockSpec((1, n, d), lambda g: (g, 0, 0)),
            pl.BlockSpec((1, d, d), lambda g: (g, 0, 0)),
            pl.BlockSpec(small.shape, lambda g: (0, 0)),
            pl.BlockSpec((n, d), lambda g: (0, 0)),
        ],
        out_specs=(
            pl.BlockSpec((n, d), lambda g: (0, 0)),
            pl.BlockSpec((SMALL, d), lambda g: (0, 0)),
        ),
        scratch_shapes=[pltpu.VMEM((n, d), F32)],
        compiler_params=params(),
        cost_estimate=cost(6 * n * d * d, 16 * n * d + 6 * d * d),
        name="input_grads",
    )(x, three_grad, weights, small, residual_grad)


def down_kernel(act_ref, w_ref, small_ref, residual_ref, out_ref, total):
    g = pl.program_id(0)
    part = dot(act_ref[0], w_ref[0])

    @pl.when(g == 0)
    def _():
        total[...] = residual_ref[...] + small_ref[4:5, :] + part

    @pl.when(g > 0)
    def _():
        total[...] += part

    @pl.when(g == 3)
    def _():
        out_ref[...] = total[...].astype(BF)


def down_out(act, weights, small, residual):
    n, d = residual.shape
    return pl.pallas_call(
        down_kernel,
        grid=(4,),
        out_shape=jax.ShapeDtypeStruct((n, d), BF),
        in_specs=[
            pl.BlockSpec((1, n, d), lambda g: (g, 0, 0)),
            pl.BlockSpec((1, d, d), lambda g: (g, 0, 0)),
            pl.BlockSpec(small.shape, lambda g: (0, 0)),
            pl.BlockSpec((n, d), lambda g: (0, 0)),
        ],
        out_specs=pl.BlockSpec((n, d), lambda g: (0, 0)),
        scratch_shapes=[pltpu.VMEM((n, d), F32)],
        compiler_params=params(),
        cost_estimate=cost(8 * n * d * d, 14 * n * d + 8 * d * d),
        name="down_out",
    )(act, weights, small, residual)


def local(dp, fsdp, tokens, lengths, *rest):
    (
        norm1_gain,
        norm1_bias,
        query_weight,
        key_weight,
        value_weight,
        output_weight,
        norm2_gain,
        norm2_bias,
        up_weight,
        up_bias,
        down_weight,
        down_bias,
        cotangent,
    ) = rest
    row_count, width = tokens.shape
    slot_count = lengths.shape[1]
    R = width // fsdp
    h = R // 2
    me_dp = lax.axis_index("dp").astype(jnp.int32)
    me_f = lax.axis_index("fsdp").astype(jnp.int32)
    d4 = me_dp % 4
    idx = jnp.stack([d4, me_f])
    masks = []
    mask = fsdp // 2
    while mask >= 1:
        masks.append(mask)
        mask //= 2
    masks = tuple(masks)
    outer = masks[:-1]

    def fswap(v, m):
        return swap(v, "fsdp", m, fsdp)

    def dswap(v, m):
        return swap(v, "dp", m, dp)

    shard4 = (query_weight, key_weight, value_weight, output_weight)
    piece1 = lax.select_n(d4, *shard4)
    piece2 = lax.dynamic_index_in_dim(
        up_weight.reshape(R, fsdp, 4, R), d4, axis=2, keepdims=False
    ).reshape(R, width)
    piece3 = lax.dynamic_slice_in_dim(down_weight, d4 * R, R, axis=0)

    tall = jnp.concatenate(
        [norm1_gain, norm1_bias, norm2_gain, norm2_bias, down_bias, up_bias]
    ).reshape(9, R)
    lane = jnp.arange(width, dtype=jnp.int32) // R
    tall = jnp.where((lane == me_f)[None, :], jnp.tile(tall, (1, fsdp)), jnp.zeros((), BF))
    tall = jnp.pad(tall, ((0, SMALL - 9), (0, 0)))

    def gather(piece, extra):
        size = R
        if extra is not None:
            piece = jnp.concatenate([piece, extra], axis=0)
            size = R + SMALL
        cur = piece[None]
        for m in outer[:-1]:
            cur = jnp.concatenate([cur, fswap(cur, m)], axis=0)
        m = outer[-1]
        other = fswap(cur, m)
        if extra is not None:
            a = jnp.concatenate(
                [
                    jnp.concatenate([t[:, :h], t[:, R:]], axis=1) for t in (cur, other)
                ],
                axis=0,
            )
        else:
            a = jnp.concatenate([cur[:, :h], other[:, :h]], axis=0)
        b = jnp.concatenate([cur[:, h:R], other[:, h:R]], axis=0)
        a_y = fswap(a, masks[-1])
        b_x = dswap(b, 2)
        small = None
        if extra is not None:
            small = jnp.sum(a[:, h:].astype(F32), axis=0) + jnp.sum(
                a_y[:, h:].astype(F32), axis=0
            )
        a1 = jnp.concatenate([a[:, :h], a_y[:, :h]], axis=0)
        b1 = jnp.concatenate([b, b_x], axis=0)
        a_x = dswap(a1, 2)
        b_y = fswap(b1, masks[-1])
        pieces = [a1, a_x, dswap(a1, 1), dswap(a_x, 1), b1, b_y, dswap(b1, 1), dswap(b_y, 1)]
        return assemble(idx, pieces, masks, fsdp, h, width), small

    first4, small = gather(piece1, tall)
    up4, _ = gather(piece2, None)
    down4, _ = gather(piece3, None)

    layout = row_layout(lengths[0], row_count, slot_count)
    cosine, sine = rotary_tables(layout[3])
    bias = jnp.where(allowed_pairs(layout, layout, BLOCK, slot_count), 0.0, NEGATIVE)
    normed, three = qkv(tokens, small, cosine, sine, first4)
    mixed, probs = attend(three, bias)
    residual, hidden_in = branch(tokens, mixed, first4, small)
    act, slope = up(hidden_in, up4, small)

    def both(xs, ys, x_of, y_of):
        args = (masks, fsdp, h)
        send = weight_grad(idx, xs, ys, x_of, y_of, (1, 3), *args)
        keep = weight_grad(idx, xs, ys, x_of, y_of, (0, 2), *args)
        return send, keep

    half = fsdp // 2

    def scatter(send, keep, small_sum=None):
        got = dswap(send, 1)
        a_send = keep[1, 0] + got[1, 0]
        a_keep = keep[0, 0] + got[0, 0]
        b_send = keep[:, 1, half:] + got[:, 1, half:]
        b_keep = keep[:, 1, :half] + got[:, 1, :half]
        extra = small_sum is not None

        def with_small(t, s):
            if not extra:
                return t
            return jnp.concatenate([t.reshape(-1, width), s.astype(BF)], axis=0)

        def parts(t, shape):
            if not extra:
                return t, None
            rows = math.prod(shape[:-1])
            return t[:rows].reshape(shape), t[rows:].astype(F32)

        if extra:
            small_sum = small_sum + dswap(small_sum.astype(BF), 1).astype(F32)
        a_got, s = parts(dswap(with_small(a_send, small_sum), 2), a_send.shape)
        b_got = fswap(b_send, masks[-1])
        if extra:
            small_sum = small_sum + s
        a_send = a_keep[half:] + a_got[half:]
        a_keep = a_keep[:half] + a_got[:half]
        b_send = b_keep[1] + b_got[1]
        b_keep = b_keep[0] + b_got[0]
        a_got, s = parts(fswap(with_small(a_send, small_sum), masks[-1]), a_send.shape)
        b_got = dswap(b_send, 2)
        if extra:
            small_sum = small_sum + s
        cur = jnp.stack([a_keep + a_got, b_keep + b_got], axis=1)
        for m in reversed(outer):
            count = cur.shape[0] // 2
            out = cur[count:]
            got, s = parts(fswap(with_small(out, small_sum), m), out.shape)
            if extra:
                small_sum = small_sum + s
            cur = cur[:count] + got
        total = cur.reshape(R, width)
        m = 4
        while m < dp:
            got, s = parts(dswap(with_small(total, small_sum), m), total.shape)
            total = total + got
            if extra:
                small_sum = small_sum + s
            m *= 2
        total_x = dswap(total, 2)
        four = jnp.stack([total, dswap(total, 1), total_x, dswap(total_x, 1)])
        return four, small_sum

    c1 = cotangent[None]
    send3, keep3 = both(act, c1, lambda d: d, lambda d: 0)
    pre_grad, sums_act, hidden_grad = act_grad(cotangent, down4, up4, slope)
    residual_grad, branch_grad, mixed_grad, sums_mid = middle(
        cotangent, hidden_grad, residual, small, first4
    )
    send2, keep2 = both(hidden_in[None], pre_grad, lambda d: 0, lambda d: d)
    three_grad = attend_back(three, probs, mixed_grad, mixed, cosine, sine)
    lefts = jnp.stack([normed, mixed])
    rights = jnp.concatenate([three_grad, branch_grad[None]], axis=0)
    send1, keep1 = both(lefts, rights, lambda d: d // 3, lambda d: d)
    input_grad, sums_in = input_grads(tokens, three_grad, first4, small, residual_grad)
    output = down_out(act, down4, small, residual)

    four3, _ = scatter(send3, keep3)
    four2, _ = scatter(send2, keep2)
    four1, small_sum = scatter(send1, keep1, sums_act + sums_mid + sums_in)

    def pick(four, d):
        return lax.dynamic_index_in_dim(four, d4 ^ d, axis=0, keepdims=False).astype(F32)

    first_grads = [pick(four1, d) for d in range(4)]
    up_grad = jnp.stack(
        [pick(four2, d).reshape(R, fsdp, R) for d in range(4)], axis=2
    ).reshape(R, 4 * width)
    down_grad = jnp.concatenate([pick(four3, d) for d in range(4)], axis=0)
    own = lax.dynamic_slice_in_dim(small_sum, me_f * R, R, axis=1)
    return (
        output,
        input_grad,
        own[0],
        own[1],
        first_grads[0],
        first_grads[1],
        first_grads[2],
        first_grads[3],
        own[2],
        own[3],
        up_grad,
        own[5:9].reshape(4 * R),
        down_grad,
        own[4],
    )


def solution(mesh):
    rows = P(("dp", "fsdp"), None)
    flat = P("fsdp")
    tall = P("fsdp", None)
    in_specs = (
        rows, rows, flat, flat, tall, tall, tall, tall, flat, flat, tall, flat, tall, flat, rows,
    )
    out_specs = (
        rows, rows, flat, flat, tall, tall, tall, tall, flat, flat, tall, flat, tall, flat,
    )
    return jax.shard_map(
        partial(local, mesh.shape["dp"], mesh.shape["fsdp"]),
        mesh=mesh,
        in_specs=in_specs,
        out_specs=out_specs,
        check_vma=False,
    )
```

```python
from functools import partial
import math

import jax
import jax.numpy as jnp
from jax import lax
from jax.experimental import pallas as pl
from jax.experimental.pallas import tpu as pltpu
from jax.sharding import PartitionSpec as P

H = 12
HD = 64
BLOCK = 16
EPSILON = 1e-05
BASE = 10000.0
NEGATIVE = -1e30
BF = jnp.bfloat16
F32 = jnp.float32
SMALL = 16
LONG = 160
VMEM_LIMIT = 56 * 1024 * 1024


def row_layout(length_row, row_count, slot_count):
    doubled = 2 * length_row
    ends_at = jnp.cumsum(doubled, dtype=jnp.int32)
    starts_at = ends_at - doubled
    row_index = jnp.arange(row_count, dtype=jnp.int32)
    member = (row_index[:, None] >= starts_at[None, :]) & (row_index[:, None] < ends_at[None, :])
    slot_ids = jnp.arange(slot_count, dtype=jnp.int32)
    slot_index = jnp.sum(jnp.where(member, slot_ids[None, :], 0), axis=1, dtype=jnp.int32)
    start_row = jnp.sum(jnp.where(member, starts_at[None, :], 0), axis=1, dtype=jnp.int32)
    seq_length = jnp.sum(jnp.where(member, length_row[None, :], 0), axis=1, dtype=jnp.int32)
    local_row = row_index - start_row
    clean_flag = (local_row >= seq_length).astype(jnp.int32)
    position = local_row - clean_flag * seq_length
    return (row_index, slot_index, clean_flag, position)


def allowed_pairs(query_side, key_side, block_size, slot_count):
    query_row, query_slot, query_clean, query_pos = query_side
    key_row, key_slot, key_clean, key_pos = key_side
    query_block = query_pos // block_size
    key_block = key_pos // block_size
    same_seq = query_slot[:, None] == key_slot[None, :]
    key_noisy = key_clean[None, :] == 0
    key_plain = key_clean[None, :] == 1
    noisy_rule = key_noisy & (key_block[None, :] == query_block[:, None]) | key_plain & (
        key_block[None, :] < query_block[:, None]
    )
    clean_rule = key_plain & (key_block[None, :] <= query_block[:, None])
    rule_held = jnp.where(query_clean[:, None] == 1, clean_rule, noisy_rule)
    padded = query_slot == slot_count - 1
    real_pairs = same_seq & rule_held & jnp.logical_not(padded)[:, None]
    self_pairs = padded[:, None] & (query_row[:, None] == key_row[None, :])
    return real_pairs | self_pairs


def rotary_tables(position):
    half = HD // 2
    lane = jnp.arange(2 * HD, dtype=jnp.int32)
    freqs = jnp.exp((lane % half).astype(F32) * (-2.0 * math.log(BASE) / HD))
    angles = position.astype(F32)[:, None] * freqs[None, :]
    sign = jnp.where(lane % HD < half, -1.0, 1.0)
    return jnp.cos(angles), jnp.sin(angles) * sign[None, :]


def swap(values, axis, mask, size):
    return lax.ppermute(values, axis, [(i, i ^ mask) for i in range(size)])


def dot(a, b):
    return jnp.dot(a, b, preferred_element_type=F32)


def dot_nt(a, b):
    return lax.dot_general(a, b, (((1,), (1,)), ((), ())), preferred_element_type=F32)


def dot_tn(a, b):
    return lax.dot_general(a, b, (((0,), (0,)), ((), ())), preferred_element_type=F32)


def params(**more):
    return pltpu.CompilerParams(vmem_limit_bytes=VMEM_LIMIT, **more)


def cost(flops, moved):
    return pl.CostEstimate(flops=int(flops), bytes_accessed=int(moved), transcendentals=0)


def norm_parts(values):
    center = values - jnp.mean(values, axis=-1, keepdims=True)
    spread = jnp.mean(center * center, axis=-1, keepdims=True)
    inv = lax.rsqrt(spread + EPSILON)
    return center * inv, inv


def norm_back(grad, unit, inv, gain):
    scaled = grad * gain
    first = jnp.mean(scaled, axis=-1, keepdims=True)
    second = jnp.mean(scaled * unit, axis=-1, keepdims=True)
    return inv * (scaled - first - unit * second)


def turn(values, cosine, sine):
    half = HD // 2
    pair = 2 * HD
    lane = lax.broadcasted_iota(jnp.int32, (1, pair), 1)
    low = (lane % HD) < half
    parts = []
    for at in range(0, values.shape[1], pair):
        part = values[:, at : at + pair]
        other = jnp.where(low, pltpu.roll(part, pair - half, 1), pltpu.roll(part, half, 1))
        parts.append(part * cosine + other * sine)
    return parts[0] if len(parts) == 1 else jnp.concatenate(parts, axis=1)


def bits_of(index, masks):
    total = 0
    for bit, mask in enumerate(masks):
        if (index >> bit) & 1:
            total |= mask
    return total


def piece_map(which, masks):
    count = 1 << len(masks)
    half = count // 2
    kind, r, y = which
    if kind == "a":
        return [((i,), r, bits_of(i, masks), 0) for i in range(count)]
    return [
        ((x * half + i,), r | (2 * x), bits_of(i, masks) | y, 1)
        for x in range(2)
        for i in range(half)
    ]


def fetch(pieces, maps, me_f, h, w_ref, slot_of, sems):
    for ref, entries in zip(pieces, maps):
        for at, r, k, colour in entries:
            slot = slot_of(r)
            pltpu.make_async_copy(
                ref.at[at],
                w_ref.at[slot, me_f ^ k, pl.ds(colour * h, h)],
                sems.at[slot],
            ).start()


def fetched(w_ref, slot, sems):
    pltpu.make_async_copy(w_ref.at[slot], w_ref.at[slot], sems.at[slot]).wait()


def qkv_kernel(
    maps, h, idx_ref, x_ref, small_ref, cos_ref, sin_ref, p0, p1, p2, p3, p4, p5, p6, p7,
    normed_ref, out_ref, w_out, keep, w_ref, sems, out_sems,
):
    g = pl.program_id(0)
    d4, me_f = idx_ref[0], idx_ref[1]
    d = keep.shape[1]

    def send(slot):
        return pltpu.make_async_copy(w_ref.at[slot], w_out.at[slot], out_sems.at[slot])

    @pl.when(g == 0)
    def _():
        fetch((p0, p1, p2, p3, p4, p5, p6, p7), maps, me_f, h, w_ref, lambda r: d4 ^ r, sems)
        unit, _ = norm_parts(x_ref[...].astype(F32))
        normed = (unit * small_ref[0:1, :] + small_ref[1:2, :]).astype(BF)
        keep[...] = normed
        normed_ref[...] = normed

    fetched(w_ref, g, sems)
    send(g).start()

    @pl.when(g == 2)
    def _():
        fetched(w_ref, 3, sems)
        send(3).start()

    product = dot(keep[...], w_ref[g].reshape(d, d))

    @pl.when(g < 2)
    def _():
        out_ref[0] = turn(product, cos_ref[...], sin_ref[...]).astype(BF)

    @pl.when(g == 2)
    def _():
        out_ref[0] = product.astype(BF)
        for slot in range(4):
            send(slot).wait()


def qkv(idx, x, small, cosine, sine, pieces, maps, shards, h):
    n, d = x.shape
    return pl.pallas_call(
        partial(qkv_kernel, maps, h),
        grid=(3,),
        out_shape=(
            jax.ShapeDtypeStruct((n, d), BF),
            jax.ShapeDtypeStruct((3, n, d), BF),
            jax.ShapeDtypeStruct((4, shards, 2 * h, d), BF),
        ),
        in_specs=[
            pl.BlockSpec(memory_space=pltpu.SMEM),
            pl.BlockSpec((n, d), lambda g: (0, 0)),
            pl.BlockSpec(small.shape, lambda g: (0, 0)),
            pl.BlockSpec(cosine.shape, lambda g: (0, 0)),
            pl.BlockSpec(sine.shape, lambda g: (0, 0)),
        ]
        + [pl.BlockSpec(memory_space=pl.ANY)] * 8,
        out_specs=(
            pl.BlockSpec((n, d), lambda g: (0, 0)),
            pl.BlockSpec((1, n, d), lambda g: (g, 0, 0)),
            pl.BlockSpec(memory_space=pl.ANY),
        ),
        scratch_shapes=[
            pltpu.VMEM((n, d), BF),
            pltpu.VMEM((4, shards, 2 * h, d), BF),
            pltpu.SemaphoreType.DMA((4,)),
            pltpu.SemaphoreType.DMA((4,)),
        ],
        compiler_params=params(),
        cost_estimate=cost(6 * n * d * d, 2 * (5 * n * d + 8 * d * d)),
        name="qkv",
    )(idx, x, small, cosine, sine, *pieces)


def head_mask(which):
    lane = lax.broadcasted_iota(jnp.int32, (1, 2 * HD), 1)
    return (lane < HD) if which == 0 else (lane >= HD)


def attend_kernel(q_ref, k_ref, v_ref, bias_ref, mixed_ref, probs_ref):
    q, k, v = q_ref[0], k_ref[0], v_ref[0]
    zero = jnp.zeros((), BF)
    parts = []
    for h in range(2):
        own = jnp.where(head_mask(h), q, zero)
        scores = dot_nt(own, k) * (HD**-0.5) + bias_ref[...]
        top = jnp.max(scores, axis=1, keepdims=True)
        raised = jnp.exp(scores - top)
        total = jnp.sum(raised, axis=1, keepdims=True)
        probs = (raised * (1.0 / total)).astype(BF)
        probs_ref[h] = probs
        parts.append(dot(probs, v))
    mixed_ref[...] = jnp.where(head_mask(0), parts[0], parts[1]).astype(BF)


def attend(three, bias):
    _, n, d = three.shape
    pair = 2 * HD
    return pl.pallas_call(
        attend_kernel,
        grid=(d // pair,),
        out_shape=(
            jax.ShapeDtypeStruct((n, d), BF),
            jax.ShapeDtypeStruct((d // HD, n, n), BF),
        ),
        in_specs=[
            pl.BlockSpec((1, n, pair), lambda p: (0, 0, p)),
            pl.BlockSpec((1, n, pair), lambda p: (1, 0, p)),
            pl.BlockSpec((1, n, pair), lambda p: (2, 0, p)),
            pl.BlockSpec((n, n), lambda p: (0, 0)),
        ],
        out_specs=(
            pl.BlockSpec((n, pair), lambda p: (0, p)),
            pl.BlockSpec((2, n, n), lambda p: (p, 0, 0)),
        ),
        compiler_params=params(),
        cost_estimate=cost(8 * n * n * d, 2 * n * n * (d // HD) + 8 * n * d),
        name="attend",
    )(three, three, three, bias)


def attend_back_kernel(
    q_ref, k_ref, v_ref, probs_ref, grad_ref, mixed_ref, cos_ref, sin_ref, out_ref
):
    q, k, v, grad = q_ref[0], k_ref[0], v_ref[0], grad_ref[...]
    zero = jnp.zeros((), BF)
    product = grad.astype(F32) * mixed_ref[...].astype(F32)
    dq, dk, dv = [], [], []
    for h in range(2):
        mask = head_mask(h)
        inner = jnp.sum(jnp.where(mask, product, 0.0), axis=1, keepdims=True)
        probs = probs_ref[h]
        prob_grad = dot_nt(jnp.where(mask, grad, zero), v)
        score_grad = (probs.astype(F32) * (prob_grad - inner)).astype(BF)
        dq.append(dot(score_grad, k))
        dk.append(dot_tn(score_grad, q))
        dv.append(dot_tn(probs, grad))
    first = head_mask(0)
    scale = HD**-0.5
    cosine, sine = cos_ref[...], sin_ref[...]
    out_ref[0] = turn(jnp.where(first, dq[0], dq[1]) * scale, cosine, -sine).astype(BF)
    out_ref[1] = turn(jnp.where(first, dk[0], dk[1]) * scale, cosine, -sine).astype(BF)
    out_ref[2] = jnp.where(first, dv[0], dv[1]).astype(BF)


def attend_back(three, probs, grad, mixed, cosine, sine):
    _, n, d = three.shape
    pair = 2 * HD
    return pl.pallas_call(
        attend_back_kernel,
        grid=(d // pair,),
        out_shape=jax.ShapeDtypeStruct((3, n, d), BF),
        in_specs=[
            pl.BlockSpec((1, n, pair), lambda p: (0, 0, p)),
            pl.BlockSpec((1, n, pair), lambda p: (1, 0, p)),
            pl.BlockSpec((1, n, pair), lambda p: (2, 0, p)),
            pl.BlockSpec((2, n, n), lambda p: (p, 0, 0)),
            pl.BlockSpec((n, pair), lambda p: (0, p)),
            pl.BlockSpec((n, pair), lambda p: (0, p)),
            pl.BlockSpec(cosine.shape, lambda p: (0, 0)),
            pl.BlockSpec(sine.shape, lambda p: (0, 0)),
        ],
        out_specs=pl.BlockSpec((3, n, pair), lambda p: (0, 0, p)),
        compiler_params=params(),
        cost_estimate=cost(16 * n * n * d, 2 * n * n * (d // HD) + 16 * n * d),
        name="attend_back",
    )(three, three, three, probs, grad, mixed, cosine, sine)


def branch_kernel(x_ref, mixed_ref, w_ref, small_ref, residual_ref, hidden_ref):
    residual = x_ref[...].astype(F32) + dot(mixed_ref[...], w_ref[0])
    residual_ref[...] = residual
    unit, _ = norm_parts(residual)
    hidden_ref[...] = (unit * small_ref[2:3, :] + small_ref[3:4, :]).astype(BF)


def branch(x, mixed, weights, small):
    n, d = x.shape
    rows = n // 2
    return pl.pallas_call(
        branch_kernel,
        grid=(2,),
        out_shape=(jax.ShapeDtypeStruct((n, d), F32), jax.ShapeDtypeStruct((n, d), BF)),
        in_specs=[
            pl.BlockSpec((rows, d), lambda g: (g, 0)),
            pl.BlockSpec((rows, d), lambda g: (g, 0)),
            pl.BlockSpec((1, d, d), lambda g: (3, 0, 0)),
            pl.BlockSpec(small.shape, lambda g: (0, 0)),
        ],
        out_specs=(
            pl.BlockSpec((rows, d), lambda g: (g, 0)),
            pl.BlockSpec((rows, d), lambda g: (g, 0)),
        ),
        compiler_params=params(),
        cost_estimate=cost(2 * n * d * d, 10 * n * d + 2 * d * d),
        name="branch",
    )(x, mixed, weights, small)


def spread(out_ref, keep, product, me_f, masks, h, shards):
    keep[...] = product.astype(BF)
    for i in range(shards):
        j = me_f ^ bits_of(i, masks)
        for colour in range(2):
            start = pl.multiple_of(j * (2 * h) + colour * h, h & -h)
            out_ref[0, colour, i] = keep[pl.ds(start, h), :]


def up_kernel(
    masks, maps, rs, h, shards, idx_ref, hidden_ref, c_ref, small_ref, p0, p1, p2, p3,
    act_ref, slope_ref, grad_ref, w_out, w_ref, keep, sems, out_sems,
):
    g = pl.program_id(0)
    d4, me_f = idx_ref[0], idx_ref[1]
    d = hidden_ref.shape[1]

    def send(slot):
        return pltpu.make_async_copy(w_ref.at[slot], w_out.at[slot], out_sems.at[slot])

    @pl.when(g == 0)
    def _():
        fetch((p0, p1, p2, p3), maps, me_f, h, w_ref, rs.index, sems)

    fetched(w_ref, g, sems)
    send(g).start()
    chunk = d4 ^ jnp.where(g == 0, rs[0], rs[1])
    bias = small_ref[5:6, :]
    for other in range(1, 4):
        bias = jnp.where(chunk == other, small_ref[5 + other : 6 + other, :], bias)
    v = dot(hidden_ref[...], w_ref[g].reshape(d, d)) + bias
    c = math.sqrt(2.0 / math.pi)
    square = v * v
    t = jnp.tanh(v * (c + (c * 0.044715) * square))
    half = 0.5 * (1.0 + t)
    act = (v * half).astype(BF)
    act_ref[0] = act
    slope = half + (0.5 * v) * (1.0 - t * t) * (c + (3.0 * c * 0.044715) * square)
    slope_ref[0] = slope.astype(BF)
    spread(grad_ref, keep, dot_tn(act, c_ref[...]), me_f, masks, h, shards)

    @pl.when(g == 1)
    def _():
        send(0).wait()
        send(1).wait()


def up(idx, hidden, c, small, pieces, maps, rs, masks, shards, h):
    n, d = hidden.shape
    return pl.pallas_call(
        partial(up_kernel, masks, maps, rs, h, shards),
        grid=(2,),
        out_shape=(
            jax.ShapeDtypeStruct((2, n, d), BF),
            jax.ShapeDtypeStruct((2, n, d), BF),
            jax.ShapeDtypeStruct((2, 2, shards, h, d), BF),
            jax.ShapeDtypeStruct((2, shards, 2 * h, d), BF),
        ),
        in_specs=[
            pl.BlockSpec(memory_space=pltpu.SMEM),
            pl.BlockSpec((n, d), lambda g: (0, 0)),
            pl.BlockSpec((n, d), lambda g: (0, 0)),
            pl.BlockSpec(small.shape, lambda g: (0, 0)),
        ]
        + [pl.BlockSpec(memory_space=pl.ANY)] * 4,
        out_specs=(
            pl.BlockSpec((1, n, d), lambda g: (g, 0, 0)),
            pl.BlockSpec((1, n, d), lambda g: (g, 0, 0)),
            pl.BlockSpec((1, 2, shards, h, d), lambda g: (g, 0, 0, 0, 0)),
            pl.BlockSpec(memory_space=pl.ANY),
        ),
        scratch_shapes=[
            pltpu.VMEM((2, shards, 2 * h, d), BF),
            pltpu.VMEM((d, d), BF),
            pltpu.SemaphoreType.DMA((2,)),
            pltpu.SemaphoreType.DMA((2,)),
        ],
        compiler_params=params(),
        cost_estimate=cost((LONG if rs[0] == 0 else 8) * n * d * d, 2 * (6 * n * d + 6 * d * d)),
        name="up",
    )(idx, hidden, c, small, *pieces)


def act_grad_kernel(
    masks, maps, rs, h, shards, first, idx_ref, c_ref, x_ref, up_ref, slope_ref, p0, p1, p2, p3,
    *more,
):
    if first:
        (hidden_ref, sums_ref, grad_ref, w_out, w_ref, keep, sems, out_sems) = more
    else:
        (
            hidden_in, sums_in, hidden_ref, sums_ref, grad_ref, w_out, w_ref, keep, sems, out_sems,
        ) = more
    g = pl.program_id(0)
    d4, me_f = idx_ref[0], idx_ref[1]
    d = x_ref.shape[1]
    c = c_ref[...]

    def send(slot):
        return pltpu.make_async_copy(w_ref.at[slot], w_out.at[slot], out_sems.at[slot])

    @pl.when(g == 0)
    def _():
        fetch((p0, p1, p2, p3), maps, me_f, h, w_ref, rs.index, sems)
        if first:
            hidden_ref[...] = jnp.zeros_like(hidden_ref)
            sums_ref[...] = jnp.zeros_like(sums_ref)
            sums_ref[4:5, :] = jnp.sum(c.astype(F32), axis=0, keepdims=True)
        else:
            hidden_ref[...] = hidden_in[...]
            sums_ref[...] = sums_in[...]

    fetched(w_ref, g, sems)
    send(g).start()
    chunk = d4 ^ jnp.where(g == 0, rs[0], rs[1])
    pre = (dot_nt(c, w_ref[g].reshape(d, d)) * slope_ref[0].astype(F32)).astype(BF)
    sums = jnp.sum(pre.astype(F32), axis=0, keepdims=True)
    row = lax.broadcasted_iota(jnp.int32, (sums_ref.shape[0], 1), 0)
    sums_ref[...] += jnp.where(row == 5 + chunk, sums, 0.0)
    hidden_ref[...] += dot_nt(pre, up_ref[0])
    spread(grad_ref, keep, dot_tn(x_ref[...], pre), me_f, masks, h, shards)

    @pl.when(g == 1)
    def _():
        send(0).wait()
        send(1).wait()


def act_grad(idx, c, hidden, up_half, slope, pieces, maps, rs, masks, shards, h, before=None):
    n, d = c.shape
    whole = pl.BlockSpec((n, d), lambda g: (0, 0))
    sums = pl.BlockSpec((SMALL, d), lambda g: (0, 0))
    return pl.pallas_call(
        partial(act_grad_kernel, masks, maps, rs, h, shards, before is None),
        grid=(2,),
        out_shape=(
            jax.ShapeDtypeStruct((n, d), F32),
            jax.ShapeDtypeStruct((SMALL, d), F32),
            jax.ShapeDtypeStruct((2, 2, shards, h, d), BF),
            jax.ShapeDtypeStruct((2, shards, 2 * h, d), BF),
        ),
        in_specs=[
            pl.BlockSpec(memory_space=pltpu.SMEM),
            whole,
            whole,
            pl.BlockSpec((1, d, d), lambda g: (g, 0, 0)),
            pl.BlockSpec((1, n, d), lambda g: (g, 0, 0)),
        ]
        + [pl.BlockSpec(memory_space=pl.ANY)] * 4
        + ([] if before is None else [whole, sums]),
        out_specs=(
            whole,
            sums,
            pl.BlockSpec((1, 2, shards, h, d), lambda g: (g, 0, 0, 0, 0)),
            pl.BlockSpec(memory_space=pl.ANY),
        ),
        scratch_shapes=[
            pltpu.VMEM((2, shards, 2 * h, d), BF),
            pltpu.VMEM((d, d), BF),
            pltpu.SemaphoreType.DMA((2,)),
            pltpu.SemaphoreType.DMA((2,)),
        ],
        compiler_params=params(),
        cost_estimate=cost((LONG if rs[0] == 0 else 12) * n * d * d, 2 * (8 * n * d + 8 * d * d)),
        name="act_grad",
    )(idx, c, hidden, up_half.reshape(2, d, d), slope, *pieces, *(before or ()))


def first_grad_kernel(
    masks, h, shards, rs, idx_ref, normed_ref, mixed_ref, three_ref, branch_ref, out_ref, keep
):
    g = pl.program_id(0)
    last = (idx_ref[0] ^ jnp.where(g == 0, rs[0], rs[1])) == 3
    x = jnp.where(last, mixed_ref[...], normed_ref[...])
    y = jnp.where(last, branch_ref[...], three_ref[0])
    spread(out_ref, keep, dot_tn(x, y), idx_ref[1], masks, h, shards)


def first_grad(idx, normed, mixed, three_grad, branch_grad, rs, masks, shards, h):
    n, d = normed.shape

    def which(g, idx_ref):
        return jnp.minimum(idx_ref[0] ^ jnp.where(g == 0, rs[0], rs[1]), 2)

    whole = pl.BlockSpec((n, d), lambda g, i: (0, 0))
    return pl.pallas_call(
        partial(first_grad_kernel, masks, h, shards, rs),
        grid_spec=pltpu.PrefetchScalarGridSpec(
            num_scalar_prefetch=1,
            grid=(2,),
            in_specs=[
                whole,
                whole,
                pl.BlockSpec((1, n, d), lambda g, i: (which(g, i), 0, 0)),
                whole,
            ],
            out_specs=pl.BlockSpec((1, 2, shards, h, d), lambda g, i: (g, 0, 0, 0, 0)),
            scratch_shapes=[pltpu.VMEM((d, d), BF)],
        ),
        out_shape=jax.ShapeDtypeStruct((2, 2, shards, h, d), BF),
        compiler_params=params(),
        cost_estimate=cost((LONG if rs[0] == 0 else 4) * n * d * d, 2 * (5 * n * d + 2 * d * d)),
        name="first_grad",
    )(idx, normed, mixed, three_grad, branch_grad)


def middle_kernel(
    c_ref, hidden_ref, residual_ref, small_ref, w_ref, grad_ref, low_ref, mixed_ref, sums_ref
):
    @pl.when(pl.program_id(0) == 0)
    def _():
        sums_ref[...] = jnp.zeros_like(sums_ref)

    grad = hidden_ref[...]
    unit, inv = norm_parts(residual_ref[...])
    sums_ref[2:3, :] += jnp.sum(grad * unit, axis=0, keepdims=True)
    sums_ref[3:4, :] += jnp.sum(grad, axis=0, keepdims=True)
    full = c_ref[...].astype(F32) + norm_back(grad, unit, inv, small_ref[2:3, :])
    grad_ref[...] = full
    low = full.astype(BF)
    low_ref[...] = low
    mixed_ref[...] = dot_nt(low, w_ref[0]).astype(BF)


def middle(c, hidden_grad, residual, small, weights):
    n, d = c.shape
    rows = n // 2
    return pl.pallas_call(
        middle_kernel,
        grid=(2,),
        out_shape=(
            jax.ShapeDtypeStruct((n, d), F32),
            jax.ShapeDtypeStruct((n, d), BF),
            jax.ShapeDtypeStruct((n, d), BF),
            jax.ShapeDtypeStruct((SMALL, d), F32),
        ),
        in_specs=[
            pl.BlockSpec((rows, d), lambda g: (g, 0)),
            pl.BlockSpec((rows, d), lambda g: (g, 0)),
            pl.BlockSpec((rows, d), lambda g: (g, 0)),
            pl.BlockSpec(small.shape, lambda g: (0, 0)),
            pl.BlockSpec((1, d, d), lambda g: (3, 0, 0)),
        ],
        out_specs=(
            pl.BlockSpec((rows, d), lambda g: (g, 0)),
            pl.BlockSpec((rows, d), lambda g: (g, 0)),
            pl.BlockSpec((rows, d), lambda g: (g, 0)),
            pl.BlockSpec((SMALL, d), lambda g: (0, 0)),
        ),
        compiler_params=params(),
        cost_estimate=cost(2 * n * d * d, 18 * n * d + 2 * d * d),
        name="middle",
    )(c, hidden_grad, residual, small, weights)


def input_kernel(x_ref, three_ref, w_ref, small_ref, grad_ref, out_ref, sums_ref, total):
    g = pl.program_id(0)
    part = dot_nt(three_ref[0], w_ref[0])

    @pl.when(g == 0)
    def _():
        total[...] = part

    @pl.when(g > 0)
    def _():
        total[...] += part

    @pl.when(g == 2)
    def _():
        grad = total[...]
        unit, inv = norm_parts(x_ref[...].astype(F32))
        sums_ref[...] = jnp.zeros_like(sums_ref)
        sums_ref[0:1, :] = jnp.sum(grad * unit, axis=0, keepdims=True)
        sums_ref[1:2, :] = jnp.sum(grad, axis=0, keepdims=True)
        out_ref[...] = grad_ref[...] + norm_back(grad, unit, inv, small_ref[0:1, :])


def input_grads(x, three_grad, weights, small, residual_grad):
    n, d = x.shape
    return pl.pallas_call(
        input_kernel,
        grid=(3,),
        out_shape=(jax.ShapeDtypeStruct((n, d), F32), jax.ShapeDtypeStruct((SMALL, d), F32)),
        in_specs=[
            pl.BlockSpec((n, d), lambda g: (0, 0)),
            pl.BlockSpec((1, n, d), lambda g: (g, 0, 0)),
            pl.BlockSpec((1, d, d), lambda g: (g, 0, 0)),
            pl.BlockSpec(small.shape, lambda g: (0, 0)),
            pl.BlockSpec((n, d), lambda g: (0, 0)),
        ],
        out_specs=(
            pl.BlockSpec((n, d), lambda g: (0, 0)),
            pl.BlockSpec((SMALL, d), lambda g: (0, 0)),
        ),
        scratch_shapes=[pltpu.VMEM((n, d), F32)],
        compiler_params=params(),
        cost_estimate=cost(6 * n * d * d, 16 * n * d + 6 * d * d),
        name="input_grads",
    )(x, three_grad, weights, small, residual_grad)


def down_kernel(a0_ref, a1_ref, w0_ref, w1_ref, small_ref, residual_ref, out_ref, total):
    g = pl.program_id(0)
    part = dot(a0_ref[0], w0_ref[0]) + dot(a1_ref[0], w1_ref[0])

    @pl.when(g == 0)
    def _():
        total[...] = residual_ref[...] + small_ref[4:5, :] + part

    @pl.when(g == 1)
    def _():
        out_ref[...] = (total[...] + part).astype(BF)


def down_out(acts, weights, small, residual):
    n, d = residual.shape
    return pl.pallas_call(
        down_kernel,
        grid=(2,),
        out_shape=jax.ShapeDtypeStruct((n, d), BF),
        in_specs=[
            pl.BlockSpec((1, n, d), lambda g: (g, 0, 0)),
            pl.BlockSpec((1, n, d), lambda g: (g, 0, 0)),
            pl.BlockSpec((1, d, d), lambda g: (g, 0, 0)),
            pl.BlockSpec((1, d, d), lambda g: (g, 0, 0)),
            pl.BlockSpec(small.shape, lambda g: (0, 0)),
            pl.BlockSpec((n, d), lambda g: (0, 0)),
        ],
        out_specs=pl.BlockSpec((n, d), lambda g: (0, 0)),
        scratch_shapes=[pltpu.VMEM((n, d), F32)],
        compiler_params=params(),
        cost_estimate=cost(8 * n * d * d, 14 * n * d + 8 * d * d),
        name="down_out",
    )(*acts, *(w.reshape(2, d, d) for w in weights), small, residual)


def local(dp, fsdp, tokens, lengths, *rest):
    (
        norm1_gain,
        norm1_bias,
        query_weight,
        key_weight,
        value_weight,
        output_weight,
        norm2_gain,
        norm2_bias,
        up_weight,
        up_bias,
        down_weight,
        down_bias,
        cotangent,
    ) = rest
    row_count, width = tokens.shape
    slot_count = lengths.shape[1]
    R = width // fsdp
    h = R // 2
    me_dp = lax.axis_index("dp").astype(jnp.int32)
    me_f = lax.axis_index("fsdp").astype(jnp.int32)
    d4 = me_dp % 4
    idx = jnp.stack([d4, me_f])
    masks = []
    mask = fsdp // 2
    while mask >= 1:
        masks.append(mask)
        mask //= 2
    masks = tuple(masks)
    outer = masks[:-1]

    def fswap(v, m):
        return swap(v, "fsdp", m, fsdp)

    def dswap(v, m):
        return swap(v, "dp", m, dp)

    def after(value, *tokens):
        return lax.optimization_barrier((value,) + tokens)[0]

    def after_all(values, *tokens):
        values = tuple(values)
        return list(lax.optimization_barrier(values + tokens)[: len(values)])

    half = fsdp // 2
    maps_own = [
        piece_map(w, masks) for w in (("a", 0, 0), ("a", 2, 0), ("b", 0, 0), ("b", 0, 1))
    ]
    maps_core = [
        piece_map(w, masks) for w in (("a", 1, 0), ("a", 3, 0), ("b", 1, 0), ("b", 1, 1))
    ]

    class Gather:
        def __init__(self, piece):
            self.cur = piece[None]

        def far(self, m):
            self.got = fswap(self.cur, m)

        def join(self):
            self.cur = jnp.concatenate([self.cur, self.got], axis=0)

        def near(self):
            self.got = fswap(self.cur, outer[-1])

        def sides(self):
            a = jnp.concatenate([self.cur[:, :h], self.got[:, :h]], axis=0)
            b = jnp.concatenate([self.cur[:, h:R], self.got[:, h:R]], axis=0)
            self.ab = (a, b)
            self.got_ab = (fswap(a, masks[-1]), dswap(b, 2))
            if self.cur.shape[1] > R:
                rest = [jnp.sum(t[:, R:].astype(F32), axis=0) for t in (self.cur, self.got)]
                self.small = rest[0] + rest[1]

        def cross(self):
            a1 = jnp.concatenate([self.ab[0], self.got_ab[0]], axis=0)
            b1 = jnp.concatenate([self.ab[1], self.got_ab[1]], axis=0)
            self.ab1 = (a1, b1)
            self.got_ab1 = (dswap(a1, 2), fswap(b1, masks[-1]))
            self.core = [dswap(a1, 1), dswap(b1, 1)]

        def finish(self):
            a_x, b_y = self.got_ab1
            a1, b1 = self.ab1
            self.own = [a1, a_x, b1, b_y]
            self.other = [self.core[0], dswap(a_x, 1), self.core[1], dswap(b_y, 1)]

    class Inner:
        def __init__(self, cur):
            self.cur = cur
            self.left = list(reversed(outer))

        def send(self):
            m = self.left.pop(0)
            count = self.cur.shape[0] // 2
            self.got = fswap(self.cur[count:], m)
            self.cur = self.cur[:count]

        def add(self, *tokens):
            self.cur = self.cur + after(self.got, *tokens)

        def sums(self):
            while self.left:
                self.send()
                self.add()

        def spread(self):
            total = self.cur[0]
            m = 4
            while m < dp:
                total = total + dswap(total, m)
                m *= 2
            self.total = total
            self.pair = dswap(total, 2)

        def four(self, *tokens):
            pair = after(self.pair, *tokens)
            return jnp.stack([self.total, dswap(self.total, 1), pair, dswap(pair, 1)])

    piece1 = lax.select_n(d4, query_weight, key_weight, value_weight, output_weight)
    g1 = Gather(piece1)
    for m in outer[:-1]:
        g1.far(m)
        g1.join()
    g1.near()
    vectors = after_all(
        (norm1_gain, norm1_bias, norm2_gain, norm2_bias, down_bias, up_bias, up_weight), piece1
    )
    tall = jnp.concatenate(vectors[:6]).reshape(9, R)
    lane = jnp.arange(width, dtype=jnp.int32) // R
    tall = jnp.where((lane == me_f)[None, :], jnp.tile(tall, (1, fsdp)), jnp.zeros((), BF))
    tall = jnp.pad(tall, ((0, SMALL - 9), (0, 0)))
    up_part = lax.dynamic_index_in_dim(
        vectors[6].reshape(R, fsdp, 4, R), d4, axis=2, keepdims=False
    ).reshape(R, width)
    piece2 = jnp.concatenate([up_part, tall], axis=0)
    g2 = Gather(after(piece2, g1.cur))
    for m in outer[:-1]:
        g2.far(m)
        g2.join()
    g1.sides()
    g2.cur, g2.got = after_all((g2.cur, g2.got), *g1.ab)
    g2.near()
    g1.cross()
    g3 = Gather(
        lax.dynamic_slice_in_dim(after(down_weight, *g1.ab1), d4 * R, R, axis=0)
    )
    for m in outer[:-1]:
        g3.far(m)
    g1.finish()
    g2.cur, g2.got = after_all((g2.cur, g2.got), *g1.got_ab1)
    g2.sides()
    small = g2.small + fswap(g2.small.astype(BF), masks[-1]).astype(F32)

    layout = row_layout(lengths[0], row_count, slot_count)
    cosine, sine = rotary_tables(layout[3])
    bias = jnp.where(allowed_pairs(layout, layout, BLOCK, slot_count), 0.0, NEGATIVE)
    normed, three, first4 = qkv(
        idx, after(tokens, *g2.ab), small, cosine, sine, g1.own + g1.other,
        maps_own + maps_core, fsdp, h,
    )
    first4 = first4.reshape(4, width, width)
    *g2.got_ab, g3.cur, g3.got = after_all((*g2.got_ab, g3.cur, g3.got), three)
    g2.cross()
    for m in outer[:-1]:
        g3.join()
    g3.near()
    mixed, probs = attend(after(three, *g2.ab1, g3.cur), bias)
    *g2.got_ab1, g3.got = after_all((*g2.got_ab1, g3.got), mixed)
    g2.finish()
    g3.sides()
    residual, hidden_in = branch(tokens, after(mixed, *g3.ab), first4, small)
    send_rs, keep_rs = (1, 3), (0, 2)
    act_s, slope_s, send3, up_s = up(
        idx, hidden_in, cotangent, small, g2.other, maps_core, send_rs, masks, fsdp, h
    )
    g3.got_ab = after_all(g3.got_ab, send3)
    g3.cross()
    act_k, slope_k, keep3, up_k = up(
        idx, after(hidden_in, *g3.ab1), cotangent, small, g2.own, maps_own, keep_rs, masks,
        fsdp, h,
    )
    g3.got_ab1 = after_all(g3.got_ab1, keep3)
    g3.finish()

    class Scatter:
        def __init__(self, send):
            self.got = dswap(send, 1)

        def sides(self, keep):
            got = self.got
            a = keep[1, 0] + got[1, 0]
            b = keep[:, 1, half:] + got[:, 1, half:]
            self.keep = (keep[0, 0] + got[0, 0], keep[:, 1, :half] + got[:, 1, :half])
            self.mid = [dswap(a, 2), fswap(b, masks[-1])]
            self.done = (a, b) + self.keep

        def cross(self):
            (a, b), (x, y) = self.keep, self.mid
            self.last = (a[:half] + x[:half], b[0] + y[0])
            out = (a[half:] + x[half:], b[1] + y[1])
            self.got_last = [fswap(out[0], masks[-1]), dswap(out[1], 2)]
            self.done = out + self.last

        def rows(self):
            (a, b), (x, y) = self.last, self.got_last
            return jnp.stack([a + x, b + y], axis=1)

    s3 = Scatter(send3)
    s3.sides(keep3)
    hidden_s, sums_s, send2, down_s = act_grad(
        idx, after(cotangent, *s3.done), hidden_in, up_s, slope_s, g3.other, maps_core, send_rs,
        masks, fsdp, h,
    )
    s2 = Scatter(send2)
    hidden_grad, sums_act, keep2, down_k = act_grad(
        idx, after(cotangent, send2), hidden_in, up_k, slope_k, g3.own, maps_own, keep_rs, masks,
        fsdp, h, (hidden_s, sums_s),
    )
    s2.sides(keep2)
    s3.mid = after_all(s3.mid, keep2)
    s3.cross()
    residual_grad, branch_grad, mixed_grad, sums_mid = middle(
        cotangent, after(hidden_grad, *s2.done, *s3.done), residual, small, first4
    )
    three_grad = attend_back(three, probs, mixed_grad, mixed, cosine, sine)
    s2.mid = after_all(s2.mid, three_grad)
    s2.cross()
    send1 = first_grad(
        idx, after(normed, *s2.done), mixed, three_grad, branch_grad, send_rs, masks, fsdp, h
    )
    s1 = Scatter(send1)
    s2.got_last = after_all(s2.got_last, send1)
    s3.got_last = after_all(s3.got_last, send1)
    rows23 = Inner(jnp.stack([s2.rows(), s3.rows()], axis=1))
    front = rows23.cur
    rows23.send()
    keep1 = first_grad(
        idx, after(normed, front), mixed, three_grad, branch_grad, keep_rs, masks, fsdp, h
    )
    s1.sides(keep1)
    rows23.add(*s1.done)
    rows23.sums()
    input_grad, sums_in = input_grads(
        after(tokens, *s1.done, rows23.cur if not rows23.left else front), three_grad, first4,
        small, residual_grad,
    )
    small_sum = sums_act + sums_mid + sums_in
    small_sum = small_sum + dswap(small_sum.astype(BF), 1).astype(F32)
    s1.mid = after_all(s1.mid, input_grad)
    s1.cross()
    rows23.cur = after(rows23.cur, *s1.done)
    rows23.spread()
    output = down_out(
        (act_s, act_k), (down_s, down_k), small, after(residual, rows23.total)
    )
    s1.got_last = after_all(s1.got_last, output)
    rows1 = Inner(s1.rows())
    m = 2
    while m < dp:
        small_sum = small_sum + dswap(small_sum.astype(BF), m).astype(F32)
        m *= 2
    for m in masks:
        small_sum = small_sum + fswap(small_sum.astype(BF), m).astype(F32)
    four23 = rows23.four(rows1.cur)
    rows1.sums()
    rows1.spread()
    four1 = rows1.four()

    def pick(four, d):
        return (
            lax.dynamic_index_in_dim(four, d4 ^ d, axis=0, keepdims=False)
            .reshape(R, width)
            .astype(F32)
        )

    first_grads = [pick(four1, d) for d in range(4)]
    up_grad = jnp.stack(
        [pick(four23[:, 0], d).reshape(R, fsdp, R) for d in range(4)], axis=2
    ).reshape(R, 4 * width)
    down_grad = jnp.concatenate([pick(four23[:, 1], d) for d in range(4)], axis=0)
    own = lax.dynamic_slice_in_dim(small_sum, me_f * R, R, axis=1)
    return (
        output,
        input_grad,
        own[0],
        own[1],
        first_grads[0],
        first_grads[1],
        first_grads[2],
        first_grads[3],
        own[2],
        own[3],
        up_grad,
        own[5:9].reshape(4 * R),
        down_grad,
        own[4],
    )


def solution(mesh):
    rows = P(("dp", "fsdp"), None)
    flat = P("fsdp")
    tall = P("fsdp", None)
    in_specs = (
        rows, rows, flat, flat, tall, tall, tall, tall, flat, flat, tall, flat, tall, flat, rows,
    )
    out_specs = (
        rows, rows, flat, flat, tall, tall, tall, tall, flat, flat, tall, flat, tall, flat,
    )
    return jax.shard_map(
        partial(local, mesh.shape["dp"], mesh.shape["fsdp"]),
        mesh=mesh,
        in_specs=in_specs,
        out_specs=out_specs,
        check_vma=False,
    )
```

```python
from functools import partial
import math

import jax
import jax.numpy as jnp
from jax import lax
from jax.experimental import pallas as pl
from jax.experimental.pallas import tpu as pltpu
from jax.sharding import PartitionSpec as P

H = 12
HD = 64
BLOCK = 16
EPSILON = 1e-05
BASE = 10000.0
NEGATIVE = -1e30
BF = jnp.bfloat16
F32 = jnp.float32
SMALL = 16
SPAN = 4.8e10
VMEM_LIMIT = 56 * 1024 * 1024


def row_layout(length_row, row_count, slot_count):
    doubled = 2 * length_row
    ends_at = jnp.cumsum(doubled, dtype=jnp.int32)
    starts_at = ends_at - doubled
    row_index = jnp.arange(row_count, dtype=jnp.int32)
    member = (row_index[:, None] >= starts_at[None, :]) & (row_index[:, None] < ends_at[None, :])
    slot_ids = jnp.arange(slot_count, dtype=jnp.int32)
    slot_index = jnp.sum(jnp.where(member, slot_ids[None, :], 0), axis=1, dtype=jnp.int32)
    start_row = jnp.sum(jnp.where(member, starts_at[None, :], 0), axis=1, dtype=jnp.int32)
    seq_length = jnp.sum(jnp.where(member, length_row[None, :], 0), axis=1, dtype=jnp.int32)
    local_row = row_index - start_row
    clean_flag = (local_row >= seq_length).astype(jnp.int32)
    position = local_row - clean_flag * seq_length
    return (row_index, slot_index, clean_flag, position)


def allowed_pairs(query_side, key_side, block_size, slot_count):
    query_row, query_slot, query_clean, query_pos = query_side
    key_row, key_slot, key_clean, key_pos = key_side
    query_block = query_pos // block_size
    key_block = key_pos // block_size
    same_seq = query_slot[:, None] == key_slot[None, :]
    key_noisy = key_clean[None, :] == 0
    key_plain = key_clean[None, :] == 1
    noisy_rule = key_noisy & (key_block[None, :] == query_block[:, None]) | key_plain & (
        key_block[None, :] < query_block[:, None]
    )
    clean_rule = key_plain & (key_block[None, :] <= query_block[:, None])
    rule_held = jnp.where(query_clean[:, None] == 1, clean_rule, noisy_rule)
    padded = query_slot == slot_count - 1
    real_pairs = same_seq & rule_held & jnp.logical_not(padded)[:, None]
    self_pairs = padded[:, None] & (query_row[:, None] == key_row[None, :])
    return real_pairs | self_pairs


def rotary_tables(position):
    half = HD // 2
    lane = jnp.arange(2 * HD, dtype=jnp.int32)
    freqs = jnp.exp((lane % half).astype(F32) * (-2.0 * math.log(BASE) / HD))
    angles = position.astype(F32)[:, None] * freqs[None, :]
    sign = jnp.where(lane % HD < half, -1.0, 1.0)
    return jnp.cos(angles), jnp.sin(angles) * sign[None, :]


def swap(values, axis, mask, size):
    return lax.ppermute(values, axis, [(i, i ^ mask) for i in range(size)])


def dot(a, b):
    return jnp.dot(a, b, preferred_element_type=F32)


def dot_nt(a, b):
    return lax.dot_general(a, b, (((1,), (1,)), ((), ())), preferred_element_type=F32)


def dot_tn(a, b):
    return lax.dot_general(a, b, (((0,), (0,)), ((), ())), preferred_element_type=F32)


def params(**more):
    return pltpu.CompilerParams(vmem_limit_bytes=VMEM_LIMIT, **more)


def cost(flops, moved):
    return pl.CostEstimate(flops=int(max(flops, SPAN)), bytes_accessed=int(moved), transcendentals=0)


def norm_parts(values):
    center = values - jnp.mean(values, axis=-1, keepdims=True)
    spread = jnp.mean(center * center, axis=-1, keepdims=True)
    inv = lax.rsqrt(spread + EPSILON)
    return center * inv, inv


def norm_back(grad, unit, inv, gain):
    scaled = grad * gain
    first = jnp.mean(scaled, axis=-1, keepdims=True)
    second = jnp.mean(scaled * unit, axis=-1, keepdims=True)
    return inv * (scaled - first - unit * second)


def turn(values, cosine, sine):
    half = HD // 2
    pair = 2 * HD
    lane = lax.broadcasted_iota(jnp.int32, (1, pair), 1)
    low = (lane % HD) < half
    parts = []
    for at in range(0, values.shape[1], pair):
        part = values[:, at : at + pair]
        other = jnp.where(low, pltpu.roll(part, pair - half, 1), pltpu.roll(part, half, 1))
        parts.append(part * cosine + other * sine)
    return parts[0] if len(parts) == 1 else jnp.concatenate(parts, axis=1)


def bits_of(index, masks):
    total = 0
    for bit, mask in enumerate(masks):
        if (index >> bit) & 1:
            total |= mask
    return total


def piece_map(which, masks):
    count = 1 << len(masks)
    half = count // 2
    kind, r, y = which
    if kind == "a":
        return [((i,), r, bits_of(i, masks), 0) for i in range(count)]
    return [
        ((x * half + i,), r | (2 * x), bits_of(i, masks) | y, 1)
        for x in range(2)
        for i in range(half)
    ]


def fetch(pieces, maps, me_f, h, w_ref, slot_of, sems):
    for ref, entries in zip(pieces, maps):
        for at, r, k, colour in entries:
            slot = slot_of(r)
            pltpu.make_async_copy(
                ref.at[at],
                w_ref.at[slot, me_f ^ k, pl.ds(colour * h, h)],
                sems.at[slot],
            ).start()


def fetched(w_ref, slot, sems):
    pltpu.make_async_copy(w_ref.at[slot], w_ref.at[slot], sems.at[slot]).wait()


def qkv_kernel(
    maps, h, idx_ref, x_ref, small_ref, cos_ref, sin_ref, p0, p1, p2, p3, p4, p5, p6, p7,
    normed_ref, out_ref, w_out, keep, w_ref, sems, out_sems,
):
    g = pl.program_id(0)
    d4, me_f = idx_ref[0], idx_ref[1]
    d = keep.shape[1]

    def send(slot):
        return pltpu.make_async_copy(w_ref.at[slot], w_out.at[slot], out_sems.at[slot])

    @pl.when(g == 0)
    def _():
        fetch((p0, p1, p2, p3, p4, p5, p6, p7), maps, me_f, h, w_ref, lambda r: d4 ^ r, sems)
        unit, _ = norm_parts(x_ref[...].astype(F32))
        normed = (unit * small_ref[0:1, :] + small_ref[1:2, :]).astype(BF)
        keep[...] = normed
        normed_ref[...] = normed

    fetched(w_ref, g, sems)
    send(g).start()

    @pl.when(g == 2)
    def _():
        fetched(w_ref, 3, sems)
        send(3).start()

    product = dot(keep[...], w_ref[g].reshape(d, d))

    @pl.when(g < 2)
    def _():
        out_ref[0] = turn(product, cos_ref[...], sin_ref[...]).astype(BF)

    @pl.when(g == 2)
    def _():
        out_ref[0] = product.astype(BF)
        for slot in range(4):
            send(slot).wait()


def qkv(idx, x, small, cosine, sine, pieces, maps, shards, h):
    n, d = x.shape
    return pl.pallas_call(
        partial(qkv_kernel, maps, h),
        grid=(3,),
        out_shape=(
            jax.ShapeDtypeStruct((n, d), BF),
            jax.ShapeDtypeStruct((3, n, d), BF),
            jax.ShapeDtypeStruct((4, shards, 2 * h, d), BF),
        ),
        in_specs=[
            pl.BlockSpec(memory_space=pltpu.SMEM),
            pl.BlockSpec((n, d), lambda g: (0, 0)),
            pl.BlockSpec(small.shape, lambda g: (0, 0)),
            pl.BlockSpec(cosine.shape, lambda g: (0, 0)),
            pl.BlockSpec(sine.shape, lambda g: (0, 0)),
        ]
        + [pl.BlockSpec(memory_space=pl.ANY)] * 8,
        out_specs=(
            pl.BlockSpec((n, d), lambda g: (0, 0)),
            pl.BlockSpec((1, n, d), lambda g: (g, 0, 0)),
            pl.BlockSpec(memory_space=pl.ANY),
        ),
        scratch_shapes=[
            pltpu.VMEM((n, d), BF),
            pltpu.VMEM((4, shards, 2 * h, d), BF),
            pltpu.SemaphoreType.DMA((4,)),
            pltpu.SemaphoreType.DMA((4,)),
        ],
        compiler_params=params(),
        cost_estimate=cost(6 * n * d * d, 2 * (5 * n * d + 8 * d * d)),
        name="qkv",
    )(idx, x, small, cosine, sine, *pieces)


def head_mask(which):
    lane = lax.broadcasted_iota(jnp.int32, (1, 2 * HD), 1)
    return (lane < HD) if which == 0 else (lane >= HD)


def attend_kernel(q_ref, k_ref, v_ref, bias_ref, mixed_ref, probs_ref):
    q, k, v = q_ref[0], k_ref[0], v_ref[0]
    zero = jnp.zeros((), BF)
    parts = []
    for h in range(2):
        own = jnp.where(head_mask(h), q, zero)
        scores = dot_nt(own, k) * (HD**-0.5) + bias_ref[...]
        top = jnp.max(scores, axis=1, keepdims=True)
        raised = jnp.exp(scores - top)
        total = jnp.sum(raised, axis=1, keepdims=True)
        probs = (raised * (1.0 / total)).astype(BF)
        probs_ref[h] = probs
        parts.append(dot(probs, v))
    mixed_ref[...] = jnp.where(head_mask(0), parts[0], parts[1]).astype(BF)


def attend(three, bias):
    _, n, d = three.shape
    pair = 2 * HD
    return pl.pallas_call(
        attend_kernel,
        grid=(d // pair,),
        out_shape=(
            jax.ShapeDtypeStruct((n, d), BF),
            jax.ShapeDtypeStruct((d // HD, n, n), BF),
        ),
        in_specs=[
            pl.BlockSpec((1, n, pair), lambda p: (0, 0, p)),
            pl.BlockSpec((1, n, pair), lambda p: (1, 0, p)),
            pl.BlockSpec((1, n, pair), lambda p: (2, 0, p)),
            pl.BlockSpec((n, n), lambda p: (0, 0)),
        ],
        out_specs=(
            pl.BlockSpec((n, pair), lambda p: (0, p)),
            pl.BlockSpec((2, n, n), lambda p: (p, 0, 0)),
        ),
        compiler_params=params(),
        cost_estimate=cost(8 * n * n * d, 2 * n * n * (d // HD) + 8 * n * d),
        name="attend",
    )(three, three, three, bias)


def attend_back_kernel(
    q_ref, k_ref, v_ref, probs_ref, grad_ref, mixed_ref, cos_ref, sin_ref, out_ref
):
    q, k, v, grad = q_ref[0], k_ref[0], v_ref[0], grad_ref[...]
    zero = jnp.zeros((), BF)
    product = grad.astype(F32) * mixed_ref[...].astype(F32)
    dq, dk, dv = [], [], []
    for h in range(2):
        mask = head_mask(h)
        inner = jnp.sum(jnp.where(mask, product, 0.0), axis=1, keepdims=True)
        probs = probs_ref[h]
        prob_grad = dot_nt(jnp.where(mask, grad, zero), v)
        score_grad = (probs.astype(F32) * (prob_grad - inner)).astype(BF)
        dq.append(dot(score_grad, k))
        dk.append(dot_tn(score_grad, q))
        dv.append(dot_tn(probs, grad))
    first = head_mask(0)
    scale = HD**-0.5
    cosine, sine = cos_ref[...], sin_ref[...]
    out_ref[0] = turn(jnp.where(first, dq[0], dq[1]) * scale, cosine, -sine).astype(BF)
    out_ref[1] = turn(jnp.where(first, dk[0], dk[1]) * scale, cosine, -sine).astype(BF)
    out_ref[2] = jnp.where(first, dv[0], dv[1]).astype(BF)


def attend_back(three, probs, grad, mixed, cosine, sine):
    _, n, d = three.shape
    pair = 2 * HD
    return pl.pallas_call(
        attend_back_kernel,
        grid=(d // pair,),
        out_shape=jax.ShapeDtypeStruct((3, n, d), BF),
        in_specs=[
            pl.BlockSpec((1, n, pair), lambda p: (0, 0, p)),
            pl.BlockSpec((1, n, pair), lambda p: (1, 0, p)),
            pl.BlockSpec((1, n, pair), lambda p: (2, 0, p)),
            pl.BlockSpec((2, n, n), lambda p: (p, 0, 0)),
            pl.BlockSpec((n, pair), lambda p: (0, p)),
            pl.BlockSpec((n, pair), lambda p: (0, p)),
            pl.BlockSpec(cosine.shape, lambda p: (0, 0)),
            pl.BlockSpec(sine.shape, lambda p: (0, 0)),
        ],
        out_specs=pl.BlockSpec((3, n, pair), lambda p: (0, 0, p)),
        compiler_params=params(),
        cost_estimate=cost(16 * n * n * d, 2 * n * n * (d // HD) + 16 * n * d),
        name="attend_back",
    )(three, three, three, probs, grad, mixed, cosine, sine)


def branch_kernel(x_ref, mixed_ref, w_ref, small_ref, residual_ref, hidden_ref):
    residual = x_ref[...].astype(F32) + dot(mixed_ref[...], w_ref[0])
    residual_ref[...] = residual
    unit, _ = norm_parts(residual)
    hidden_ref[...] = (unit * small_ref[2:3, :] + small_ref[3:4, :]).astype(BF)


def branch(x, mixed, weights, small):
    n, d = x.shape
    rows = n // 2
    return pl.pallas_call(
        branch_kernel,
        grid=(2,),
        out_shape=(jax.ShapeDtypeStruct((n, d), F32), jax.ShapeDtypeStruct((n, d), BF)),
        in_specs=[
            pl.BlockSpec((rows, d), lambda g: (g, 0)),
            pl.BlockSpec((rows, d), lambda g: (g, 0)),
            pl.BlockSpec((1, d, d), lambda g: (3, 0, 0)),
            pl.BlockSpec(small.shape, lambda g: (0, 0)),
        ],
        out_specs=(
            pl.BlockSpec((rows, d), lambda g: (g, 0)),
            pl.BlockSpec((rows, d), lambda g: (g, 0)),
        ),
        compiler_params=params(),
        cost_estimate=cost(2 * n * d * d, 10 * n * d + 2 * d * d),
        name="branch",
    )(x, mixed, weights, small)


def spread(out_ref, keep, product, me_f, masks, h, shards):
    keep[...] = product.astype(BF)
    for i in range(shards):
        j = me_f ^ bits_of(i, masks)
        for colour in range(2):
            start = pl.multiple_of(j * (2 * h) + colour * h, h & -h)
            out_ref[0, colour, i] = keep[pl.ds(start, h), :]


def up_kernel(
    masks, maps, rs, h, shards, idx_ref, hidden_ref, c_ref, small_ref, p0, p1, p2, p3,
    act_ref, slope_ref, grad_ref, w_out, w_ref, keep, sems, out_sems,
):
    g = pl.program_id(0)
    d4, me_f = idx_ref[0], idx_ref[1]
    d = hidden_ref.shape[1]

    def send(slot):
        return pltpu.make_async_copy(w_ref.at[slot], w_out.at[slot], out_sems.at[slot])

    @pl.when(g == 0)
    def _():
        fetch((p0, p1, p2, p3), maps, me_f, h, w_ref, rs.index, sems)

    fetched(w_ref, g, sems)
    send(g).start()
    chunk = d4 ^ jnp.where(g == 0, rs[0], rs[1])
    bias = small_ref[5:6, :]
    for other in range(1, 4):
        bias = jnp.where(chunk == other, small_ref[5 + other : 6 + other, :], bias)
    v = dot(hidden_ref[...], w_ref[g].reshape(d, d)) + bias
    c = math.sqrt(2.0 / math.pi)
    square = v * v
    t = jnp.tanh(v * (c + (c * 0.044715) * square))
    half = 0.5 * (1.0 + t)
    act = (v * half).astype(BF)
    act_ref[0] = act
    slope = half + (0.5 * v) * (1.0 - t * t) * (c + (3.0 * c * 0.044715) * square)
    slope_ref[0] = slope.astype(BF)
    spread(grad_ref, keep, dot_tn(act, c_ref[...]), me_f, masks, h, shards)

    @pl.when(g == 1)
    def _():
        send(0).wait()
        send(1).wait()


def up(idx, hidden, c, small, pieces, maps, rs, masks, shards, h):
    n, d = hidden.shape
    return pl.pallas_call(
        partial(up_kernel, masks, maps, rs, h, shards),
        grid=(2,),
        out_shape=(
            jax.ShapeDtypeStruct((2, n, d), BF),
            jax.ShapeDtypeStruct((2, n, d), BF),
            jax.ShapeDtypeStruct((2, 2, shards, h, d), BF),
            jax.ShapeDtypeStruct((2, shards, 2 * h, d), BF),
        ),
        in_specs=[
            pl.BlockSpec(memory_space=pltpu.SMEM),
            pl.BlockSpec((n, d), lambda g: (0, 0)),
            pl.BlockSpec((n, d), lambda g: (0, 0)),
            pl.BlockSpec(small.shape, lambda g: (0, 0)),
        ]
        + [pl.BlockSpec(memory_space=pl.ANY)] * 4,
        out_specs=(
            pl.BlockSpec((1, n, d), lambda g: (g, 0, 0)),
            pl.BlockSpec((1, n, d), lambda g: (g, 0, 0)),
            pl.BlockSpec((1, 2, shards, h, d), lambda g: (g, 0, 0, 0, 0)),
            pl.BlockSpec(memory_space=pl.ANY),
        ),
        scratch_shapes=[
            pltpu.VMEM((2, shards, 2 * h, d), BF),
            pltpu.VMEM((d, d), BF),
            pltpu.SemaphoreType.DMA((2,)),
            pltpu.SemaphoreType.DMA((2,)),
        ],
        compiler_params=params(),
        cost_estimate=cost(8 * n * d * d, 2 * (6 * n * d + 6 * d * d)),
        name="up",
    )(idx, hidden, c, small, *pieces)


def act_grad_kernel(
    masks, maps, rs, h, shards, first, idx_ref, c_ref, x_ref, up_ref, slope_ref, p0, p1, p2, p3,
    *more,
):
    if first:
        (hidden_ref, sums_ref, grad_ref, w_out, w_ref, keep, sems, out_sems) = more
    else:
        (
            hidden_in, sums_in, hidden_ref, sums_ref, grad_ref, w_out, w_ref, keep, sems, out_sems,
        ) = more
    g = pl.program_id(0)
    d4, me_f = idx_ref[0], idx_ref[1]
    d = x_ref.shape[1]
    c = c_ref[...]

    def send(slot):
        return pltpu.make_async_copy(w_ref.at[slot], w_out.at[slot], out_sems.at[slot])

    @pl.when(g == 0)
    def _():
        fetch((p0, p1, p2, p3), maps, me_f, h, w_ref, rs.index, sems)
        if first:
            hidden_ref[...] = jnp.zeros_like(hidden_ref)
            sums_ref[...] = jnp.zeros_like(sums_ref)
            sums_ref[4:5, :] = jnp.sum(c.astype(F32), axis=0, keepdims=True)
        else:
            hidden_ref[...] = hidden_in[...]
            sums_ref[...] = sums_in[...]

    fetched(w_ref, g, sems)
    send(g).start()
    chunk = d4 ^ jnp.where(g == 0, rs[0], rs[1])
    pre = (dot_nt(c, w_ref[g].reshape(d, d)) * slope_ref[0].astype(F32)).astype(BF)
    sums = jnp.sum(pre.astype(F32), axis=0, keepdims=True)
    row = lax.broadcasted_iota(jnp.int32, (sums_ref.shape[0], 1), 0)
    sums_ref[...] += jnp.where(row == 5 + chunk, sums, 0.0)
    hidden_ref[...] += dot_nt(pre, up_ref[0])
    spread(grad_ref, keep, dot_tn(x_ref[...], pre), me_f, masks, h, shards)

    @pl.when(g == 1)
    def _():
        send(0).wait()
        send(1).wait()


def act_grad(idx, c, hidden, up_half, slope, pieces, maps, rs, masks, shards, h, before=None):
    n, d = c.shape
    whole = pl.BlockSpec((n, d), lambda g: (0, 0))
    sums = pl.BlockSpec((SMALL, d), lambda g: (0, 0))
    return pl.pallas_call(
        partial(act_grad_kernel, masks, maps, rs, h, shards, before is None),
        grid=(2,),
        out_shape=(
            jax.ShapeDtypeStruct((n, d), F32),
            jax.ShapeDtypeStruct((SMALL, d), F32),
            jax.ShapeDtypeStruct((2, 2, shards, h, d), BF),
            jax.ShapeDtypeStruct((2, shards, 2 * h, d), BF),
        ),
        in_specs=[
            pl.BlockSpec(memory_space=pltpu.SMEM),
            whole,
            whole,
            pl.BlockSpec((1, d, d), lambda g: (g, 0, 0)),
            pl.BlockSpec((1, n, d), lambda g: (g, 0, 0)),
        ]
        + [pl.BlockSpec(memory_space=pl.ANY)] * 4
        + ([] if before is None else [whole, sums]),
        out_specs=(
            whole,
            sums,
            pl.BlockSpec((1, 2, shards, h, d), lambda g: (g, 0, 0, 0, 0)),
            pl.BlockSpec(memory_space=pl.ANY),
        ),
        scratch_shapes=[
            pltpu.VMEM((2, shards, 2 * h, d), BF),
            pltpu.VMEM((d, d), BF),
            pltpu.SemaphoreType.DMA((2,)),
            pltpu.SemaphoreType.DMA((2,)),
        ],
        compiler_params=params(),
        cost_estimate=cost(12 * n * d * d, 2 * (8 * n * d + 8 * d * d)),
        name="act_grad",
    )(idx, c, hidden, up_half.reshape(2, d, d), slope, *pieces, *(before or ()))


def first_grad_kernel(
    masks, h, shards, rs, idx_ref, normed_ref, mixed_ref, three_ref, branch_ref, out_ref, keep
):
    g = pl.program_id(0)
    last = (idx_ref[0] ^ jnp.where(g == 0, rs[0], rs[1])) == 3
    x = jnp.where(last, mixed_ref[...], normed_ref[...])
    y = jnp.where(last, branch_ref[...], three_ref[0])
    spread(out_ref, keep, dot_tn(x, y), idx_ref[1], masks, h, shards)


def first_grad(idx, normed, mixed, three_grad, branch_grad, rs, masks, shards, h):
    n, d = normed.shape

    def which(g, idx_ref):
        return jnp.minimum(idx_ref[0] ^ jnp.where(g == 0, rs[0], rs[1]), 2)

    whole = pl.BlockSpec((n, d), lambda g, i: (0, 0))
    return pl.pallas_call(
        partial(first_grad_kernel, masks, h, shards, rs),
        grid_spec=pltpu.PrefetchScalarGridSpec(
            num_scalar_prefetch=1,
            grid=(2,),
            in_specs=[
                whole,
                whole,
                pl.BlockSpec((1, n, d), lambda g, i: (which(g, i), 0, 0)),
                whole,
            ],
            out_specs=pl.BlockSpec((1, 2, shards, h, d), lambda g, i: (g, 0, 0, 0, 0)),
            scratch_shapes=[pltpu.VMEM((d, d), BF)],
        ),
        out_shape=jax.ShapeDtypeStruct((2, 2, shards, h, d), BF),
        compiler_params=params(),
        cost_estimate=cost(4 * n * d * d, 2 * (5 * n * d + 2 * d * d)),
        name="first_grad",
    )(idx, normed, mixed, three_grad, branch_grad)


def middle_kernel(
    c_ref, hidden_ref, residual_ref, small_ref, w_ref, grad_ref, low_ref, mixed_ref, sums_ref
):
    @pl.when(pl.program_id(0) == 0)
    def _():
        sums_ref[...] = jnp.zeros_like(sums_ref)

    grad = hidden_ref[...]
    unit, inv = norm_parts(residual_ref[...])
    sums_ref[2:3, :] += jnp.sum(grad * unit, axis=0, keepdims=True)
    sums_ref[3:4, :] += jnp.sum(grad, axis=0, keepdims=True)
    full = c_ref[...].astype(F32) + norm_back(grad, unit, inv, small_ref[2:3, :])
    grad_ref[...] = full
    low = full.astype(BF)
    low_ref[...] = low
    mixed_ref[...] = dot_nt(low, w_ref[0]).astype(BF)


def middle(c, hidden_grad, residual, small, weights):
    n, d = c.shape
    rows = n // 2
    return pl.pallas_call(
        middle_kernel,
        grid=(2,),
        out_shape=(
            jax.ShapeDtypeStruct((n, d), F32),
            jax.ShapeDtypeStruct((n, d), BF),
            jax.ShapeDtypeStruct((n, d), BF),
            jax.ShapeDtypeStruct((SMALL, d), F32),
        ),
        in_specs=[
            pl.BlockSpec((rows, d), lambda g: (g, 0)),
            pl.BlockSpec((rows, d), lambda g: (g, 0)),
            pl.BlockSpec((rows, d), lambda g: (g, 0)),
            pl.BlockSpec(small.shape, lambda g: (0, 0)),
            pl.BlockSpec((1, d, d), lambda g: (3, 0, 0)),
        ],
        out_specs=(
            pl.BlockSpec((rows, d), lambda g: (g, 0)),
            pl.BlockSpec((rows, d), lambda g: (g, 0)),
            pl.BlockSpec((rows, d), lambda g: (g, 0)),
            pl.BlockSpec((SMALL, d), lambda g: (0, 0)),
        ),
        compiler_params=params(),
        cost_estimate=cost(2 * n * d * d, 18 * n * d + 2 * d * d),
        name="middle",
    )(c, hidden_grad, residual, small, weights)


def input_kernel(x_ref, three_ref, w_ref, small_ref, grad_ref, out_ref, sums_ref, total):
    g = pl.program_id(0)
    part = dot_nt(three_ref[0], w_ref[0])

    @pl.when(g == 0)
    def _():
        total[...] = part

    @pl.when(g > 0)
    def _():
        total[...] += part

    @pl.when(g == 2)
    def _():
        grad = total[...]
        unit, inv = norm_parts(x_ref[...].astype(F32))
        sums_ref[...] = jnp.zeros_like(sums_ref)
        sums_ref[0:1, :] = jnp.sum(grad * unit, axis=0, keepdims=True)
        sums_ref[1:2, :] = jnp.sum(grad, axis=0, keepdims=True)
        out_ref[...] = grad_ref[...] + norm_back(grad, unit, inv, small_ref[0:1, :])


def input_grads(x, three_grad, weights, small, residual_grad):
    n, d = x.shape
    return pl.pallas_call(
        input_kernel,
        grid=(3,),
        out_shape=(jax.ShapeDtypeStruct((n, d), F32), jax.ShapeDtypeStruct((SMALL, d), F32)),
        in_specs=[
            pl.BlockSpec((n, d), lambda g: (0, 0)),
            pl.BlockSpec((1, n, d), lambda g: (g, 0, 0)),
            pl.BlockSpec((1, d, d), lambda g: (g, 0, 0)),
            pl.BlockSpec(small.shape, lambda g: (0, 0)),
            pl.BlockSpec((n, d), lambda g: (0, 0)),
        ],
        out_specs=(
            pl.BlockSpec((n, d), lambda g: (0, 0)),
            pl.BlockSpec((SMALL, d), lambda g: (0, 0)),
        ),
        scratch_shapes=[pltpu.VMEM((n, d), F32)],
        compiler_params=params(),
        cost_estimate=cost(6 * n * d * d, 16 * n * d + 6 * d * d),
        name="input_grads",
    )(x, three_grad, weights, small, residual_grad)


def down_kernel(a0_ref, a1_ref, w0_ref, w1_ref, small_ref, residual_ref, out_ref, total):
    g = pl.program_id(0)
    part = dot(a0_ref[0], w0_ref[0]) + dot(a1_ref[0], w1_ref[0])

    @pl.when(g == 0)
    def _():
        total[...] = residual_ref[...] + small_ref[4:5, :] + part

    @pl.when(g == 1)
    def _():
        out_ref[...] = (total[...] + part).astype(BF)


def down_out(acts, weights, small, residual):
    n, d = residual.shape
    return pl.pallas_call(
        down_kernel,
        grid=(2,),
        out_shape=jax.ShapeDtypeStruct((n, d), BF),
        in_specs=[
            pl.BlockSpec((1, n, d), lambda g: (g, 0, 0)),
            pl.BlockSpec((1, n, d), lambda g: (g, 0, 0)),
            pl.BlockSpec((1, d, d), lambda g: (g, 0, 0)),
            pl.BlockSpec((1, d, d), lambda g: (g, 0, 0)),
            pl.BlockSpec(small.shape, lambda g: (0, 0)),
            pl.BlockSpec((n, d), lambda g: (0, 0)),
        ],
        out_specs=pl.BlockSpec((n, d), lambda g: (0, 0)),
        scratch_shapes=[pltpu.VMEM((n, d), F32)],
        compiler_params=params(),
        cost_estimate=cost(8 * n * d * d, 14 * n * d + 8 * d * d),
        name="down_out",
    )(*acts, *(w.reshape(2, d, d) for w in weights), small, residual)


def local(dp, fsdp, tokens, lengths, *rest):
    (
        norm1_gain,
        norm1_bias,
        query_weight,
        key_weight,
        value_weight,
        output_weight,
        norm2_gain,
        norm2_bias,
        up_weight,
        up_bias,
        down_weight,
        down_bias,
        cotangent,
    ) = rest
    row_count, width = tokens.shape
    slot_count = lengths.shape[1]
    R = width // fsdp
    h = R // 2
    me_dp = lax.axis_index("dp").astype(jnp.int32)
    me_f = lax.axis_index("fsdp").astype(jnp.int32)
    d4 = me_dp % 4
    idx = jnp.stack([d4, me_f])
    masks = []
    mask = fsdp // 2
    while mask >= 1:
        masks.append(mask)
        mask //= 2
    masks = tuple(masks)
    outer = masks[:-1]

    def fswap(v, m):
        return swap(v, "fsdp", m, fsdp)

    def dswap(v, m):
        return swap(v, "dp", m, dp)

    def after(value, *tokens):
        return lax.optimization_barrier((value,) + tokens)[0]

    def after_all(values, *tokens):
        values = tuple(values)
        return list(lax.optimization_barrier(values + tokens)[: len(values)])

    half = fsdp // 2
    maps_own = [
        piece_map(w, masks) for w in (("a", 0, 0), ("a", 2, 0), ("b", 0, 0), ("b", 0, 1))
    ]
    maps_core = [
        piece_map(w, masks) for w in (("a", 1, 0), ("a", 3, 0), ("b", 1, 0), ("b", 1, 1))
    ]

    class Gather:
        def __init__(self, piece):
            self.cur = piece[None]

        def far(self, m):
            self.got = fswap(self.cur, m)

        def join(self):
            self.cur = jnp.concatenate([self.cur, self.got], axis=0)

        def near(self):
            self.got = fswap(self.cur, outer[-1])

        def sides(self):
            a = jnp.concatenate([self.cur[:, :h], self.got[:, :h]], axis=0)
            b = jnp.concatenate([self.cur[:, h:R], self.got[:, h:R]], axis=0)
            self.ab = (a, b)
            self.got_ab = (fswap(a, masks[-1]), dswap(b, 2))

        def cross(self):
            a1 = jnp.concatenate([self.ab[0], self.got_ab[0]], axis=0)
            b1 = jnp.concatenate([self.ab[1], self.got_ab[1]], axis=0)
            self.ab1 = (a1, b1)
            self.got_ab1 = (dswap(a1, 2), fswap(b1, masks[-1]))
            self.core = [dswap(a1, 1), dswap(b1, 1)]

        def finish(self):
            a_x, b_y = self.got_ab1
            a1, b1 = self.ab1
            self.own = [a1, a_x, b1, b_y]
            self.other = [self.core[0], dswap(a_x, 1), self.core[1], dswap(b_y, 1)]

    class Inner:
        def __init__(self, cur):
            self.cur = cur
            self.got = None
            self.left = list(reversed(outer))

        def step(self, *tokens):
            if self.got is not None:
                self.cur = self.cur + after(self.got, *tokens)
                self.got = None
            if self.left:
                count = self.cur.shape[0] // 2
                front = self.cur[count:]
                self.got = fswap(front, self.left.pop(0))
                self.cur = self.cur[:count]
                return front
            return self.cur

        def sums(self):
            while self.got is not None or self.left:
                self.step()
            return self.cur[0]

    class Spread:
        def __init__(self, total):
            m = 4
            while m < dp:
                total = total + dswap(total, m)
                m *= 2
            self.total = total
            self.pair = dswap(total, 2)
            self.core = dswap(total, 1)

        def four(self, *tokens):
            pair = after(self.pair, *tokens)
            return jnp.stack([self.total, self.core, pair, dswap(pair, 1)])

    piece1 = lax.select_n(d4, query_weight, key_weight, value_weight, output_weight)
    g1 = Gather(piece1)
    for m in outer[:-1]:
        g1.far(m)
        g1.join()
    g1_first = g1.cur
    g1.near()
    vectors = after_all(
        (norm1_gain, norm1_bias, norm2_gain, norm2_bias, down_bias, up_bias, up_weight), piece1
    )
    tall = jnp.concatenate(vectors[:6]).reshape(9, R)
    lane = jnp.arange(width, dtype=jnp.int32) // R
    tall = jnp.where((lane == me_f)[None, :], jnp.tile(tall, (1, fsdp)), jnp.zeros((), BF))
    tall = jnp.pad(tall, ((0, SMALL - 9), (0, 0)))
    fronts = []
    for m in reversed(masks):
        if len(fronts) == 1:
            tall = after(tall, g1.got)
        fronts.append(tall)
        tall = tall + fswap(tall, m)
    small = tall.astype(F32)
    piece2 = lax.dynamic_index_in_dim(
        vectors[6].reshape(R, fsdp, 4, R), d4, axis=2, keepdims=False
    ).reshape(R, width)
    g2 = Gather(after(piece2, g1.got, *fronts[2:]))
    for m in outer[:-1]:
        g2.far(m)
        g2.join()
    g1.sides()
    g2.cur, g2.got = after_all((g2.cur, g2.got), *g1.ab)
    g2.near()
    g1.cross()
    early = outer[:-1]
    g3 = Gather(
        lax.dynamic_slice_in_dim(after(down_weight, g2.cur), d4 * R, R, axis=0)
    )
    for m in early[:-1]:
        g3.far(m)
        g3.join()
    g3.far(early[-1])
    g1.finish()
    g2.cur, g2.got = after_all((g2.cur, g2.got), *g1.got_ab1)
    g2.sides()
    g3.join()
    g3.near()

    layout = row_layout(after(lengths, g1_first)[0], row_count, slot_count)
    cosine, sine = rotary_tables(layout[3])
    bias = jnp.where(allowed_pairs(layout, layout, BLOCK, slot_count), 0.0, NEGATIVE)
    normed, three, first4 = qkv(
        idx, after(tokens, *g2.ab, g3.cur, bias), small, cosine, sine, g1.own + g1.other,
        maps_own + maps_core, fsdp, h,
    )
    first4 = first4.reshape(4, width, width)
    g2.got_ab = after_all(g2.got_ab, three)
    g2.cross()
    mixed, probs = attend(after(three, *g2.ab1), bias)
    g2.got_ab1 = after_all(g2.got_ab1, mixed)
    g2.finish()
    g3.cur, g3.got = after_all((g3.cur, g3.got), mixed)
    g3.sides()
    residual, hidden_in = branch(tokens, after(mixed, *g2.got_ab1, *g2.core, *g3.ab), first4, small)
    g3.got_ab = after_all(g3.got_ab, hidden_in)
    g3.cross()
    send_rs, keep_rs = (1, 3), (0, 2)
    act_s, slope_s, send3, up_s = up(
        idx, after(hidden_in, *g3.ab1), cotangent, small, g2.other, maps_core, send_rs, masks,
        fsdp, h,
    )
    act_k, slope_k, keep3, up_k = up(
        idx, after(hidden_in, send3), cotangent, small, g2.own, maps_own, keep_rs, masks, fsdp, h,
    )
    g3.got_ab1 = after_all(g3.got_ab1, keep3)
    g3.finish()

    class Scatter:
        def __init__(self, send):
            self.got = dswap(send, 1)

        def sides(self, keep):
            got = self.got
            a = keep[1, 0] + got[1, 0]
            b = keep[:, 1, half:] + got[:, 1, half:]
            self.keep = (keep[0, 0] + got[0, 0], keep[:, 1, :half] + got[:, 1, :half])
            self.mid = [dswap(a, 2), fswap(b, masks[-1])]
            self.done = (a, b) + self.keep

        def cross(self):
            (a, b), (x, y) = self.keep, self.mid
            self.last = (a[:half] + x[:half], b[0] + y[0])
            out = (a[half:] + x[half:], b[1] + y[1])
            self.got_last = [fswap(out[0], masks[-1]), dswap(out[1], 2)]
            self.done = out + self.last

        def rows(self):
            (a, b), (x, y) = self.last, self.got_last
            return jnp.stack([a + x, b + y], axis=1)

    s3 = Scatter(send3)
    s3.sides(keep3)
    hidden_s, sums_s, send2, down_s = act_grad(
        idx, after(cotangent, *s3.done), hidden_in, up_s, slope_s, g3.other, maps_core, send_rs,
        masks, fsdp, h,
    )
    s2 = Scatter(send2)
    s3.mid = after_all(s3.mid, send2)
    s3.cross()
    hidden_grad, sums_act, keep2, down_k = act_grad(
        idx, after(cotangent, send2, *s3.done), hidden_in, up_k, slope_k, g3.own, maps_own,
        keep_rs, masks, fsdp, h, (hidden_s, sums_s),
    )
    s2.sides(keep2)
    s3.got_last = after_all(s3.got_last, keep2)
    rows3 = Inner(s3.rows())
    front = rows3.step()
    residual_grad, branch_grad, mixed_grad, sums_mid = middle(
        cotangent, after(hidden_grad, *s2.done, front), residual, small, first4
    )
    front = rows3.step(mixed_grad)
    three_grad = attend_back(three, probs, after(mixed_grad, front), mixed, cosine, sine)
    s2.mid = after_all(s2.mid, three_grad)
    s2.cross()
    front = rows3.step(three_grad)
    send1 = first_grad(
        idx, after(normed, *s2.done, front), mixed, three_grad, branch_grad, send_rs, masks, fsdp,
        h,
    )
    s1 = Scatter(send1)
    s2.got_last = after_all(s2.got_last, send1)
    rows2 = Inner(s2.rows())
    front = rows2.step()
    keep1 = first_grad(
        idx, after(normed, front, send1), mixed, three_grad, branch_grad, keep_rs, masks, fsdp, h
    )
    s1.sides(keep1)
    front = rows2.step(*s1.done)
    input_grad, sums_in = input_grads(
        after(tokens, *s1.done, front), three_grad, first4, small, residual_grad
    )
    front = rows2.step(input_grad)
    small_sum = sums_act + sums_mid + sums_in

    def small_step(swapper, m, *tokens):
        low = after(small_sum.astype(BF), *tokens)
        return low, swapper(low, m)

    low, small_got = small_step(dswap, 1)
    output = down_out(
        (act_s, act_k), (down_s, down_k), small, after(residual, front, low)
    )
    s1.mid = after_all(s1.mid, output)
    s1.cross()
    both = Spread(after(jnp.stack([rows2.sums(), rows3.sums()]), *s1.done))
    rest = [(fswap, m) for m in reversed(masks)]
    m = 2
    while m < dp:
        rest.append((dswap, m))
        m *= 2
    small_sum = small_sum + after(small_got, output).astype(F32)
    low, small_got = small_step(*rest.pop(), *s1.done)
    rows1 = Inner(s1.rows())
    small_sum = small_sum + after(small_got, rows1.cur).astype(F32)
    front = rows1.step()
    low, small_got = small_step(*rest.pop(), front)
    both.pair = after(both.pair, rows1.cur)
    front = rows1.step(low)
    small_sum = small_sum + after(small_got, front).astype(F32)
    low, small_got = small_step(*rest.pop(), front)
    four23 = both.four(front)

    def pick(four, d):
        return (
            lax.dynamic_index_in_dim(four, d4 ^ d, axis=0, keepdims=False)
            .reshape(R, width)
            .astype(F32)
        )

    up_grad = jnp.stack(
        [pick(four23[:, 0], d).reshape(R, fsdp, R) for d in range(4)], axis=2
    ).reshape(R, 4 * width)
    if rows1.got is not None:
        rows1.got = after(rows1.got, up_grad)
    one = Spread(rows1.sums())
    small_sum = small_sum + after(small_got, one.total).astype(F32)
    while rest:
        low, small_got = small_step(*rest.pop(), one.total)
        small_sum = small_sum + small_got.astype(F32)
    four23 = after(four23, one.total)
    down_grad = jnp.concatenate([pick(four23[:, 1], d) for d in range(4)], axis=0)
    four1 = one.four(down_grad)
    first_grads = [pick(four1, d) for d in range(4)]
    own = lax.dynamic_slice_in_dim(small_sum, me_f * R, R, axis=1)
    return (
        output,
        input_grad,
        own[0],
        own[1],
        first_grads[0],
        first_grads[1],
        first_grads[2],
        first_grads[3],
        own[2],
        own[3],
        up_grad,
        own[5:9].reshape(4 * R),
        down_grad,
        own[4],
    )


def solution(mesh):
    rows = P(("dp", "fsdp"), None)
    flat = P("fsdp")
    tall = P("fsdp", None)
    in_specs = (
        rows, rows, flat, flat, tall, tall, tall, tall, flat, flat, tall, flat, tall, flat, rows,
    )
    out_specs = (
        rows, rows, flat, flat, tall, tall, tall, tall, flat, flat, tall, flat, tall, flat,
    )
    return jax.shard_map(
        partial(local, mesh.shape["dp"], mesh.shape["fsdp"]),
        mesh=mesh,
        in_specs=in_specs,
        out_specs=out_specs,
        check_vma=False,
    )
```

```python
from functools import partial
import math

import jax
import jax.numpy as jnp
from jax import lax
from jax.experimental import pallas as pl
from jax.experimental.pallas import tpu as pltpu
from jax.sharding import PartitionSpec as P

H = 12
HD = 64
BLOCK = 16
EPSILON = 1e-05
BASE = 10000.0
NEGATIVE = -1e30
BF = jnp.bfloat16
F32 = jnp.float32
SMALL = 16
SPAN = 4.8e10
VMEM_LIMIT = 56 * 1024 * 1024


def row_layout(length_row, row_count, slot_count):
    doubled = 2 * length_row
    ends_at = jnp.cumsum(doubled, dtype=jnp.int32)
    starts_at = ends_at - doubled
    row_index = jnp.arange(row_count, dtype=jnp.int32)
    member = (row_index[:, None] >= starts_at[None, :]) & (row_index[:, None] < ends_at[None, :])
    slot_ids = jnp.arange(slot_count, dtype=jnp.int32)
    slot_index = jnp.sum(jnp.where(member, slot_ids[None, :], 0), axis=1, dtype=jnp.int32)
    start_row = jnp.sum(jnp.where(member, starts_at[None, :], 0), axis=1, dtype=jnp.int32)
    seq_length = jnp.sum(jnp.where(member, length_row[None, :], 0), axis=1, dtype=jnp.int32)
    local_row = row_index - start_row
    clean_flag = (local_row >= seq_length).astype(jnp.int32)
    position = local_row - clean_flag * seq_length
    return (row_index, slot_index, clean_flag, position)


def allowed_pairs(query_side, key_side, block_size, slot_count):
    query_row, query_slot, query_clean, query_pos = query_side
    key_row, key_slot, key_clean, key_pos = key_side
    query_block = query_pos // block_size
    key_block = key_pos // block_size
    same_seq = query_slot[:, None] == key_slot[None, :]
    key_noisy = key_clean[None, :] == 0
    key_plain = key_clean[None, :] == 1
    noisy_rule = key_noisy & (key_block[None, :] == query_block[:, None]) | key_plain & (
        key_block[None, :] < query_block[:, None]
    )
    clean_rule = key_plain & (key_block[None, :] <= query_block[:, None])
    rule_held = jnp.where(query_clean[:, None] == 1, clean_rule, noisy_rule)
    padded = query_slot == slot_count - 1
    real_pairs = same_seq & rule_held & jnp.logical_not(padded)[:, None]
    self_pairs = padded[:, None] & (query_row[:, None] == key_row[None, :])
    return real_pairs | self_pairs


def rotary_tables(position):
    half = HD // 2
    lane = jnp.arange(2 * HD, dtype=jnp.int32)
    freqs = jnp.exp((lane % half).astype(F32) * (-2.0 * math.log(BASE) / HD))
    angles = position.astype(F32)[:, None] * freqs[None, :]
    sign = jnp.where(lane % HD < half, -1.0, 1.0)
    return jnp.cos(angles), jnp.sin(angles) * sign[None, :]


def swap(values, axis, mask, size):
    return lax.ppermute(values, axis, [(i, i ^ mask) for i in range(size)])


def dot(a, b):
    return jnp.dot(a, b, preferred_element_type=F32)


def dot_nt(a, b):
    return lax.dot_general(a, b, (((1,), (1,)), ((), ())), preferred_element_type=F32)


def dot_tn(a, b):
    return lax.dot_general(a, b, (((0,), (0,)), ((), ())), preferred_element_type=F32)


def params(**more):
    return pltpu.CompilerParams(vmem_limit_bytes=VMEM_LIMIT, **more)


def cost(flops, moved):
    return pl.CostEstimate(flops=int(max(flops, SPAN)), bytes_accessed=int(moved), transcendentals=0)


def norm_parts(values):
    center = values - jnp.mean(values, axis=-1, keepdims=True)
    spread = jnp.mean(center * center, axis=-1, keepdims=True)
    inv = lax.rsqrt(spread + EPSILON)
    return center * inv, inv


def norm_back(grad, unit, inv, gain):
    scaled = grad * gain
    first = jnp.mean(scaled, axis=-1, keepdims=True)
    second = jnp.mean(scaled * unit, axis=-1, keepdims=True)
    return inv * (scaled - first - unit * second)


def turn(values, cosine, sine):
    half = HD // 2
    pair = 2 * HD
    lane = lax.broadcasted_iota(jnp.int32, (1, pair), 1)
    low = (lane % HD) < half
    parts = []
    for at in range(0, values.shape[1], pair):
        part = values[:, at : at + pair]
        other = jnp.where(low, pltpu.roll(part, pair - half, 1), pltpu.roll(part, half, 1))
        parts.append(part * cosine + other * sine)
    return parts[0] if len(parts) == 1 else jnp.concatenate(parts, axis=1)


def bits_of(index, masks):
    total = 0
    for bit, mask in enumerate(masks):
        if (index >> bit) & 1:
            total |= mask
    return total


def piece_map(which, masks):
    count = 1 << len(masks)
    half = count // 2
    kind, r, y = which
    if kind == "a":
        return [((i,), r, bits_of(i, masks), 0) for i in range(count)]
    return [
        ((x * half + i,), r | (2 * x), bits_of(i, masks) | y, 1)
        for x in range(2)
        for i in range(half)
    ]


def fetch(pieces, maps, me_f, h, w_ref, slot_of, sems):
    for ref, entries in zip(pieces, maps):
        for at, r, k, colour in entries:
            slot = slot_of(r)
            pltpu.make_async_copy(
                ref.at[at],
                w_ref.at[slot, me_f ^ k, pl.ds(colour * h, h)],
                sems.at[slot],
            ).start()


def fetched(w_ref, slot, sems):
    pltpu.make_async_copy(w_ref.at[slot], w_ref.at[slot], sems.at[slot]).wait()


def qkv_kernel(
    maps, h, idx_ref, x_ref, small_ref, cos_ref, sin_ref, p0, p1, p2, p3, p4, p5, p6, p7,
    normed_ref, out_ref, w_out, keep, w_ref, sems, out_sems,
):
    g = pl.program_id(0)
    d4, me_f = idx_ref[0], idx_ref[1]
    d = keep.shape[1]

    def send(slot):
        return pltpu.make_async_copy(w_ref.at[slot], w_out.at[slot], out_sems.at[slot])

    @pl.when(g == 0)
    def _():
        fetch((p0, p1, p2, p3, p4, p5, p6, p7), maps, me_f, h, w_ref, lambda r: d4 ^ r, sems)
        unit, _ = norm_parts(x_ref[...].astype(F32))
        normed = (unit * small_ref[0:1, :] + small_ref[1:2, :]).astype(BF)
        keep[...] = normed
        normed_ref[...] = normed

    fetched(w_ref, g, sems)
    send(g).start()

    @pl.when(g == 2)
    def _():
        fetched(w_ref, 3, sems)
        send(3).start()

    product = dot(keep[...], w_ref[g].reshape(d, d))

    @pl.when(g < 2)
    def _():
        out_ref[0] = turn(product, cos_ref[...], sin_ref[...]).astype(BF)

    @pl.when(g == 2)
    def _():
        out_ref[0] = product.astype(BF)
        for slot in range(4):
            send(slot).wait()


def qkv(idx, x, small, cosine, sine, pieces, maps, shards, h):
    n, d = x.shape
    return pl.pallas_call(
        partial(qkv_kernel, maps, h),
        grid=(3,),
        out_shape=(
            jax.ShapeDtypeStruct((n, d), BF),
            jax.ShapeDtypeStruct((3, n, d), BF),
            jax.ShapeDtypeStruct((4, shards, 2 * h, d), BF),
        ),
        in_specs=[
            pl.BlockSpec(memory_space=pltpu.SMEM),
            pl.BlockSpec((n, d), lambda g: (0, 0)),
            pl.BlockSpec(small.shape, lambda g: (0, 0)),
            pl.BlockSpec(cosine.shape, lambda g: (0, 0)),
            pl.BlockSpec(sine.shape, lambda g: (0, 0)),
        ]
        + [pl.BlockSpec(memory_space=pl.ANY)] * 8,
        out_specs=(
            pl.BlockSpec((n, d), lambda g: (0, 0)),
            pl.BlockSpec((1, n, d), lambda g: (g, 0, 0)),
            pl.BlockSpec(memory_space=pl.ANY),
        ),
        scratch_shapes=[
            pltpu.VMEM((n, d), BF),
            pltpu.VMEM((4, shards, 2 * h, d), BF),
            pltpu.SemaphoreType.DMA((4,)),
            pltpu.SemaphoreType.DMA((4,)),
        ],
        compiler_params=params(),
        cost_estimate=cost(6 * n * d * d, 2 * (5 * n * d + 8 * d * d)),
        name="qkv",
    )(idx, x, small, cosine, sine, *pieces)


def head_mask(which):
    lane = lax.broadcasted_iota(jnp.int32, (1, 2 * HD), 1)
    return (lane < HD) if which == 0 else (lane >= HD)


def attend_kernel(q_ref, k_ref, v_ref, bias_ref, mixed_ref, probs_ref):
    q, k, v = q_ref[0], k_ref[0], v_ref[0]
    zero = jnp.zeros((), BF)
    parts = []
    for h in range(2):
        own = jnp.where(head_mask(h), q, zero)
        scores = dot_nt(own, k) * (HD**-0.5) + bias_ref[...]
        top = jnp.max(scores, axis=1, keepdims=True)
        raised = jnp.exp(scores - top)
        total = jnp.sum(raised, axis=1, keepdims=True)
        probs = (raised * (1.0 / total)).astype(BF)
        probs_ref[h] = probs
        parts.append(dot(probs, v))
    mixed_ref[...] = jnp.where(head_mask(0), parts[0], parts[1]).astype(BF)


def attend(three, bias):
    _, n, d = three.shape
    pair = 2 * HD
    return pl.pallas_call(
        attend_kernel,
        grid=(d // pair,),
        out_shape=(
            jax.ShapeDtypeStruct((n, d), BF),
            jax.ShapeDtypeStruct((d // HD, n, n), BF),
        ),
        in_specs=[
            pl.BlockSpec((1, n, pair), lambda p: (0, 0, p)),
            pl.BlockSpec((1, n, pair), lambda p: (1, 0, p)),
            pl.BlockSpec((1, n, pair), lambda p: (2, 0, p)),
            pl.BlockSpec((n, n), lambda p: (0, 0)),
        ],
        out_specs=(
            pl.BlockSpec((n, pair), lambda p: (0, p)),
            pl.BlockSpec((2, n, n), lambda p: (p, 0, 0)),
        ),
        compiler_params=params(),
        cost_estimate=cost(8 * n * n * d, 2 * n * n * (d // HD) + 8 * n * d),
        name="attend",
    )(three, three, three, bias)


def attend_back_kernel(
    q_ref, k_ref, v_ref, probs_ref, grad_ref, mixed_ref, cos_ref, sin_ref, out_ref
):
    q, k, v, grad = q_ref[0], k_ref[0], v_ref[0], grad_ref[...]
    zero = jnp.zeros((), BF)
    product = grad.astype(F32) * mixed_ref[...].astype(F32)
    dq, dk, dv = [], [], []
    for h in range(2):
        mask = head_mask(h)
        inner = jnp.sum(jnp.where(mask, product, 0.0), axis=1, keepdims=True)
        probs = probs_ref[h]
        prob_grad = dot_nt(jnp.where(mask, grad, zero), v)
        score_grad = (probs.astype(F32) * (prob_grad - inner)).astype(BF)
        dq.append(dot(score_grad, k))
        dk.append(dot_tn(score_grad, q))
        dv.append(dot_tn(probs, grad))
    first = head_mask(0)
    scale = HD**-0.5
    cosine, sine = cos_ref[...], sin_ref[...]
    out_ref[0] = turn(jnp.where(first, dq[0], dq[1]) * scale, cosine, -sine).astype(BF)
    out_ref[1] = turn(jnp.where(first, dk[0], dk[1]) * scale, cosine, -sine).astype(BF)
    out_ref[2] = jnp.where(first, dv[0], dv[1]).astype(BF)


def attend_back(three, probs, grad, mixed, cosine, sine):
    _, n, d = three.shape
    pair = 2 * HD
    return pl.pallas_call(
        attend_back_kernel,
        grid=(d // pair,),
        out_shape=jax.ShapeDtypeStruct((3, n, d), BF),
        in_specs=[
            pl.BlockSpec((1, n, pair), lambda p: (0, 0, p)),
            pl.BlockSpec((1, n, pair), lambda p: (1, 0, p)),
            pl.BlockSpec((1, n, pair), lambda p: (2, 0, p)),
            pl.BlockSpec((2, n, n), lambda p: (p, 0, 0)),
            pl.BlockSpec((n, pair), lambda p: (0, p)),
            pl.BlockSpec((n, pair), lambda p: (0, p)),
            pl.BlockSpec(cosine.shape, lambda p: (0, 0)),
            pl.BlockSpec(sine.shape, lambda p: (0, 0)),
        ],
        out_specs=pl.BlockSpec((3, n, pair), lambda p: (0, 0, p)),
        compiler_params=params(),
        cost_estimate=cost(16 * n * n * d, 2 * n * n * (d // HD) + 16 * n * d),
        name="attend_back",
    )(three, three, three, probs, grad, mixed, cosine, sine)


def branch_kernel(x_ref, mixed_ref, w_ref, small_ref, residual_ref, hidden_ref):
    residual = x_ref[...].astype(F32) + dot(mixed_ref[...], w_ref[0])
    residual_ref[...] = residual
    unit, _ = norm_parts(residual)
    hidden_ref[...] = (unit * small_ref[2:3, :] + small_ref[3:4, :]).astype(BF)


def branch(x, mixed, weights, small):
    n, d = x.shape
    rows = n // 2
    return pl.pallas_call(
        branch_kernel,
        grid=(2,),
        out_shape=(jax.ShapeDtypeStruct((n, d), F32), jax.ShapeDtypeStruct((n, d), BF)),
        in_specs=[
            pl.BlockSpec((rows, d), lambda g: (g, 0)),
            pl.BlockSpec((rows, d), lambda g: (g, 0)),
            pl.BlockSpec((1, d, d), lambda g: (3, 0, 0)),
            pl.BlockSpec(small.shape, lambda g: (0, 0)),
        ],
        out_specs=(
            pl.BlockSpec((rows, d), lambda g: (g, 0)),
            pl.BlockSpec((rows, d), lambda g: (g, 0)),
        ),
        compiler_params=params(),
        cost_estimate=cost(2 * n * d * d, 10 * n * d + 2 * d * d),
        name="branch",
    )(x, mixed, weights, small)


def spread(out_ref, keep, product, me_f, masks, h, shards):
    keep[...] = product.astype(BF)
    for i in range(shards):
        j = me_f ^ bits_of(i, masks)
        for colour in range(2):
            start = pl.multiple_of(j * (2 * h) + colour * h, h & -h)
            out_ref[0, colour, i] = keep[pl.ds(start, h), :]


def up_kernel(
    masks, maps, rs, h, shards, idx_ref, hidden_ref, c_ref, small_ref, p0, p1, p2, p3,
    act_ref, slope_ref, grad_ref, w_out, w_ref, keep, sems, out_sems,
):
    g = pl.program_id(0)
    d4, me_f = idx_ref[0], idx_ref[1]
    d = hidden_ref.shape[1]

    def send(slot):
        return pltpu.make_async_copy(w_ref.at[slot], w_out.at[slot], out_sems.at[slot])

    @pl.when(g == 0)
    def _():
        fetch((p0, p1, p2, p3), maps, me_f, h, w_ref, rs.index, sems)

    fetched(w_ref, g, sems)
    send(g).start()
    chunk = d4 ^ jnp.where(g == 0, rs[0], rs[1])
    bias = small_ref[5:6, :]
    for other in range(1, 4):
        bias = jnp.where(chunk == other, small_ref[5 + other : 6 + other, :], bias)
    v = dot(hidden_ref[...], w_ref[g].reshape(d, d)) + bias
    c = math.sqrt(2.0 / math.pi)
    square = v * v
    t = jnp.tanh(v * (c + (c * 0.044715) * square))
    half = 0.5 * (1.0 + t)
    act = (v * half).astype(BF)
    act_ref[0] = act
    slope = half + (0.5 * v) * (1.0 - t * t) * (c + (3.0 * c * 0.044715) * square)
    slope_ref[0] = slope.astype(BF)
    spread(grad_ref, keep, dot_tn(act, c_ref[...]), me_f, masks, h, shards)

    @pl.when(g == 1)
    def _():
        send(0).wait()
        send(1).wait()


def up(idx, hidden, c, small, pieces, maps, rs, masks, shards, h):
    n, d = hidden.shape
    return pl.pallas_call(
        partial(up_kernel, masks, maps, rs, h, shards),
        grid=(2,),
        out_shape=(
            jax.ShapeDtypeStruct((2, n, d), BF),
            jax.ShapeDtypeStruct((2, n, d), BF),
            jax.ShapeDtypeStruct((2, 2, shards, h, d), BF),
            jax.ShapeDtypeStruct((2, shards, 2 * h, d), BF),
        ),
        in_specs=[
            pl.BlockSpec(memory_space=pltpu.SMEM),
            pl.BlockSpec((n, d), lambda g: (0, 0)),
            pl.BlockSpec((n, d), lambda g: (0, 0)),
            pl.BlockSpec(small.shape, lambda g: (0, 0)),
        ]
        + [pl.BlockSpec(memory_space=pl.ANY)] * 4,
        out_specs=(
            pl.BlockSpec((1, n, d), lambda g: (g, 0, 0)),
            pl.BlockSpec((1, n, d), lambda g: (g, 0, 0)),
            pl.BlockSpec((1, 2, shards, h, d), lambda g: (g, 0, 0, 0, 0)),
            pl.BlockSpec(memory_space=pl.ANY),
        ),
        scratch_shapes=[
            pltpu.VMEM((2, shards, 2 * h, d), BF),
            pltpu.VMEM((d, d), BF),
            pltpu.SemaphoreType.DMA((2,)),
            pltpu.SemaphoreType.DMA((2,)),
        ],
        compiler_params=params(),
        cost_estimate=cost(8 * n * d * d, 2 * (6 * n * d + 6 * d * d)),
        name="up",
    )(idx, hidden, c, small, *pieces)


def act_grad_kernel(
    masks, maps, rs, h, shards, first, idx_ref, c_ref, x_ref, up_ref, slope_ref, p0, p1, p2, p3,
    *more,
):
    if first:
        (hidden_ref, sums_ref, grad_ref, w_out, w_ref, keep, sems, out_sems) = more
    else:
        (
            hidden_in, sums_in, hidden_ref, sums_ref, grad_ref, w_out, w_ref, keep, sems, out_sems,
        ) = more
    g = pl.program_id(0)
    d4, me_f = idx_ref[0], idx_ref[1]
    d = x_ref.shape[1]
    c = c_ref[...]

    def send(slot):
        return pltpu.make_async_copy(w_ref.at[slot], w_out.at[slot], out_sems.at[slot])

    @pl.when(g == 0)
    def _():
        fetch((p0, p1, p2, p3), maps, me_f, h, w_ref, rs.index, sems)
        if first:
            hidden_ref[...] = jnp.zeros_like(hidden_ref)
            sums_ref[...] = jnp.zeros_like(sums_ref)
            sums_ref[4:5, :] = jnp.sum(c.astype(F32), axis=0, keepdims=True)
        else:
            hidden_ref[...] = hidden_in[...]
            sums_ref[...] = sums_in[...]

    fetched(w_ref, g, sems)
    send(g).start()
    chunk = d4 ^ jnp.where(g == 0, rs[0], rs[1])
    pre = (dot_nt(c, w_ref[g].reshape(d, d)) * slope_ref[0].astype(F32)).astype(BF)
    sums = jnp.sum(pre.astype(F32), axis=0, keepdims=True)
    row = lax.broadcasted_iota(jnp.int32, (sums_ref.shape[0], 1), 0)
    sums_ref[...] += jnp.where(row == 5 + chunk, sums, 0.0)
    hidden_ref[...] += dot_nt(pre, up_ref[0])
    spread(grad_ref, keep, dot_tn(x_ref[...], pre), me_f, masks, h, shards)

    @pl.when(g == 1)
    def _():
        send(0).wait()
        send(1).wait()


def act_grad(idx, c, hidden, up_half, slope, pieces, maps, rs, masks, shards, h, before=None):
    n, d = c.shape
    whole = pl.BlockSpec((n, d), lambda g: (0, 0))
    sums = pl.BlockSpec((SMALL, d), lambda g: (0, 0))
    return pl.pallas_call(
        partial(act_grad_kernel, masks, maps, rs, h, shards, before is None),
        grid=(2,),
        out_shape=(
            jax.ShapeDtypeStruct((n, d), F32),
            jax.ShapeDtypeStruct((SMALL, d), F32),
            jax.ShapeDtypeStruct((2, 2, shards, h, d), BF),
            jax.ShapeDtypeStruct((2, shards, 2 * h, d), BF),
        ),
        in_specs=[
            pl.BlockSpec(memory_space=pltpu.SMEM),
            whole,
            whole,
            pl.BlockSpec((1, d, d), lambda g: (g, 0, 0)),
            pl.BlockSpec((1, n, d), lambda g: (g, 0, 0)),
        ]
        + [pl.BlockSpec(memory_space=pl.ANY)] * 4
        + ([] if before is None else [whole, sums]),
        out_specs=(
            whole,
            sums,
            pl.BlockSpec((1, 2, shards, h, d), lambda g: (g, 0, 0, 0, 0)),
            pl.BlockSpec(memory_space=pl.ANY),
        ),
        scratch_shapes=[
            pltpu.VMEM((2, shards, 2 * h, d), BF),
            pltpu.VMEM((d, d), BF),
            pltpu.SemaphoreType.DMA((2,)),
            pltpu.SemaphoreType.DMA((2,)),
        ],
        compiler_params=params(),
        cost_estimate=cost(12 * n * d * d, 2 * (8 * n * d + 8 * d * d)),
        name="act_grad",
    )(idx, c, hidden, up_half.reshape(2, d, d), slope, *pieces, *(before or ()))


def first_grad_kernel(
    masks, h, shards, rs, idx_ref, normed_ref, mixed_ref, three_ref, branch_ref, out_ref, keep
):
    g = pl.program_id(0)
    last = (idx_ref[0] ^ jnp.where(g == 0, rs[0], rs[1])) == 3
    x = jnp.where(last, mixed_ref[...], normed_ref[...])
    y = jnp.where(last, branch_ref[...], three_ref[0])
    spread(out_ref, keep, dot_tn(x, y), idx_ref[1], masks, h, shards)


def first_grad(idx, normed, mixed, three_grad, branch_grad, rs, masks, shards, h):
    n, d = normed.shape

    def which(g, idx_ref):
        return jnp.minimum(idx_ref[0] ^ jnp.where(g == 0, rs[0], rs[1]), 2)

    whole = pl.BlockSpec((n, d), lambda g, i: (0, 0))
    return pl.pallas_call(
        partial(first_grad_kernel, masks, h, shards, rs),
        grid_spec=pltpu.PrefetchScalarGridSpec(
            num_scalar_prefetch=1,
            grid=(2,),
            in_specs=[
                whole,
                whole,
                pl.BlockSpec((1, n, d), lambda g, i: (which(g, i), 0, 0)),
                whole,
            ],
            out_specs=pl.BlockSpec((1, 2, shards, h, d), lambda g, i: (g, 0, 0, 0, 0)),
            scratch_shapes=[pltpu.VMEM((d, d), BF)],
        ),
        out_shape=jax.ShapeDtypeStruct((2, 2, shards, h, d), BF),
        compiler_params=params(),
        cost_estimate=cost(4 * n * d * d, 2 * (5 * n * d + 2 * d * d)),
        name="first_grad",
    )(idx, normed, mixed, three_grad, branch_grad)


def middle_kernel(
    c_ref, hidden_ref, residual_ref, small_ref, w_ref, grad_ref, low_ref, mixed_ref, sums_ref
):
    @pl.when(pl.program_id(0) == 0)
    def _():
        sums_ref[...] = jnp.zeros_like(sums_ref)

    grad = hidden_ref[...]
    unit, inv = norm_parts(residual_ref[...])
    sums_ref[2:3, :] += jnp.sum(grad * unit, axis=0, keepdims=True)
    sums_ref[3:4, :] += jnp.sum(grad, axis=0, keepdims=True)
    full = c_ref[...].astype(F32) + norm_back(grad, unit, inv, small_ref[2:3, :])
    grad_ref[...] = full
    low = full.astype(BF)
    low_ref[...] = low
    mixed_ref[...] = dot_nt(low, w_ref[0]).astype(BF)


def middle(c, hidden_grad, residual, small, weights):
    n, d = c.shape
    rows = n // 2
    return pl.pallas_call(
        middle_kernel,
        grid=(2,),
        out_shape=(
            jax.ShapeDtypeStruct((n, d), F32),
            jax.ShapeDtypeStruct((n, d), BF),
            jax.ShapeDtypeStruct((n, d), BF),
            jax.ShapeDtypeStruct((SMALL, d), F32),
        ),
        in_specs=[
            pl.BlockSpec((rows, d), lambda g: (g, 0)),
            pl.BlockSpec((rows, d), lambda g: (g, 0)),
            pl.BlockSpec((rows, d), lambda g: (g, 0)),
            pl.BlockSpec(small.shape, lambda g: (0, 0)),
            pl.BlockSpec((1, d, d), lambda g: (3, 0, 0)),
        ],
        out_specs=(
            pl.BlockSpec((rows, d), lambda g: (g, 0)),
            pl.BlockSpec((rows, d), lambda g: (g, 0)),
            pl.BlockSpec((rows, d), lambda g: (g, 0)),
            pl.BlockSpec((SMALL, d), lambda g: (0, 0)),
        ),
        compiler_params=params(),
        cost_estimate=cost(2 * n * d * d, 18 * n * d + 2 * d * d),
        name="middle",
    )(c, hidden_grad, residual, small, weights)


def input_kernel(x_ref, three_ref, w_ref, small_ref, grad_ref, out_ref, sums_ref, total):
    g = pl.program_id(0)
    part = dot_nt(three_ref[0], w_ref[0])

    @pl.when(g == 0)
    def _():
        total[...] = part

    @pl.when(g > 0)
    def _():
        total[...] += part

    @pl.when(g == 2)
    def _():
        grad = total[...]
        unit, inv = norm_parts(x_ref[...].astype(F32))
        sums_ref[...] = jnp.zeros_like(sums_ref)
        sums_ref[0:1, :] = jnp.sum(grad * unit, axis=0, keepdims=True)
        sums_ref[1:2, :] = jnp.sum(grad, axis=0, keepdims=True)
        out_ref[...] = grad_ref[...] + norm_back(grad, unit, inv, small_ref[0:1, :])


def input_grads(x, three_grad, weights, small, residual_grad):
    n, d = x.shape
    return pl.pallas_call(
        input_kernel,
        grid=(3,),
        out_shape=(jax.ShapeDtypeStruct((n, d), F32), jax.ShapeDtypeStruct((SMALL, d), F32)),
        in_specs=[
            pl.BlockSpec((n, d), lambda g: (0, 0)),
            pl.BlockSpec((1, n, d), lambda g: (g, 0, 0)),
            pl.BlockSpec((1, d, d), lambda g: (g, 0, 0)),
            pl.BlockSpec(small.shape, lambda g: (0, 0)),
            pl.BlockSpec((n, d), lambda g: (0, 0)),
        ],
        out_specs=(
            pl.BlockSpec((n, d), lambda g: (0, 0)),
            pl.BlockSpec((SMALL, d), lambda g: (0, 0)),
        ),
        scratch_shapes=[pltpu.VMEM((n, d), F32)],
        compiler_params=params(),
        cost_estimate=cost(6 * n * d * d, 16 * n * d + 6 * d * d),
        name="input_grads",
    )(x, three_grad, weights, small, residual_grad)


def down_kernel(a0_ref, a1_ref, w0_ref, w1_ref, small_ref, residual_ref, out_ref, total):
    g = pl.program_id(0)
    part = dot(a0_ref[0], w0_ref[0]) + dot(a1_ref[0], w1_ref[0])

    @pl.when(g == 0)
    def _():
        total[...] = residual_ref[...] + small_ref[4:5, :] + part

    @pl.when(g == 1)
    def _():
        out_ref[...] = (total[...] + part).astype(BF)


def down_out(acts, weights, small, residual):
    n, d = residual.shape
    return pl.pallas_call(
        down_kernel,
        grid=(2,),
        out_shape=jax.ShapeDtypeStruct((n, d), BF),
        in_specs=[
            pl.BlockSpec((1, n, d), lambda g: (g, 0, 0)),
            pl.BlockSpec((1, n, d), lambda g: (g, 0, 0)),
            pl.BlockSpec((1, d, d), lambda g: (g, 0, 0)),
            pl.BlockSpec((1, d, d), lambda g: (g, 0, 0)),
            pl.BlockSpec(small.shape, lambda g: (0, 0)),
            pl.BlockSpec((n, d), lambda g: (0, 0)),
        ],
        out_specs=pl.BlockSpec((n, d), lambda g: (0, 0)),
        scratch_shapes=[pltpu.VMEM((n, d), F32)],
        compiler_params=params(),
        cost_estimate=cost(8 * n * d * d, 14 * n * d + 8 * d * d),
        name="down_out",
    )(*acts, *(w.reshape(2, d, d) for w in weights), small, residual)


def last_kernel(shards, idx_ref, p0, p1, p2, p3, up_ref, down_ref, keep):
    _, rows, d = keep.shape
    for r, ref in enumerate((p0, p1, p2, p3)):
        at = idx_ref[0] ^ r
        keep[at] = ref[0].reshape(rows, d).astype(F32)
        down_ref[pl.ds(pl.multiple_of(at * rows, 8), rows), :] = ref[1].reshape(rows, d).astype(F32)
    for i in range(shards):
        part = [keep[chunk, :, i * rows : (i + 1) * rows] for chunk in range(4)]
        up_ref[:, 4 * rows * i : 4 * rows * (i + 1)] = jnp.concatenate(part, axis=1)


def last_out(idx, pieces, shards):
    d = pieces[0].shape[-1]
    rows = d // shards
    vmem = pl.BlockSpec(memory_space=pltpu.VMEM)
    return pl.pallas_call(
        partial(last_kernel, shards),
        out_shape=(
            jax.ShapeDtypeStruct((rows, 4 * d), F32),
            jax.ShapeDtypeStruct((4 * rows, d), F32),
        ),
        in_specs=[pl.BlockSpec(memory_space=pltpu.SMEM)] + [vmem] * 4,
        out_specs=(vmem, vmem),
        scratch_shapes=[pltpu.VMEM((4, rows, d), F32)],
        compiler_params=params(),
        name="last_out",
    )(idx, *pieces)


def local(dp, fsdp, tokens, lengths, *rest):
    (
        norm1_gain,
        norm1_bias,
        query_weight,
        key_weight,
        value_weight,
        output_weight,
        norm2_gain,
        norm2_bias,
        up_weight,
        up_bias,
        down_weight,
        down_bias,
        cotangent,
    ) = rest
    row_count, width = tokens.shape
    slot_count = lengths.shape[1]
    R = width // fsdp
    h = R // 2
    me_dp = lax.axis_index("dp").astype(jnp.int32)
    me_f = lax.axis_index("fsdp").astype(jnp.int32)
    d4 = me_dp % 4
    idx = jnp.stack([d4, me_f])
    masks = []
    mask = fsdp // 2
    while mask >= 1:
        masks.append(mask)
        mask //= 2
    masks = tuple(masks)
    outer = masks[:-1]

    def fswap(v, m):
        return swap(v, "fsdp", m, fsdp)

    def dswap(v, m):
        return swap(v, "dp", m, dp)

    def after(value, *tokens):
        return lax.optimization_barrier((value,) + tokens)[0]

    def after_all(values, *tokens):
        values = tuple(values)
        return list(lax.optimization_barrier(values + tokens)[: len(values)])

    half = fsdp // 2
    maps_own = [
        piece_map(w, masks) for w in (("a", 0, 0), ("a", 2, 0), ("b", 0, 0), ("b", 0, 1))
    ]
    maps_core = [
        piece_map(w, masks) for w in (("a", 1, 0), ("a", 3, 0), ("b", 1, 0), ("b", 1, 1))
    ]

    class Gather:
        def __init__(self, piece):
            self.cur = piece[None]

        def far(self, m):
            self.got = fswap(self.cur, m)

        def join(self):
            self.cur = jnp.concatenate([self.cur, self.got], axis=0)

        def near(self):
            self.got = fswap(self.cur, outer[-1])

        def sides(self):
            a = jnp.concatenate([self.cur[:, :h], self.got[:, :h]], axis=0)
            b = jnp.concatenate([self.cur[:, h:R], self.got[:, h:R]], axis=0)
            self.ab = (a, b)
            self.got_ab = (fswap(a, masks[-1]), dswap(b, 2))

        def cross(self):
            a1 = jnp.concatenate([self.ab[0], self.got_ab[0]], axis=0)
            b1 = jnp.concatenate([self.ab[1], self.got_ab[1]], axis=0)
            self.ab1 = (a1, b1)
            self.got_ab1 = (dswap(a1, 2), fswap(b1, masks[-1]))
            self.core = [dswap(a1, 1), dswap(b1, 1)]

        def finish(self):
            a_x, b_y = self.got_ab1
            a1, b1 = self.ab1
            self.own = [a1, a_x, b1, b_y]
            self.other = [self.core[0], dswap(a_x, 1), self.core[1], dswap(b_y, 1)]

    class Inner:
        def __init__(self, cur):
            self.cur = cur
            self.got = None
            self.left = list(reversed(outer))

        def step(self, *tokens):
            if self.got is not None:
                self.cur = self.cur + after(self.got, *tokens)
                self.got = None
            if self.left:
                count = self.cur.shape[0] // 2
                front = self.cur[count:]
                self.got = fswap(front, self.left.pop(0))
                self.cur = self.cur[:count]
                return front
            return self.cur

        def sums(self):
            while self.got is not None or self.left:
                self.step()
            return self.cur[0]

    class Spread:
        def __init__(self, total):
            m = 4
            while m < dp:
                total = total + dswap(total, m)
                m *= 2
            self.total = total
            self.pair = dswap(total, 2)
            self.core = dswap(total, 1)

        def four(self, *tokens):
            pair = after(self.pair, *tokens)
            return [self.total, self.core, pair, dswap(pair, 1)]

    piece1 = lax.select_n(d4, query_weight, key_weight, value_weight, output_weight)
    g1 = Gather(piece1)
    for m in outer[:-1]:
        g1.far(m)
        g1.join()
    g1_first = g1.cur
    g1.near()
    vectors = after_all(
        (norm1_gain, norm1_bias, norm2_gain, norm2_bias, down_bias, up_bias, up_weight), piece1
    )
    tall = jnp.concatenate(vectors[:6]).reshape(9, R)
    lane = jnp.arange(width, dtype=jnp.int32) // R
    tall = jnp.where((lane == me_f)[None, :], jnp.tile(tall, (1, fsdp)), jnp.zeros((), BF))
    tall = jnp.pad(tall, ((0, SMALL - 9), (0, 0)))
    fronts = []
    for m in reversed(masks):
        if len(fronts) == 1:
            tall = after(tall, g1.got)
        fronts.append(tall)
        tall = tall + fswap(tall, m)
    small = tall.astype(F32)
    piece2 = lax.dynamic_index_in_dim(
        vectors[6].reshape(R, fsdp, 4, R), d4, axis=2, keepdims=False
    ).reshape(R, width)
    g2 = Gather(after(piece2, g1.got, *fronts[2:]))
    for m in outer[:-1]:
        g2.far(m)
        g2.join()
    g1.sides()
    g2.cur, g2.got = after_all((g2.cur, g2.got), *g1.ab)
    g2.near()
    g1.cross()
    early = outer[:-1]
    g3 = Gather(
        lax.dynamic_slice_in_dim(after(down_weight, g2.cur), d4 * R, R, axis=0)
    )
    for m in early[:-1]:
        g3.far(m)
        g3.join()
    g3.far(early[-1])
    g1.finish()
    g2.cur, g2.got = after_all((g2.cur, g2.got), *g1.got_ab1)
    g2.sides()
    g3.join()
    g3.near()

    layout = row_layout(after(lengths, g1_first)[0], row_count, slot_count)
    cosine, sine = rotary_tables(layout[3])
    bias = jnp.where(allowed_pairs(layout, layout, BLOCK, slot_count), 0.0, NEGATIVE)
    normed, three, first4 = qkv(
        idx, after(tokens, *g2.ab, g3.cur, bias), small, cosine, sine, g1.own + g1.other,
        maps_own + maps_core, fsdp, h,
    )
    first4 = first4.reshape(4, width, width)
    g2.got_ab = after_all(g2.got_ab, three)
    g2.cross()
    mixed, probs = attend(after(three, *g2.ab1), bias)
    g2.got_ab1 = after_all(g2.got_ab1, mixed)
    g2.finish()
    g3.cur, g3.got = after_all((g3.cur, g3.got), mixed)
    g3.sides()
    residual, hidden_in = branch(tokens, after(mixed, *g2.got_ab1, *g2.core, *g3.ab), first4, small)
    g3.got_ab = after_all(g3.got_ab, hidden_in)
    g3.cross()
    send_rs, keep_rs = (1, 3), (0, 2)
    act_s, slope_s, send3, up_s = up(
        idx, after(hidden_in, *g3.ab1), cotangent, small, g2.other, maps_core, send_rs, masks,
        fsdp, h,
    )
    act_k, slope_k, keep3, up_k = up(
        idx, after(hidden_in, send3), cotangent, small, g2.own, maps_own, keep_rs, masks, fsdp, h,
    )
    g3.got_ab1 = after_all(g3.got_ab1, keep3)
    g3.finish()

    class Scatter:
        def __init__(self, send):
            self.got = dswap(send, 1)

        def sides(self, keep):
            got = self.got
            a = keep[1, 0] + got[1, 0]
            b = keep[:, 1, half:] + got[:, 1, half:]
            self.keep = (keep[0, 0] + got[0, 0], keep[:, 1, :half] + got[:, 1, :half])
            self.mid = [dswap(a, 2), fswap(b, masks[-1])]
            self.done = (a, b) + self.keep

        def cross(self):
            (a, b), (x, y) = self.keep, self.mid
            self.last = (a[:half] + x[:half], b[0] + y[0])
            out = (a[half:] + x[half:], b[1] + y[1])
            self.got_last = [fswap(out[0], masks[-1]), dswap(out[1], 2)]
            self.done = out + self.last

        def rows(self):
            (a, b), (x, y) = self.last, self.got_last
            return jnp.stack([a + x, b + y], axis=1)

    s3 = Scatter(send3)
    s3.sides(keep3)
    hidden_s, sums_s, send2, down_s = act_grad(
        idx, after(cotangent, *s3.done), hidden_in, up_s, slope_s, g3.other, maps_core, send_rs,
        masks, fsdp, h,
    )
    s2 = Scatter(send2)
    s3.mid = after_all(s3.mid, send2)
    s3.cross()
    hidden_grad, sums_act, keep2, down_k = act_grad(
        idx, after(cotangent, send2, *s3.done), hidden_in, up_k, slope_k, g3.own, maps_own,
        keep_rs, masks, fsdp, h, (hidden_s, sums_s),
    )
    s2.sides(keep2)
    s3.got_last = after_all(s3.got_last, keep2)
    rows3 = Inner(s3.rows())
    front = rows3.step()
    residual_grad, branch_grad, mixed_grad, sums_mid = middle(
        cotangent, after(hidden_grad, *s2.done, front), residual, small, first4
    )
    front = rows3.step(mixed_grad)
    three_grad = attend_back(three, probs, after(mixed_grad, front), mixed, cosine, sine)
    s2.mid = after_all(s2.mid, three_grad)
    s2.cross()
    front = rows3.step(three_grad)
    send1 = first_grad(
        idx, after(normed, *s2.done, front), mixed, three_grad, branch_grad, send_rs, masks, fsdp,
        h,
    )
    s1 = Scatter(send1)
    s2.got_last = after_all(s2.got_last, send1)
    rows2 = Inner(s2.rows())
    front = rows2.step()
    keep1 = first_grad(
        idx, after(normed, front, send1), mixed, three_grad, branch_grad, keep_rs, masks, fsdp, h
    )
    s1.sides(keep1)
    front = rows2.step(*s1.done)
    input_grad, sums_in = input_grads(
        after(tokens, *s1.done, front), three_grad, first4, small, residual_grad
    )
    front = rows2.step(input_grad)
    small_sum = sums_act + sums_mid + sums_in

    def small_step(swapper, m, *tokens):
        low = after(small_sum.astype(BF), *tokens)
        return low, swapper(low, m)

    low, small_got = small_step(dswap, 1)
    output = down_out(
        (act_s, act_k), (down_s, down_k), small, after(residual, front, low)
    )
    s1.mid = after_all(s1.mid, output)
    s1.cross()
    both = Spread(after(jnp.stack([rows2.sums(), rows3.sums()]), *s1.done))
    rest = [(fswap, m) for m in reversed(masks)]
    m = 2
    while m < dp:
        rest.append((dswap, m))
        m *= 2
    small_sum = small_sum + after(small_got, output).astype(F32)
    low, small_got = small_step(*rest.pop(), *s1.done)
    rows1 = Inner(s1.rows())
    small_sum = small_sum + after(small_got, rows1.cur).astype(F32)
    front = rows1.step()
    low, small_got = small_step(*rest.pop(), front)
    both.pair = after(both.pair, rows1.cur)
    front = rows1.step(low)
    small_sum = small_sum + after(small_got, front).astype(F32)
    low, small_got = small_step(*rest.pop(), front)
    four23 = both.four(front)

    up_grad, down_grad = last_out(idx, four23, fsdp)
    if rows1.got is not None:
        rows1.got = after(rows1.got, up_grad)
    one = Spread(rows1.sums())
    small_sum = small_sum + after(small_got, one.total).astype(F32)
    while rest:
        low, small_got = small_step(*rest.pop(), one.total)
        small_sum = small_sum + small_got.astype(F32)
    four1 = jnp.stack(one.four())
    first_grads = [
        lax.dynamic_index_in_dim(four1, d4 ^ d, axis=0, keepdims=False)
        .reshape(R, width)
        .astype(F32)
        for d in range(4)
    ]
    own = lax.dynamic_slice_in_dim(small_sum, me_f * R, R, axis=1)
    return (
        output,
        input_grad,
        own[0],
        own[1],
        first_grads[0],
        first_grads[1],
        first_grads[2],
        first_grads[3],
        own[2],
        own[3],
        up_grad,
        own[5:9].reshape(4 * R),
        down_grad,
        own[4],
    )


def solution(mesh):
    rows = P(("dp", "fsdp"), None)
    flat = P("fsdp")
    tall = P("fsdp", None)
    in_specs = (
        rows, rows, flat, flat, tall, tall, tall, tall, flat, flat, tall, flat, tall, flat, rows,
    )
    out_specs = (
        rows, rows, flat, flat, tall, tall, tall, tall, flat, flat, tall, flat, tall, flat,
    )
    return jax.shard_map(
        partial(local, mesh.shape["dp"], mesh.shape["fsdp"]),
        mesh=mesh,
        in_specs=in_specs,
        out_specs=out_specs,
        check_vma=False,
    )
```

```python
from functools import partial
import math

import jax
import jax.numpy as jnp
from jax import lax
from jax.experimental import pallas as pl
from jax.experimental.pallas import tpu as pltpu
from jax.sharding import PartitionSpec as P

H = 12
HD = 64
BLOCK = 16
EPSILON = 1e-05
BASE = 10000.0
NEGATIVE = -1e30
BF = jnp.bfloat16
F32 = jnp.float32
SMALL = 16
SPAN = 4.8e10
VMEM_LIMIT = 16 * 1024 * 1024


def row_layout(length_row, row_count, slot_count):
    doubled = 2 * length_row
    ends_at = jnp.cumsum(doubled, dtype=jnp.int32)
    starts_at = ends_at - doubled
    row_index = jnp.arange(row_count, dtype=jnp.int32)
    member = (row_index[:, None] >= starts_at[None, :]) & (row_index[:, None] < ends_at[None, :])
    slot_ids = jnp.arange(slot_count, dtype=jnp.int32)
    slot_index = jnp.sum(jnp.where(member, slot_ids[None, :], 0), axis=1, dtype=jnp.int32)
    start_row = jnp.sum(jnp.where(member, starts_at[None, :], 0), axis=1, dtype=jnp.int32)
    seq_length = jnp.sum(jnp.where(member, length_row[None, :], 0), axis=1, dtype=jnp.int32)
    local_row = row_index - start_row
    clean_flag = (local_row >= seq_length).astype(jnp.int32)
    position = local_row - clean_flag * seq_length
    return (row_index, slot_index, clean_flag, position)


def allowed_pairs(query_side, key_side, block_size, slot_count):
    query_row, query_slot, query_clean, query_pos = query_side
    key_row, key_slot, key_clean, key_pos = key_side
    query_block = query_pos // block_size
    key_block = key_pos // block_size
    same_seq = query_slot[:, None] == key_slot[None, :]
    key_noisy = key_clean[None, :] == 0
    key_plain = key_clean[None, :] == 1
    noisy_rule = key_noisy & (key_block[None, :] == query_block[:, None]) | key_plain & (
        key_block[None, :] < query_block[:, None]
    )
    clean_rule = key_plain & (key_block[None, :] <= query_block[:, None])
    rule_held = jnp.where(query_clean[:, None] == 1, clean_rule, noisy_rule)
    padded = query_slot == slot_count - 1
    real_pairs = same_seq & rule_held & jnp.logical_not(padded)[:, None]
    self_pairs = padded[:, None] & (query_row[:, None] == key_row[None, :])
    return real_pairs | self_pairs


def rotary_tables(position):
    half = HD // 2
    lane = jnp.arange(2 * HD, dtype=jnp.int32)
    freqs = jnp.exp((lane % half).astype(F32) * (-2.0 * math.log(BASE) / HD))
    angles = position.astype(F32)[:, None] * freqs[None, :]
    sign = jnp.where(lane % HD < half, -1.0, 1.0)
    return jnp.cos(angles), jnp.sin(angles) * sign[None, :]


def swap(values, axis, mask, size):
    return lax.ppermute(values, axis, [(i, i ^ mask) for i in range(size)])


def dot(a, b):
    return jnp.dot(a, b, preferred_element_type=F32)


def dot_nt(a, b):
    return lax.dot_general(a, b, (((1,), (1,)), ((), ())), preferred_element_type=F32)


def dot_tn(a, b):
    return lax.dot_general(a, b, (((0,), (0,)), ((), ())), preferred_element_type=F32)


def params(**more):
    return pltpu.CompilerParams(vmem_limit_bytes=VMEM_LIMIT, **more)


def cost(flops, moved):
    return pl.CostEstimate(flops=int(max(flops, SPAN)), bytes_accessed=int(moved), transcendentals=0)


def norm_parts(values):
    center = values - jnp.mean(values, axis=-1, keepdims=True)
    spread = jnp.mean(center * center, axis=-1, keepdims=True)
    inv = lax.rsqrt(spread + EPSILON)
    return center * inv, inv


def norm_back(grad, unit, inv, gain):
    scaled = grad * gain
    first = jnp.mean(scaled, axis=-1, keepdims=True)
    second = jnp.mean(scaled * unit, axis=-1, keepdims=True)
    return inv * (scaled - first - unit * second)


def turn(values, cosine, sine):
    half = HD // 2
    pair = 2 * HD
    lane = lax.broadcasted_iota(jnp.int32, (1, pair), 1)
    low = (lane % HD) < half
    parts = []
    for at in range(0, values.shape[1], pair):
        part = values[:, at : at + pair]
        other = jnp.where(low, pltpu.roll(part, pair - half, 1), pltpu.roll(part, half, 1))
        parts.append(part * cosine + other * sine)
    return parts[0] if len(parts) == 1 else jnp.concatenate(parts, axis=1)


def bits_of(index, masks):
    total = 0
    for bit, mask in enumerate(masks):
        if (index >> bit) & 1:
            total |= mask
    return total


def piece_map(which, masks):
    count = 1 << len(masks)
    half = count // 2
    kind, r, y = which
    if kind == "a":
        return [((i,), r, bits_of(i, masks), 0) for i in range(count)]
    return [
        ((x * half + i,), r | (2 * x), bits_of(i, masks) | y, 1)
        for x in range(2)
        for i in range(half)
    ]


def place(pieces, maps, me_f, h, w_ref, slot_of):
    for ref, entries in zip(pieces, maps):
        for at, r, k, colour in entries:
            w_ref[slot_of(r), me_f ^ k, colour * h : (colour + 1) * h, :] = ref[at]


def times(count, body):
    def step(g, carry):
        body(g)
        return carry

    lax.fori_loop(0, count, step, 0)


def vmem(count):
    return [pl.BlockSpec(memory_space=pltpu.VMEM)] * count


def qkv_kernel(
    maps, h, idx_ref, x_ref, small_ref, cos_ref, sin_ref, p0, p1, p2, p3, p4, p5, p6, p7,
    normed_ref, out_ref, w_ref,
):
    d4, me_f = idx_ref[0], idx_ref[1]
    d = x_ref.shape[1]
    place((p0, p1, p2, p3, p4, p5, p6, p7), maps, me_f, h, w_ref, lambda r: d4 ^ r)
    unit, _ = norm_parts(x_ref[...].astype(F32))
    normed_ref[...] = (unit * small_ref[0:1, :] + small_ref[1:2, :]).astype(BF)

    def product(g):
        return dot(normed_ref[...], w_ref[g].reshape(d, d))

    def turned(g):
        out_ref[g] = turn(product(g), cos_ref[...], sin_ref[...]).astype(BF)

    times(2, turned)
    out_ref[2] = product(2).astype(BF)


def qkv(idx, x, small, cosine, sine, pieces, maps, shards, h):
    n, d = x.shape
    return pl.pallas_call(
        partial(qkv_kernel, maps, h),
        out_shape=(
            jax.ShapeDtypeStruct((n, d), BF),
            jax.ShapeDtypeStruct((3, n, d), BF),
            jax.ShapeDtypeStruct((4, shards, 2 * h, d), BF),
        ),
        in_specs=[pl.BlockSpec(memory_space=pltpu.SMEM)] + vmem(12),
        out_specs=tuple(vmem(3)),
        compiler_params=params(),
        cost_estimate=cost(6 * n * d * d, 2 * (5 * n * d + 8 * d * d)),
        name="qkv",
    )(idx, x, small, cosine, sine, *pieces)


def head_mask(which):
    lane = lax.broadcasted_iota(jnp.int32, (1, 2 * HD), 1)
    return (lane < HD) if which == 0 else (lane >= HD)


def attend_kernel(q_ref, k_ref, v_ref, bias_ref, mixed_ref, probs_ref):
    q, k, v = q_ref[0], k_ref[0], v_ref[0]
    zero = jnp.zeros((), BF)
    parts = []
    for h in range(2):
        own = jnp.where(head_mask(h), q, zero)
        scores = dot_nt(own, k) * (HD**-0.5) + bias_ref[...]
        top = jnp.max(scores, axis=1, keepdims=True)
        raised = jnp.exp(scores - top)
        total = jnp.sum(raised, axis=1, keepdims=True)
        probs = (raised * (1.0 / total)).astype(BF)
        probs_ref[h] = probs
        parts.append(dot(probs, v))
    mixed_ref[...] = jnp.where(head_mask(0), parts[0], parts[1]).astype(BF)


def attend(three, bias):
    _, n, d = three.shape
    pair = 2 * HD
    return pl.pallas_call(
        attend_kernel,
        grid=(d // pair,),
        out_shape=(
            jax.ShapeDtypeStruct((n, d), BF),
            jax.ShapeDtypeStruct((d // HD, n, n), BF),
        ),
        in_specs=[
            pl.BlockSpec((1, n, pair), lambda p: (0, 0, p)),
            pl.BlockSpec((1, n, pair), lambda p: (1, 0, p)),
            pl.BlockSpec((1, n, pair), lambda p: (2, 0, p)),
            pl.BlockSpec((n, n), lambda p: (0, 0)),
        ],
        out_specs=(
            pl.BlockSpec((n, pair), lambda p: (0, p)),
            pl.BlockSpec((2, n, n), lambda p: (p, 0, 0)),
        ),
        compiler_params=params(),
        cost_estimate=cost(8 * n * n * d, 2 * n * n * (d // HD) + 8 * n * d),
        name="attend",
    )(three, three, three, bias)


def attend_back_kernel(
    q_ref, k_ref, v_ref, probs_ref, grad_ref, mixed_ref, cos_ref, sin_ref, out_ref
):
    q, k, v, grad = q_ref[0], k_ref[0], v_ref[0], grad_ref[...]
    zero = jnp.zeros((), BF)
    product = grad.astype(F32) * mixed_ref[...].astype(F32)
    dq, dk, dv = [], [], []
    for h in range(2):
        mask = head_mask(h)
        inner = jnp.sum(jnp.where(mask, product, 0.0), axis=1, keepdims=True)
        probs = probs_ref[h]
        prob_grad = dot_nt(jnp.where(mask, grad, zero), v)
        score_grad = (probs.astype(F32) * (prob_grad - inner)).astype(BF)
        dq.append(dot(score_grad, k))
        dk.append(dot_tn(score_grad, q))
        dv.append(dot_tn(probs, grad))
    first = head_mask(0)
    scale = HD**-0.5
    cosine, sine = cos_ref[...], sin_ref[...]
    out_ref[0] = turn(jnp.where(first, dq[0], dq[1]) * scale, cosine, -sine).astype(BF)
    out_ref[1] = turn(jnp.where(first, dk[0], dk[1]) * scale, cosine, -sine).astype(BF)
    out_ref[2] = jnp.where(first, dv[0], dv[1]).astype(BF)


def attend_back(three, probs, grad, mixed, cosine, sine):
    _, n, d = three.shape
    pair = 2 * HD
    return pl.pallas_call(
        attend_back_kernel,
        grid=(d // pair,),
        out_shape=jax.ShapeDtypeStruct((3, n, d), BF),
        in_specs=[
            pl.BlockSpec((1, n, pair), lambda p: (0, 0, p)),
            pl.BlockSpec((1, n, pair), lambda p: (1, 0, p)),
            pl.BlockSpec((1, n, pair), lambda p: (2, 0, p)),
            pl.BlockSpec((2, n, n), lambda p: (p, 0, 0)),
            pl.BlockSpec((n, pair), lambda p: (0, p)),
            pl.BlockSpec((n, pair), lambda p: (0, p)),
            pl.BlockSpec(cosine.shape, lambda p: (0, 0)),
            pl.BlockSpec(sine.shape, lambda p: (0, 0)),
        ],
        out_specs=pl.BlockSpec((3, n, pair), lambda p: (0, 0, p)),
        compiler_params=params(),
        cost_estimate=cost(16 * n * n * d, 2 * n * n * (d // HD) + 16 * n * d),
        name="attend_back",
    )(three, three, three, probs, grad, mixed, cosine, sine)


def branch_kernel(x_ref, mixed_ref, w_ref, small_ref, residual_ref, hidden_ref):
    residual = x_ref[...].astype(F32) + dot(mixed_ref[...], w_ref[0])
    residual_ref[...] = residual
    unit, _ = norm_parts(residual)
    hidden_ref[...] = (unit * small_ref[2:3, :] + small_ref[3:4, :]).astype(BF)


def branch(x, mixed, weights, small):
    n, d = x.shape
    rows = n // 2
    return pl.pallas_call(
        branch_kernel,
        grid=(2,),
        out_shape=(jax.ShapeDtypeStruct((n, d), F32), jax.ShapeDtypeStruct((n, d), BF)),
        in_specs=[
            pl.BlockSpec((rows, d), lambda g: (g, 0)),
            pl.BlockSpec((rows, d), lambda g: (g, 0)),
            pl.BlockSpec((1, d, d), lambda g: (3, 0, 0)),
            pl.BlockSpec(small.shape, lambda g: (0, 0)),
        ],
        out_specs=(
            pl.BlockSpec((rows, d), lambda g: (g, 0)),
            pl.BlockSpec((rows, d), lambda g: (g, 0)),
        ),
        compiler_params=params(),
        cost_estimate=cost(2 * n * d * d, 10 * n * d + 2 * d * d),
        name="branch",
    )(x, mixed, weights, small)


def spread(out_ref, g, keep, product, me_f, masks, h, shards):
    keep[...] = product.astype(BF)
    for i in range(shards):
        j = me_f ^ bits_of(i, masks)
        for colour in range(2):
            start = pl.multiple_of(j * (2 * h) + colour * h, h & -h)
            out_ref[g, colour, i] = keep[pl.ds(start, h), :]


def up_kernel(
    masks, maps, rs, h, shards, idx_ref, hidden_ref, c_ref, small_ref, p0, p1, p2, p3,
    act_ref, slope_ref, grad_ref, w_ref, keep,
):
    d4, me_f = idx_ref[0], idx_ref[1]
    d = hidden_ref.shape[1]
    place((p0, p1, p2, p3), maps, me_f, h, w_ref, rs.index)

    def half_step(g):
        chunk = d4 ^ jnp.where(g == 0, rs[0], rs[1])
        bias = small_ref[5:6, :]
        for other in range(1, 4):
            bias = jnp.where(chunk == other, small_ref[5 + other : 6 + other, :], bias)
        v = dot(hidden_ref[...], w_ref[g].reshape(d, d)) + bias
        c = math.sqrt(2.0 / math.pi)
        square = v * v
        t = jnp.tanh(v * (c + (c * 0.044715) * square))
        half = 0.5 * (1.0 + t)
        act = (v * half).astype(BF)
        act_ref[g] = act
        slope = half + (0.5 * v) * (1.0 - t * t) * (c + (3.0 * c * 0.044715) * square)
        slope_ref[g] = slope.astype(BF)
        spread(grad_ref, g, keep, dot_tn(act, c_ref[...]), me_f, masks, h, shards)

    times(2, half_step)


def up(idx, hidden, c, small, pieces, maps, rs, masks, shards, h):
    n, d = hidden.shape
    return pl.pallas_call(
        partial(up_kernel, masks, maps, rs, h, shards),
        out_shape=(
            jax.ShapeDtypeStruct((2, n, d), BF),
            jax.ShapeDtypeStruct((2, n, d), BF),
            jax.ShapeDtypeStruct((2, 2, shards, h, d), BF),
            jax.ShapeDtypeStruct((2, shards, 2 * h, d), BF),
        ),
        in_specs=[pl.BlockSpec(memory_space=pltpu.SMEM)] + vmem(7),
        out_specs=tuple(vmem(4)),
        scratch_shapes=[pltpu.VMEM((d, d), BF)],
        compiler_params=params(),
        cost_estimate=cost(8 * n * d * d, 2 * (6 * n * d + 6 * d * d)),
        name="up",
    )(idx, hidden, c, small, *pieces)


def act_grad_kernel(
    masks, maps, rs, h, shards, first, idx_ref, c_ref, x_ref, up_ref, slope_ref, p0, p1, p2, p3,
    *more,
):
    if first:
        hidden_ref, sums_ref, grad_ref, w_ref, keep = more
    else:
        hidden_in, sums_in, hidden_ref, sums_ref, grad_ref, w_ref, keep = more
    d4, me_f = idx_ref[0], idx_ref[1]
    d = x_ref.shape[1]
    place((p0, p1, p2, p3), maps, me_f, h, w_ref, rs.index)
    if first:
        hidden_ref[...] = jnp.zeros_like(hidden_ref)
        sums_ref[...] = jnp.zeros_like(sums_ref)
        sums_ref[4:5, :] = jnp.sum(c_ref[...].astype(F32), axis=0, keepdims=True)
    else:
        hidden_ref[...] = hidden_in[...]
        sums_ref[...] = sums_in[...]

    def half_step(g):
        chunk = d4 ^ jnp.where(g == 0, rs[0], rs[1])
        grad = dot_nt(c_ref[...], w_ref[g].reshape(d, d))
        pre = (grad * slope_ref[g].astype(F32)).astype(BF)
        sums = jnp.sum(pre.astype(F32), axis=0, keepdims=True)
        row = lax.broadcasted_iota(jnp.int32, (sums_ref.shape[0], 1), 0)
        sums_ref[...] += jnp.where(row == 5 + chunk, sums, 0.0)
        hidden_ref[...] += dot_nt(pre, up_ref[g])
        spread(grad_ref, g, keep, dot_tn(x_ref[...], pre), me_f, masks, h, shards)

    times(2, half_step)


def act_grad(idx, c, hidden, up_half, slope, pieces, maps, rs, masks, shards, h, before=None):
    n, d = c.shape
    before = before or ()
    return pl.pallas_call(
        partial(act_grad_kernel, masks, maps, rs, h, shards, not before),
        out_shape=(
            jax.ShapeDtypeStruct((n, d), F32),
            jax.ShapeDtypeStruct((SMALL, d), F32),
            jax.ShapeDtypeStruct((2, 2, shards, h, d), BF),
            jax.ShapeDtypeStruct((2, shards, 2 * h, d), BF),
        ),
        in_specs=[pl.BlockSpec(memory_space=pltpu.SMEM)] + vmem(8 + len(before)),
        out_specs=tuple(vmem(4)),
        scratch_shapes=[pltpu.VMEM((d, d), BF)],
        compiler_params=params(),
        cost_estimate=cost(12 * n * d * d, 2 * (8 * n * d + 8 * d * d)),
        name="act_grad",
    )(idx, c, hidden, up_half.reshape(2, d, d), slope, *pieces, *before)


def first_grad_kernel(
    masks, h, shards, rs, idx_ref, normed_ref, mixed_ref, three_ref, branch_ref, out_ref, keep
):
    g = pl.program_id(0)
    last = (idx_ref[0] ^ jnp.where(g == 0, rs[0], rs[1])) == 3
    x = jnp.where(last, mixed_ref[...], normed_ref[...])
    y = jnp.where(last, branch_ref[...], three_ref[0])
    spread(out_ref, 0, keep, dot_tn(x, y), idx_ref[1], masks, h, shards)


def first_grad(idx, normed, mixed, three_grad, branch_grad, rs, masks, shards, h):
    n, d = normed.shape

    def which(g, idx_ref):
        return jnp.minimum(idx_ref[0] ^ jnp.where(g == 0, rs[0], rs[1]), 2)

    whole = pl.BlockSpec((n, d), lambda g, i: (0, 0))
    return pl.pallas_call(
        partial(first_grad_kernel, masks, h, shards, rs),
        grid_spec=pltpu.PrefetchScalarGridSpec(
            num_scalar_prefetch=1,
            grid=(2,),
            in_specs=[
                whole,
                whole,
                pl.BlockSpec((1, n, d), lambda g, i: (which(g, i), 0, 0)),
                whole,
            ],
            out_specs=pl.BlockSpec((1, 2, shards, h, d), lambda g, i: (g, 0, 0, 0, 0)),
            scratch_shapes=[pltpu.VMEM((d, d), BF)],
        ),
        out_shape=jax.ShapeDtypeStruct((2, 2, shards, h, d), BF),
        compiler_params=params(),
        cost_estimate=cost(4 * n * d * d, 2 * (5 * n * d + 2 * d * d)),
        name="first_grad",
    )(idx, normed, mixed, three_grad, branch_grad)


def middle_kernel(
    c_ref, hidden_ref, residual_ref, small_ref, w_ref, grad_ref, low_ref, mixed_ref, sums_ref
):
    @pl.when(pl.program_id(0) == 0)
    def _():
        sums_ref[...] = jnp.zeros_like(sums_ref)

    grad = hidden_ref[...]
    unit, inv = norm_parts(residual_ref[...])
    sums_ref[2:3, :] += jnp.sum(grad * unit, axis=0, keepdims=True)
    sums_ref[3:4, :] += jnp.sum(grad, axis=0, keepdims=True)
    full = c_ref[...].astype(F32) + norm_back(grad, unit, inv, small_ref[2:3, :])
    grad_ref[...] = full
    low = full.astype(BF)
    low_ref[...] = low
    mixed_ref[...] = dot_nt(low, w_ref[0]).astype(BF)


def middle(c, hidden_grad, residual, small, weights):
    n, d = c.shape
    rows = n // 2
    return pl.pallas_call(
        middle_kernel,
        grid=(2,),
        out_shape=(
            jax.ShapeDtypeStruct((n, d), F32),
            jax.ShapeDtypeStruct((n, d), BF),
            jax.ShapeDtypeStruct((n, d), BF),
            jax.ShapeDtypeStruct((SMALL, d), F32),
        ),
        in_specs=[
            pl.BlockSpec((rows, d), lambda g: (g, 0)),
            pl.BlockSpec((rows, d), lambda g: (g, 0)),
            pl.BlockSpec((rows, d), lambda g: (g, 0)),
            pl.BlockSpec(small.shape, lambda g: (0, 0)),
            pl.BlockSpec((1, d, d), lambda g: (3, 0, 0)),
        ],
        out_specs=(
            pl.BlockSpec((rows, d), lambda g: (g, 0)),
            pl.BlockSpec((rows, d), lambda g: (g, 0)),
            pl.BlockSpec((rows, d), lambda g: (g, 0)),
            pl.BlockSpec((SMALL, d), lambda g: (0, 0)),
        ),
        compiler_params=params(),
        cost_estimate=cost(2 * n * d * d, 18 * n * d + 2 * d * d),
        name="middle",
    )(c, hidden_grad, residual, small, weights)


def input_kernel(x_ref, three_ref, w_ref, small_ref, grad_ref, out_ref, sums_ref, total):
    g = pl.program_id(0)
    part = dot_nt(three_ref[0], w_ref[0])

    @pl.when(g == 0)
    def _():
        total[...] = part

    @pl.when(g > 0)
    def _():
        total[...] += part

    @pl.when(g == 2)
    def _():
        grad = total[...]
        unit, inv = norm_parts(x_ref[...].astype(F32))
        sums_ref[...] = jnp.zeros_like(sums_ref)
        sums_ref[0:1, :] = jnp.sum(grad * unit, axis=0, keepdims=True)
        sums_ref[1:2, :] = jnp.sum(grad, axis=0, keepdims=True)
        out_ref[...] = grad_ref[...] + norm_back(grad, unit, inv, small_ref[0:1, :])


def input_grads(x, three_grad, weights, small, residual_grad):
    n, d = x.shape
    return pl.pallas_call(
        input_kernel,
        grid=(3,),
        out_shape=(jax.ShapeDtypeStruct((n, d), F32), jax.ShapeDtypeStruct((SMALL, d), F32)),
        in_specs=[
            pl.BlockSpec((n, d), lambda g: (0, 0)),
            pl.BlockSpec((1, n, d), lambda g: (g, 0, 0)),
            pl.BlockSpec((1, d, d), lambda g: (g, 0, 0)),
            pl.BlockSpec(small.shape, lambda g: (0, 0)),
            pl.BlockSpec((n, d), lambda g: (0, 0)),
        ],
        out_specs=(
            pl.BlockSpec((n, d), lambda g: (0, 0)),
            pl.BlockSpec((SMALL, d), lambda g: (0, 0)),
        ),
        scratch_shapes=[pltpu.VMEM((n, d), F32)],
        compiler_params=params(),
        cost_estimate=cost(6 * n * d * d, 16 * n * d + 6 * d * d),
        name="input_grads",
    )(x, three_grad, weights, small, residual_grad)


def down_kernel(a0_ref, a1_ref, w0_ref, w1_ref, small_ref, residual_ref, out_ref, total):
    g = pl.program_id(0)
    part = dot(a0_ref[0], w0_ref[0]) + dot(a1_ref[0], w1_ref[0])

    @pl.when(g == 0)
    def _():
        total[...] = residual_ref[...] + small_ref[4:5, :] + part

    @pl.when(g == 1)
    def _():
        out_ref[...] = (total[...] + part).astype(BF)


def down_out(acts, weights, small, residual):
    n, d = residual.shape
    return pl.pallas_call(
        down_kernel,
        grid=(2,),
        out_shape=jax.ShapeDtypeStruct((n, d), BF),
        in_specs=[
            pl.BlockSpec((1, n, d), lambda g: (g, 0, 0)),
            pl.BlockSpec((1, n, d), lambda g: (g, 0, 0)),
            pl.BlockSpec((1, d, d), lambda g: (g, 0, 0)),
            pl.BlockSpec((1, d, d), lambda g: (g, 0, 0)),
            pl.BlockSpec(small.shape, lambda g: (0, 0)),
            pl.BlockSpec((n, d), lambda g: (0, 0)),
        ],
        out_specs=pl.BlockSpec((n, d), lambda g: (0, 0)),
        scratch_shapes=[pltpu.VMEM((n, d), F32)],
        compiler_params=params(),
        cost_estimate=cost(8 * n * d * d, 14 * n * d + 8 * d * d),
        name="down_out",
    )(*acts, *(w.reshape(2, d, d) for w in weights), small, residual)


def last_kernel(shards, idx_ref, p0, p1, p2, p3, up_ref, down_ref, keep):
    _, rows, d = keep.shape
    for r, ref in enumerate((p0, p1, p2, p3)):
        at = idx_ref[0] ^ r
        keep[at] = ref[0].reshape(rows, d).astype(F32)
        down_ref[pl.ds(pl.multiple_of(at * rows, 8), rows), :] = ref[1].reshape(rows, d).astype(F32)
    for i in range(shards):
        part = [keep[chunk, :, i * rows : (i + 1) * rows] for chunk in range(4)]
        up_ref[:, 4 * rows * i : 4 * rows * (i + 1)] = jnp.concatenate(part, axis=1)


def last_out(idx, pieces, shards):
    d = pieces[0].shape[-1]
    rows = d // shards
    vmem = pl.BlockSpec(memory_space=pltpu.VMEM)
    return pl.pallas_call(
        partial(last_kernel, shards),
        out_shape=(
            jax.ShapeDtypeStruct((rows, 4 * d), F32),
            jax.ShapeDtypeStruct((4 * rows, d), F32),
        ),
        in_specs=[pl.BlockSpec(memory_space=pltpu.SMEM)] + [vmem] * 4,
        out_specs=(vmem, vmem),
        scratch_shapes=[pltpu.VMEM((4, rows, d), F32)],
        compiler_params=params(),
        name="last_out",
    )(idx, *pieces)


def local(dp, fsdp, tokens, lengths, *rest):
    (
        norm1_gain,
        norm1_bias,
        query_weight,
        key_weight,
        value_weight,
        output_weight,
        norm2_gain,
        norm2_bias,
        up_weight,
        up_bias,
        down_weight,
        down_bias,
        cotangent,
    ) = rest
    row_count, width = tokens.shape
    slot_count = lengths.shape[1]
    R = width // fsdp
    h = R // 2
    me_dp = lax.axis_index("dp").astype(jnp.int32)
    me_f = lax.axis_index("fsdp").astype(jnp.int32)
    d4 = me_dp % 4
    idx = jnp.stack([d4, me_f])
    masks = []
    mask = fsdp // 2
    while mask >= 1:
        masks.append(mask)
        mask //= 2
    masks = tuple(masks)
    outer = masks[:-1]

    def fswap(v, m):
        return swap(v, "fsdp", m, fsdp)

    def dswap(v, m):
        return swap(v, "dp", m, dp)

    def after(value, *tokens):
        return lax.optimization_barrier((value,) + tokens)[0]

    def after_all(values, *tokens):
        values = tuple(values)
        return list(lax.optimization_barrier(values + tokens)[: len(values)])

    half = fsdp // 2
    maps_own = [
        piece_map(w, masks) for w in (("a", 0, 0), ("a", 2, 0), ("b", 0, 0), ("b", 0, 1))
    ]
    maps_core = [
        piece_map(w, masks) for w in (("a", 1, 0), ("a", 3, 0), ("b", 1, 0), ("b", 1, 1))
    ]

    class Gather:
        def __init__(self, piece):
            self.cur = piece[None]

        def far(self, m):
            self.got = fswap(self.cur, m)

        def join(self):
            self.cur = jnp.concatenate([self.cur, self.got], axis=0)

        def near(self):
            self.got = fswap(self.cur, outer[-1])

        def sides(self):
            a = jnp.concatenate([self.cur[:, :h], self.got[:, :h]], axis=0)
            b = jnp.concatenate([self.cur[:, h:R], self.got[:, h:R]], axis=0)
            self.ab = (a, b)
            self.got_ab = (fswap(a, masks[-1]), dswap(b, 2))

        def cross(self):
            a1 = jnp.concatenate([self.ab[0], self.got_ab[0]], axis=0)
            b1 = jnp.concatenate([self.ab[1], self.got_ab[1]], axis=0)
            self.ab1 = (a1, b1)
            self.got_ab1 = (dswap(a1, 2), fswap(b1, masks[-1]))
            self.core = [dswap(a1, 1), dswap(b1, 1)]

        def finish(self):
            a_x, b_y = self.got_ab1
            a1, b1 = self.ab1
            self.own = [a1, a_x, b1, b_y]
            self.other = [self.core[0], dswap(a_x, 1), self.core[1], dswap(b_y, 1)]

    class Inner:
        def __init__(self, cur):
            self.cur = cur
            self.got = None
            self.left = list(reversed(outer))

        def step(self, *tokens):
            if self.got is not None:
                self.cur = self.cur + after(self.got, *tokens)
                self.got = None
            if self.left:
                count = self.cur.shape[0] // 2
                front = self.cur[count:]
                self.got = fswap(front, self.left.pop(0))
                self.cur = self.cur[:count]
                return front
            return self.cur

        def sums(self):
            while self.got is not None or self.left:
                self.step()
            return self.cur[0]

    class Spread:
        def __init__(self, total):
            m = 4
            while m < dp:
                total = total + dswap(total, m)
                m *= 2
            self.total = total
            self.pair = dswap(total, 2)
            self.core = dswap(total, 1)

        def four(self, *tokens):
            pair = after(self.pair, *tokens)
            return [self.total, self.core, pair, dswap(pair, 1)]

    piece1 = lax.select_n(d4, query_weight, key_weight, value_weight, output_weight)
    g1 = Gather(piece1)
    for m in outer[:-1]:
        g1.far(m)
        g1.join()
    g1_first = g1.cur
    g1.near()
    vectors = after_all(
        (norm1_gain, norm1_bias, norm2_gain, norm2_bias, down_bias, up_bias, up_weight), piece1
    )
    tall = jnp.concatenate(vectors[:6]).reshape(9, R)
    lane = jnp.arange(width, dtype=jnp.int32) // R
    tall = jnp.where((lane == me_f)[None, :], jnp.tile(tall, (1, fsdp)), jnp.zeros((), BF))
    tall = jnp.pad(tall, ((0, SMALL - 9), (0, 0)))
    fronts = []
    for m in reversed(masks):
        if len(fronts) == 1:
            tall = after(tall, g1.got)
        fronts.append(tall)
        tall = tall + fswap(tall, m)
    small = tall.astype(F32)
    piece2 = lax.dynamic_index_in_dim(
        vectors[6].reshape(R, fsdp, 4, R), d4, axis=2, keepdims=False
    ).reshape(R, width)
    g2 = Gather(after(piece2, g1.got, *fronts[2:]))
    for m in outer[:-1]:
        g2.far(m)
        g2.join()
    g1.sides()
    g2.cur, g2.got = after_all((g2.cur, g2.got), *g1.ab)
    g2.near()
    g1.cross()
    early = outer[:-1]
    g3 = Gather(
        lax.dynamic_slice_in_dim(after(down_weight, g2.cur), d4 * R, R, axis=0)
    )
    for m in early[:-1]:
        g3.far(m)
        g3.join()
    g3.far(early[-1])
    g1.finish()
    g2.cur, g2.got = after_all((g2.cur, g2.got), *g1.got_ab1)
    g2.sides()
    g3.join()
    g3.near()

    layout = row_layout(after(lengths, g1_first)[0], row_count, slot_count)
    cosine, sine = rotary_tables(layout[3])
    bias = jnp.where(allowed_pairs(layout, layout, BLOCK, slot_count), 0.0, NEGATIVE)
    normed, three, first4 = qkv(
        idx, after(tokens, *g2.ab, g3.cur, bias), small, cosine, sine, g1.own + g1.other,
        maps_own + maps_core, fsdp, h,
    )
    first4 = first4.reshape(4, width, width)
    g2.got_ab = after_all(g2.got_ab, three)
    g2.cross()
    mixed, probs = attend(after(three, *g2.ab1), bias)
    g2.got_ab1 = after_all(g2.got_ab1, mixed)
    g2.finish()
    g3.cur, g3.got = after_all((g3.cur, g3.got), mixed)
    g3.sides()
    residual, hidden_in = branch(tokens, after(mixed, *g2.got_ab1, *g2.core, *g3.ab), first4, small)
    g3.got_ab = after_all(g3.got_ab, hidden_in)
    g3.cross()
    send_rs, keep_rs = (1, 3), (0, 2)
    act_s, slope_s, send3, up_s = up(
        idx, after(hidden_in, *g3.ab1), cotangent, small, g2.other, maps_core, send_rs, masks,
        fsdp, h,
    )
    act_k, slope_k, keep3, up_k = up(
        idx, after(hidden_in, send3), cotangent, small, g2.own, maps_own, keep_rs, masks, fsdp, h,
    )
    g3.got_ab1 = after_all(g3.got_ab1, keep3)
    g3.finish()

    class Scatter:
        def __init__(self, send):
            self.got = dswap(send, 1)

        def sides(self, keep):
            got = self.got
            a = keep[1, 0] + got[1, 0]
            b = keep[:, 1, half:] + got[:, 1, half:]
            self.keep = (keep[0, 0] + got[0, 0], keep[:, 1, :half] + got[:, 1, :half])
            self.mid = [dswap(a, 2), fswap(b, masks[-1])]
            self.done = (a, b) + self.keep

        def cross(self):
            (a, b), (x, y) = self.keep, self.mid
            self.last = (a[:half] + x[:half], b[0] + y[0])
            out = (a[half:] + x[half:], b[1] + y[1])
            self.got_last = [fswap(out[0], masks[-1]), dswap(out[1], 2)]
            self.done = out + self.last

        def rows(self):
            (a, b), (x, y) = self.last, self.got_last
            return jnp.stack([a + x, b + y], axis=1)

    s3 = Scatter(send3)
    s3.sides(keep3)
    hidden_s, sums_s, send2, down_s = act_grad(
        idx, after(cotangent, *s3.done), hidden_in, up_s, slope_s, g3.other, maps_core, send_rs,
        masks, fsdp, h,
    )
    s2 = Scatter(send2)
    s3.mid = after_all(s3.mid, send2)
    s3.cross()
    hidden_grad, sums_act, keep2, down_k = act_grad(
        idx, after(cotangent, send2, *s3.done), hidden_in, up_k, slope_k, g3.own, maps_own,
        keep_rs, masks, fsdp, h, (hidden_s, sums_s),
    )
    s2.sides(keep2)
    s3.got_last = after_all(s3.got_last, keep2)
    rows3 = Inner(s3.rows())
    front = rows3.step()
    residual_grad, branch_grad, mixed_grad, sums_mid = middle(
        cotangent, after(hidden_grad, *s2.done, front), residual, small, first4
    )
    front = rows3.step(mixed_grad)
    three_grad = attend_back(three, probs, after(mixed_grad, front), mixed, cosine, sine)
    s2.mid = after_all(s2.mid, three_grad)
    s2.cross()
    front = rows3.step(three_grad)
    send1 = first_grad(
        idx, after(normed, *s2.done, front), mixed, three_grad, branch_grad, send_rs, masks, fsdp,
        h,
    )
    s1 = Scatter(send1)
    s2.got_last = after_all(s2.got_last, send1)
    rows2 = Inner(s2.rows())
    front = rows2.step()
    keep1 = first_grad(
        idx, after(normed, front, send1), mixed, three_grad, branch_grad, keep_rs, masks, fsdp, h
    )
    s1.sides(keep1)
    front = rows2.step(*s1.done)
    input_grad, sums_in = input_grads(
        after(tokens, *s1.done, front), three_grad, first4, small, residual_grad
    )
    front = rows2.step(input_grad)
    small_sum = sums_act + sums_mid + sums_in

    def small_step(swapper, m, *tokens):
        low = after(small_sum.astype(BF), *tokens)
        return low, swapper(low, m)

    low, small_got = small_step(dswap, 1)
    output = down_out(
        (act_s, act_k), (down_s, down_k), small, after(residual, front, low)
    )
    s1.mid = after_all(s1.mid, output)
    s1.cross()
    both = Spread(after(jnp.stack([rows2.sums(), rows3.sums()]), *s1.done))
    rest = [(fswap, m) for m in reversed(masks)]
    m = 2
    while m < dp:
        rest.append((dswap, m))
        m *= 2
    small_sum = small_sum + after(small_got, output).astype(F32)
    low, small_got = small_step(*rest.pop(), *s1.done)
    rows1 = Inner(s1.rows())
    small_sum = small_sum + after(small_got, rows1.cur).astype(F32)
    front = rows1.step()
    low, small_got = small_step(*rest.pop(), front)
    both.pair = after(both.pair, rows1.cur)
    front = rows1.step(low)
    small_sum = small_sum + after(small_got, front).astype(F32)
    low, small_got = small_step(*rest.pop(), front)
    four23 = both.four(front)

    up_grad, down_grad = last_out(idx, four23, fsdp)
    if rows1.got is not None:
        rows1.got = after(rows1.got, up_grad)
    one = Spread(rows1.sums())
    small_sum = small_sum + after(small_got, one.total).astype(F32)
    while rest:
        low, small_got = small_step(*rest.pop(), one.total)
        small_sum = small_sum + small_got.astype(F32)
    four1 = jnp.stack(one.four())
    first_grads = [
        lax.dynamic_index_in_dim(four1, d4 ^ d, axis=0, keepdims=False)
        .reshape(R, width)
        .astype(F32)
        for d in range(4)
    ]
    own = lax.dynamic_slice_in_dim(small_sum, me_f * R, R, axis=1)
    return (
        output,
        input_grad,
        own[0],
        own[1],
        first_grads[0],
        first_grads[1],
        first_grads[2],
        first_grads[3],
        own[2],
        own[3],
        up_grad,
        own[5:9].reshape(4 * R),
        down_grad,
        own[4],
    )


def solution(mesh):
    rows = P(("dp", "fsdp"), None)
    flat = P("fsdp")
    tall = P("fsdp", None)
    in_specs = (
        rows, rows, flat, flat, tall, tall, tall, tall, flat, flat, tall, flat, tall, flat, rows,
    )
    out_specs = (
        rows, rows, flat, flat, tall, tall, tall, tall, flat, flat, tall, flat, tall, flat,
    )
    return jax.shard_map(
        partial(local, mesh.shape["dp"], mesh.shape["fsdp"]),
        mesh=mesh,
        in_specs=in_specs,
        out_specs=out_specs,
        check_vma=False,
    )
```

```python
from functools import partial
import math

import jax
import jax.numpy as jnp
from jax import lax
from jax.experimental import pallas as pl
from jax.experimental.pallas import tpu as pltpu
from jax.sharding import PartitionSpec as P

H = 12
HD = 64
BLOCK = 16
EPSILON = 1e-05
BASE = 10000.0
NEGATIVE = -1e30
BF = jnp.bfloat16
F32 = jnp.float32
SMALL = 16
SPAN = 4.8e10
VMEM_LIMIT = 16 * 1024 * 1024


def row_layout(length_row, row_count, slot_count):
    doubled = 2 * length_row
    ends_at = jnp.cumsum(doubled, dtype=jnp.int32)
    starts_at = ends_at - doubled
    row_index = jnp.arange(row_count, dtype=jnp.int32)
    member = (row_index[:, None] >= starts_at[None, :]) & (row_index[:, None] < ends_at[None, :])
    slot_ids = jnp.arange(slot_count, dtype=jnp.int32)
    slot_index = jnp.sum(jnp.where(member, slot_ids[None, :], 0), axis=1, dtype=jnp.int32)
    start_row = jnp.sum(jnp.where(member, starts_at[None, :], 0), axis=1, dtype=jnp.int32)
    seq_length = jnp.sum(jnp.where(member, length_row[None, :], 0), axis=1, dtype=jnp.int32)
    local_row = row_index - start_row
    clean_flag = (local_row >= seq_length).astype(jnp.int32)
    position = local_row - clean_flag * seq_length
    return (row_index, slot_index, clean_flag, position)


def allowed_pairs(query_side, key_side, block_size, slot_count):
    query_row, query_slot, query_clean, query_pos = query_side
    key_row, key_slot, key_clean, key_pos = key_side
    query_block = query_pos // block_size
    key_block = key_pos // block_size
    same_seq = query_slot[:, None] == key_slot[None, :]
    key_noisy = key_clean[None, :] == 0
    key_plain = key_clean[None, :] == 1
    noisy_rule = key_noisy & (key_block[None, :] == query_block[:, None]) | key_plain & (
        key_block[None, :] < query_block[:, None]
    )
    clean_rule = key_plain & (key_block[None, :] <= query_block[:, None])
    rule_held = jnp.where(query_clean[:, None] == 1, clean_rule, noisy_rule)
    padded = query_slot == slot_count - 1
    real_pairs = same_seq & rule_held & jnp.logical_not(padded)[:, None]
    self_pairs = padded[:, None] & (query_row[:, None] == key_row[None, :])
    return real_pairs | self_pairs


def rotary_tables(position):
    half = HD // 2
    lane = jnp.arange(2 * HD, dtype=jnp.int32)
    freqs = jnp.exp((lane % half).astype(F32) * (-2.0 * math.log(BASE) / HD))
    angles = position.astype(F32)[:, None] * freqs[None, :]
    sign = jnp.where(lane % HD < half, -1.0, 1.0)
    return jnp.cos(angles), jnp.sin(angles) * sign[None, :]


def swap(values, axis, mask, size):
    return lax.ppermute(values, axis, [(i, i ^ mask) for i in range(size)])


def dot(a, b):
    return jnp.dot(a, b, preferred_element_type=F32)


def dot_nt(a, b):
    return lax.dot_general(a, b, (((1,), (1,)), ((), ())), preferred_element_type=F32)


def dot_tn(a, b):
    return lax.dot_general(a, b, (((0,), (0,)), ((), ())), preferred_element_type=F32)


def params(**more):
    return pltpu.CompilerParams(vmem_limit_bytes=VMEM_LIMIT, **more)


def cost(flops, moved):
    return pl.CostEstimate(flops=int(max(flops, SPAN)), bytes_accessed=int(moved), transcendentals=0)


def norm_parts(values):
    center = values - jnp.mean(values, axis=-1, keepdims=True)
    spread = jnp.mean(center * center, axis=-1, keepdims=True)
    inv = lax.rsqrt(spread + EPSILON)
    return center * inv, inv


def norm_back(grad, unit, inv, gain):
    scaled = grad * gain
    first = jnp.mean(scaled, axis=-1, keepdims=True)
    second = jnp.mean(scaled * unit, axis=-1, keepdims=True)
    return inv * (scaled - first - unit * second)


def turn(values, cosine, sine):
    half = HD // 2
    pair = 2 * HD
    lane = lax.broadcasted_iota(jnp.int32, (1, pair), 1)
    low = (lane % HD) < half
    parts = []
    for at in range(0, values.shape[1], pair):
        part = values[:, at : at + pair]
        other = jnp.where(low, pltpu.roll(part, pair - half, 1), pltpu.roll(part, half, 1))
        parts.append(part * cosine + other * sine)
    return parts[0] if len(parts) == 1 else jnp.concatenate(parts, axis=1)


def bits_of(index, masks):
    total = 0
    for bit, mask in enumerate(masks):
        if (index >> bit) & 1:
            total |= mask
    return total


def piece_map(which, masks):
    count = 1 << len(masks)
    half = count // 2
    kind, r, y = which
    if kind == "a":
        return [((i,), r, bits_of(i, masks), 0) for i in range(count)]
    return [
        ((x * half + i,), r | (2 * x), bits_of(i, masks) | y, 1)
        for x in range(2)
        for i in range(half)
    ]


def place(pieces, maps, me_f, h, w_ref, slot_of):
    for ref, entries in zip(pieces, maps):
        for at, r, k, colour in entries:
            w_ref[slot_of(r), me_f ^ k, colour * h : (colour + 1) * h, :] = ref[at]


def times(count, body):
    def step(g, carry):
        body(g)
        return carry

    lax.fori_loop(0, count, step, 0)


def vmem(count):
    return [pl.BlockSpec(memory_space=pltpu.VMEM)] * count


def qkv_kernel(
    maps, h, idx_ref, x_ref, small_ref, cos_ref, sin_ref, p0, p1, p2, p3, p4, p5, p6, p7,
    normed_ref, out_ref, w_ref,
):
    d4, me_f = idx_ref[0], idx_ref[1]
    d = x_ref.shape[1]
    place((p0, p1, p2, p3, p4, p5, p6, p7), maps, me_f, h, w_ref, lambda r: d4 ^ r)
    unit, _ = norm_parts(x_ref[...].astype(F32))
    normed_ref[...] = (unit * small_ref[0:1, :] + small_ref[1:2, :]).astype(BF)

    def product(g):
        return dot(normed_ref[...], w_ref[g].reshape(d, d))

    def turned(g):
        out_ref[g] = turn(product(g), cos_ref[...], sin_ref[...]).astype(BF)

    times(2, turned)
    out_ref[2] = product(2).astype(BF)


def qkv(idx, x, small, cosine, sine, pieces, maps, shards, h):
    n, d = x.shape
    return pl.pallas_call(
        partial(qkv_kernel, maps, h),
        out_shape=(
            jax.ShapeDtypeStruct((n, d), BF),
            jax.ShapeDtypeStruct((3, n, d), BF),
            jax.ShapeDtypeStruct((4, shards, 2 * h, d), BF),
        ),
        in_specs=[pl.BlockSpec(memory_space=pltpu.SMEM)] + vmem(12),
        out_specs=tuple(vmem(3)),
        compiler_params=params(),
        cost_estimate=cost(6 * n * d * d, 2 * (5 * n * d + 8 * d * d)),
        name="qkv",
    )(idx, x, small, cosine, sine, *pieces)


def head_mask(which):
    lane = lax.broadcasted_iota(jnp.int32, (1, 2 * HD), 1)
    return (lane < HD) if which == 0 else (lane >= HD)


def attend_kernel(q_ref, k_ref, v_ref, bias_ref, mixed_ref, probs_ref):
    q, k, v = q_ref[0], k_ref[0], v_ref[0]
    zero = jnp.zeros((), BF)
    parts = []
    for h in range(2):
        own = jnp.where(head_mask(h), q, zero)
        scores = dot_nt(own, k) * (HD**-0.5) + bias_ref[...]
        top = jnp.max(scores, axis=1, keepdims=True)
        raised = jnp.exp(scores - top)
        total = jnp.sum(raised, axis=1, keepdims=True)
        probs = (raised * (1.0 / total)).astype(BF)
        probs_ref[h] = probs
        parts.append(dot(probs, v))
    mixed_ref[...] = jnp.where(head_mask(0), parts[0], parts[1]).astype(BF)


def attend(three, bias):
    _, n, d = three.shape
    pair = 2 * HD
    return pl.pallas_call(
        attend_kernel,
        grid=(d // pair,),
        out_shape=(
            jax.ShapeDtypeStruct((n, d), BF),
            jax.ShapeDtypeStruct((d // HD, n, n), BF),
        ),
        in_specs=[
            pl.BlockSpec((1, n, pair), lambda p: (0, 0, p)),
            pl.BlockSpec((1, n, pair), lambda p: (1, 0, p)),
            pl.BlockSpec((1, n, pair), lambda p: (2, 0, p)),
            pl.BlockSpec((n, n), lambda p: (0, 0)),
        ],
        out_specs=(
            pl.BlockSpec((n, pair), lambda p: (0, p)),
            pl.BlockSpec((2, n, n), lambda p: (p, 0, 0)),
        ),
        compiler_params=params(),
        cost_estimate=cost(8 * n * n * d, 2 * n * n * (d // HD) + 8 * n * d),
        name="attend",
    )(three, three, three, bias)


def attend_back_kernel(
    q_ref, k_ref, v_ref, probs_ref, grad_ref, mixed_ref, cos_ref, sin_ref, out_ref
):
    q, k, v, grad = q_ref[0], k_ref[0], v_ref[0], grad_ref[...]
    zero = jnp.zeros((), BF)
    product = grad.astype(F32) * mixed_ref[...].astype(F32)
    dq, dk, dv = [], [], []
    for h in range(2):
        mask = head_mask(h)
        inner = jnp.sum(jnp.where(mask, product, 0.0), axis=1, keepdims=True)
        probs = probs_ref[h]
        prob_grad = dot_nt(jnp.where(mask, grad, zero), v)
        score_grad = (probs.astype(F32) * (prob_grad - inner)).astype(BF)
        dq.append(dot(score_grad, k))
        dk.append(dot_tn(score_grad, q))
        dv.append(dot_tn(probs, grad))
    first = head_mask(0)
    scale = HD**-0.5
    cosine, sine = cos_ref[...], sin_ref[...]
    out_ref[0] = turn(jnp.where(first, dq[0], dq[1]) * scale, cosine, -sine).astype(BF)
    out_ref[1] = turn(jnp.where(first, dk[0], dk[1]) * scale, cosine, -sine).astype(BF)
    out_ref[2] = jnp.where(first, dv[0], dv[1]).astype(BF)


def attend_back(three, probs, grad, mixed, cosine, sine):
    _, n, d = three.shape
    pair = 2 * HD
    return pl.pallas_call(
        attend_back_kernel,
        grid=(d // pair,),
        out_shape=jax.ShapeDtypeStruct((3, n, d), BF),
        in_specs=[
            pl.BlockSpec((1, n, pair), lambda p: (0, 0, p)),
            pl.BlockSpec((1, n, pair), lambda p: (1, 0, p)),
            pl.BlockSpec((1, n, pair), lambda p: (2, 0, p)),
            pl.BlockSpec((2, n, n), lambda p: (p, 0, 0)),
            pl.BlockSpec((n, pair), lambda p: (0, p)),
            pl.BlockSpec((n, pair), lambda p: (0, p)),
            pl.BlockSpec(cosine.shape, lambda p: (0, 0)),
            pl.BlockSpec(sine.shape, lambda p: (0, 0)),
        ],
        out_specs=pl.BlockSpec((3, n, pair), lambda p: (0, 0, p)),
        compiler_params=params(),
        cost_estimate=cost(16 * n * n * d, 2 * n * n * (d // HD) + 16 * n * d),
        name="attend_back",
    )(three, three, three, probs, grad, mixed, cosine, sine)


def branch_kernel(x_ref, mixed_ref, w_ref, small_ref, residual_ref, hidden_ref):
    residual = x_ref[...].astype(F32) + dot(mixed_ref[...], w_ref[0])
    residual_ref[...] = residual
    unit, _ = norm_parts(residual)
    hidden_ref[...] = (unit * small_ref[2:3, :] + small_ref[3:4, :]).astype(BF)


def branch(x, mixed, weights, small):
    n, d = x.shape
    rows = n // 2
    return pl.pallas_call(
        branch_kernel,
        grid=(2,),
        out_shape=(jax.ShapeDtypeStruct((n, d), F32), jax.ShapeDtypeStruct((n, d), BF)),
        in_specs=[
            pl.BlockSpec((rows, d), lambda g: (g, 0)),
            pl.BlockSpec((rows, d), lambda g: (g, 0)),
            pl.BlockSpec((1, d, d), lambda g: (3, 0, 0)),
            pl.BlockSpec(small.shape, lambda g: (0, 0)),
        ],
        out_specs=(
            pl.BlockSpec((rows, d), lambda g: (g, 0)),
            pl.BlockSpec((rows, d), lambda g: (g, 0)),
        ),
        compiler_params=params(),
        cost_estimate=cost(2 * n * d * d, 10 * n * d + 2 * d * d),
        name="branch",
    )(x, mixed, weights, small)


def spread(out_ref, g, keep, product, me_f, masks, h, shards):
    keep[...] = product.astype(BF)
    for i in range(shards):
        j = me_f ^ bits_of(i, masks)
        for colour in range(2):
            start = pl.multiple_of(j * (2 * h) + colour * h, h & -h)
            out_ref[g, colour, i] = keep[pl.ds(start, h), :]


def up_kernel(
    masks, maps, rs, h, shards, idx_ref, hidden_ref, c_ref, small_ref, p0, p1, p2, p3,
    act_ref, slope_ref, grad_ref, w_ref, keep,
):
    d4, me_f = idx_ref[0], idx_ref[1]
    d = hidden_ref.shape[1]
    place((p0, p1, p2, p3), maps, me_f, h, w_ref, rs.index)

    def half_step(g):
        chunk = d4 ^ jnp.where(g == 0, rs[0], rs[1])
        bias = small_ref[5:6, :]
        for other in range(1, 4):
            bias = jnp.where(chunk == other, small_ref[5 + other : 6 + other, :], bias)
        v = dot(hidden_ref[...], w_ref[g].reshape(d, d)) + bias
        c = math.sqrt(2.0 / math.pi)
        square = v * v
        t = jnp.tanh(v * (c + (c * 0.044715) * square))
        half = 0.5 * (1.0 + t)
        act = (v * half).astype(BF)
        act_ref[g] = act
        slope = half + (0.5 * v) * (1.0 - t * t) * (c + (3.0 * c * 0.044715) * square)
        slope_ref[g] = slope.astype(BF)
        spread(grad_ref, g, keep, dot_tn(act, c_ref[...]), me_f, masks, h, shards)

    times(2, half_step)


def up(idx, hidden, c, small, pieces, maps, rs, masks, shards, h):
    n, d = hidden.shape
    return pl.pallas_call(
        partial(up_kernel, masks, maps, rs, h, shards),
        out_shape=(
            jax.ShapeDtypeStruct((2, n, d), BF),
            jax.ShapeDtypeStruct((2, n, d), BF),
            jax.ShapeDtypeStruct((2, 2, shards, h, d), BF),
            jax.ShapeDtypeStruct((2, shards, 2 * h, d), BF),
        ),
        in_specs=[pl.BlockSpec(memory_space=pltpu.SMEM)] + vmem(7),
        out_specs=tuple(vmem(4)),
        scratch_shapes=[pltpu.VMEM((d, d), BF)],
        compiler_params=params(),
        cost_estimate=cost(8 * n * d * d, 2 * (6 * n * d + 6 * d * d)),
        name="up",
    )(idx, hidden, c, small, *pieces)


def act_grad_kernel(
    masks, maps, rs, h, shards, first, idx_ref, c_ref, x_ref, up_ref, slope_ref, p0, p1, p2, p3,
    *more,
):
    if first:
        hidden_ref, sums_ref, grad_ref, w_ref, keep = more
    else:
        hidden_in, sums_in, hidden_ref, sums_ref, grad_ref, w_ref, keep = more
    d4, me_f = idx_ref[0], idx_ref[1]
    d = x_ref.shape[1]
    place((p0, p1, p2, p3), maps, me_f, h, w_ref, rs.index)
    if first:
        hidden_ref[...] = jnp.zeros_like(hidden_ref)
        sums_ref[...] = jnp.zeros_like(sums_ref)
        sums_ref[4:5, :] = jnp.sum(c_ref[...].astype(F32), axis=0, keepdims=True)
    else:
        hidden_ref[...] = hidden_in[...]
        sums_ref[...] = sums_in[...]

    def half_step(g):
        chunk = d4 ^ jnp.where(g == 0, rs[0], rs[1])
        grad = dot_nt(c_ref[...], w_ref[g].reshape(d, d))
        pre = (grad * slope_ref[g].astype(F32)).astype(BF)
        sums = jnp.sum(pre.astype(F32), axis=0, keepdims=True)
        row = lax.broadcasted_iota(jnp.int32, (sums_ref.shape[0], 1), 0)
        sums_ref[...] += jnp.where(row == 5 + chunk, sums, 0.0)
        hidden_ref[...] += dot_nt(pre, up_ref[g])
        spread(grad_ref, g, keep, dot_tn(x_ref[...], pre), me_f, masks, h, shards)

    times(2, half_step)


def act_grad(idx, c, hidden, up_half, slope, pieces, maps, rs, masks, shards, h, before=None):
    n, d = c.shape
    before = before or ()
    return pl.pallas_call(
        partial(act_grad_kernel, masks, maps, rs, h, shards, not before),
        out_shape=(
            jax.ShapeDtypeStruct((n, d), F32),
            jax.ShapeDtypeStruct((SMALL, d), F32),
            jax.ShapeDtypeStruct((2, 2, shards, h, d), BF),
            jax.ShapeDtypeStruct((2, shards, 2 * h, d), BF),
        ),
        in_specs=[pl.BlockSpec(memory_space=pltpu.SMEM)] + vmem(8 + len(before)),
        out_specs=tuple(vmem(4)),
        scratch_shapes=[pltpu.VMEM((d, d), BF)],
        compiler_params=params(),
        cost_estimate=cost(12 * n * d * d, 2 * (8 * n * d + 8 * d * d)),
        name="act_grad",
    )(idx, c, hidden, up_half.reshape(2, d, d), slope, *pieces, *before)


def first_grad_kernel(
    masks, h, shards, rs, idx_ref, normed_ref, mixed_ref, three_ref, branch_ref, out_ref, keep
):
    g = pl.program_id(0)
    last = (idx_ref[0] ^ jnp.where(g == 0, rs[0], rs[1])) == 3
    x = jnp.where(last, mixed_ref[...], normed_ref[...])
    y = jnp.where(last, branch_ref[...], three_ref[0])
    spread(out_ref, 0, keep, dot_tn(x, y), idx_ref[1], masks, h, shards)


def first_grad(idx, normed, mixed, three_grad, branch_grad, rs, masks, shards, h):
    n, d = normed.shape

    def which(g, idx_ref):
        return jnp.minimum(idx_ref[0] ^ jnp.where(g == 0, rs[0], rs[1]), 2)

    whole = pl.BlockSpec((n, d), lambda g, i: (0, 0))
    return pl.pallas_call(
        partial(first_grad_kernel, masks, h, shards, rs),
        grid_spec=pltpu.PrefetchScalarGridSpec(
            num_scalar_prefetch=1,
            grid=(2,),
            in_specs=[
                whole,
                whole,
                pl.BlockSpec((1, n, d), lambda g, i: (which(g, i), 0, 0)),
                whole,
            ],
            out_specs=pl.BlockSpec((1, 2, shards, h, d), lambda g, i: (g, 0, 0, 0, 0)),
            scratch_shapes=[pltpu.VMEM((d, d), BF)],
        ),
        out_shape=jax.ShapeDtypeStruct((2, 2, shards, h, d), BF),
        compiler_params=params(),
        cost_estimate=cost(4 * n * d * d, 2 * (5 * n * d + 2 * d * d)),
        name="first_grad",
    )(idx, normed, mixed, three_grad, branch_grad)


def middle_kernel(
    c_ref, hidden_ref, residual_ref, small_ref, w_ref, grad_ref, low_ref, mixed_ref, sums_ref
):
    @pl.when(pl.program_id(0) == 0)
    def _():
        sums_ref[...] = jnp.zeros_like(sums_ref)

    grad = hidden_ref[...]
    unit, inv = norm_parts(residual_ref[...])
    sums_ref[2:3, :] += jnp.sum(grad * unit, axis=0, keepdims=True)
    sums_ref[3:4, :] += jnp.sum(grad, axis=0, keepdims=True)
    full = c_ref[...].astype(F32) + norm_back(grad, unit, inv, small_ref[2:3, :])
    grad_ref[...] = full
    low = full.astype(BF)
    low_ref[...] = low
    mixed_ref[...] = dot_nt(low, w_ref[0]).astype(BF)


def middle(c, hidden_grad, residual, small, weights):
    n, d = c.shape
    rows = n // 2
    return pl.pallas_call(
        middle_kernel,
        grid=(2,),
        out_shape=(
            jax.ShapeDtypeStruct((n, d), F32),
            jax.ShapeDtypeStruct((n, d), BF),
            jax.ShapeDtypeStruct((n, d), BF),
            jax.ShapeDtypeStruct((SMALL, d), F32),
        ),
        in_specs=[
            pl.BlockSpec((rows, d), lambda g: (g, 0)),
            pl.BlockSpec((rows, d), lambda g: (g, 0)),
            pl.BlockSpec((rows, d), lambda g: (g, 0)),
            pl.BlockSpec(small.shape, lambda g: (0, 0)),
            pl.BlockSpec((1, d, d), lambda g: (3, 0, 0)),
        ],
        out_specs=(
            pl.BlockSpec((rows, d), lambda g: (g, 0)),
            pl.BlockSpec((rows, d), lambda g: (g, 0)),
            pl.BlockSpec((rows, d), lambda g: (g, 0)),
            pl.BlockSpec((SMALL, d), lambda g: (0, 0)),
        ),
        compiler_params=params(),
        cost_estimate=cost(2 * n * d * d, 18 * n * d + 2 * d * d),
        name="middle",
    )(c, hidden_grad, residual, small, weights)


def input_kernel(x_ref, three_ref, w_ref, small_ref, grad_ref, out_ref, sums_ref, total):
    g = pl.program_id(0)
    part = dot_nt(three_ref[0], w_ref[0])

    @pl.when(g == 0)
    def _():
        total[...] = part

    @pl.when(g > 0)
    def _():
        total[...] += part

    @pl.when(g == 2)
    def _():
        grad = total[...]
        unit, inv = norm_parts(x_ref[...].astype(F32))
        sums_ref[...] = jnp.zeros_like(sums_ref)
        sums_ref[0:1, :] = jnp.sum(grad * unit, axis=0, keepdims=True)
        sums_ref[1:2, :] = jnp.sum(grad, axis=0, keepdims=True)
        out_ref[...] = grad_ref[...] + norm_back(grad, unit, inv, small_ref[0:1, :])


def input_grads(x, three_grad, weights, small, residual_grad):
    n, d = x.shape
    return pl.pallas_call(
        input_kernel,
        grid=(3,),
        out_shape=(jax.ShapeDtypeStruct((n, d), F32), jax.ShapeDtypeStruct((SMALL, d), F32)),
        in_specs=[
            pl.BlockSpec((n, d), lambda g: (0, 0)),
            pl.BlockSpec((1, n, d), lambda g: (g, 0, 0)),
            pl.BlockSpec((1, d, d), lambda g: (g, 0, 0)),
            pl.BlockSpec(small.shape, lambda g: (0, 0)),
            pl.BlockSpec((n, d), lambda g: (0, 0)),
        ],
        out_specs=(
            pl.BlockSpec((n, d), lambda g: (0, 0)),
            pl.BlockSpec((SMALL, d), lambda g: (0, 0)),
        ),
        scratch_shapes=[pltpu.VMEM((n, d), F32)],
        compiler_params=params(),
        cost_estimate=cost(6 * n * d * d, 16 * n * d + 6 * d * d),
        name="input_grads",
    )(x, three_grad, weights, small, residual_grad)


def down_kernel(a0_ref, a1_ref, w0_ref, w1_ref, small_ref, residual_ref, out_ref, total):
    g = pl.program_id(0)
    part = dot(a0_ref[0], w0_ref[0]) + dot(a1_ref[0], w1_ref[0])

    @pl.when(g == 0)
    def _():
        total[...] = residual_ref[...] + small_ref[4:5, :] + part

    @pl.when(g == 1)
    def _():
        out_ref[...] = (total[...] + part).astype(BF)


def down_out(acts, weights, small, residual):
    n, d = residual.shape
    return pl.pallas_call(
        down_kernel,
        grid=(2,),
        out_shape=jax.ShapeDtypeStruct((n, d), BF),
        in_specs=[
            pl.BlockSpec((1, n, d), lambda g: (g, 0, 0)),
            pl.BlockSpec((1, n, d), lambda g: (g, 0, 0)),
            pl.BlockSpec((1, d, d), lambda g: (g, 0, 0)),
            pl.BlockSpec((1, d, d), lambda g: (g, 0, 0)),
            pl.BlockSpec(small.shape, lambda g: (0, 0)),
            pl.BlockSpec((n, d), lambda g: (0, 0)),
        ],
        out_specs=pl.BlockSpec((n, d), lambda g: (0, 0)),
        scratch_shapes=[pltpu.VMEM((n, d), F32)],
        compiler_params=params(),
        cost_estimate=cost(8 * n * d * d, 14 * n * d + 8 * d * d),
        name="down_out",
    )(*acts, *(w.reshape(2, d, d) for w in weights), small, residual)


def last_kernel(shards, idx_ref, p0, p1, p2, p3, up_ref, down_ref, keep):
    _, rows, d = keep.shape
    for r, ref in enumerate((p0, p1, p2, p3)):
        at = idx_ref[0] ^ r
        keep[at] = ref[0].reshape(rows, d).astype(F32)
        down_ref[pl.ds(pl.multiple_of(at * rows, 8), rows), :] = ref[1].reshape(rows, d).astype(F32)
    for i in range(shards):
        part = [keep[chunk, :, i * rows : (i + 1) * rows] for chunk in range(4)]
        up_ref[:, 4 * rows * i : 4 * rows * (i + 1)] = jnp.concatenate(part, axis=1)


def last_out(idx, pieces, shards):
    d = pieces[0].shape[-1]
    rows = d // shards
    vmem = pl.BlockSpec(memory_space=pltpu.VMEM)
    return pl.pallas_call(
        partial(last_kernel, shards),
        out_shape=(
            jax.ShapeDtypeStruct((rows, 4 * d), F32),
            jax.ShapeDtypeStruct((4 * rows, d), F32),
        ),
        in_specs=[pl.BlockSpec(memory_space=pltpu.SMEM)] + [vmem] * 4,
        out_specs=(vmem, vmem),
        scratch_shapes=[pltpu.VMEM((4, rows, d), F32)],
        compiler_params=params(),
        name="last_out",
    )(idx, *pieces)


def local(dp, fsdp, tokens, lengths, *rest):
    (
        norm1_gain,
        norm1_bias,
        query_weight,
        key_weight,
        value_weight,
        output_weight,
        norm2_gain,
        norm2_bias,
        up_weight,
        up_bias,
        down_weight,
        down_bias,
        cotangent,
    ) = rest
    row_count, width = tokens.shape
    slot_count = lengths.shape[1]
    R = width // fsdp
    h = R // 2
    me_dp = lax.axis_index("dp").astype(jnp.int32)
    me_f = lax.axis_index("fsdp").astype(jnp.int32)
    d4 = me_dp % 4
    idx = jnp.stack([d4, me_f])
    masks = []
    mask = fsdp // 2
    while mask >= 1:
        masks.append(mask)
        mask //= 2
    masks = tuple(masks)
    outer = masks[:-1]

    def fswap(v, m):
        return swap(v, "fsdp", m, fsdp)

    def dswap(v, m):
        return swap(v, "dp", m, dp)

    def after(value, *tokens):
        return lax.optimization_barrier((value,) + tokens)[0]

    def after_all(values, *tokens):
        values = tuple(values)
        return list(lax.optimization_barrier(values + tokens)[: len(values)])

    half = fsdp // 2
    maps_own = [
        piece_map(w, masks) for w in (("a", 0, 0), ("a", 2, 0), ("b", 0, 0), ("b", 0, 1))
    ]
    maps_core = [
        piece_map(w, masks) for w in (("a", 1, 0), ("a", 3, 0), ("b", 1, 0), ("b", 1, 1))
    ]

    class Gather:
        def __init__(self, piece):
            self.cur = piece[None]

        def far(self, m):
            self.got = fswap(self.cur, m)

        def join(self):
            self.cur = jnp.concatenate([self.cur, self.got], axis=0)

        def near(self):
            self.got = fswap(self.cur, outer[-1])

        def sides(self):
            a = jnp.concatenate([self.cur[:, :h], self.got[:, :h]], axis=0)
            b = jnp.concatenate([self.cur[:, h:R], self.got[:, h:R]], axis=0)
            self.ab = (a, b)
            self.got_ab = (fswap(a, masks[-1]), dswap(b, 2))

        def cross(self):
            a1 = jnp.concatenate([self.ab[0], self.got_ab[0]], axis=0)
            b1 = jnp.concatenate([self.ab[1], self.got_ab[1]], axis=0)
            self.ab1 = (a1, b1)
            self.got_ab1 = (dswap(a1, 2), fswap(b1, masks[-1]))
            self.core = [dswap(a1, 1), dswap(b1, 1)]

        def finish(self):
            a_x, b_y = self.got_ab1
            a1, b1 = self.ab1
            self.own = [a1, a_x, b1, b_y]
            self.other = [self.core[0], dswap(a_x, 1), self.core[1], dswap(b_y, 1)]

    class Inner:
        def __init__(self, cur):
            self.cur = cur
            self.got = None
            self.left = list(reversed(outer))

        def step(self, *tokens):
            if self.got is not None:
                self.cur = self.cur + after(self.got, *tokens)
                self.got = None
            if self.left:
                count = self.cur.shape[0] // 2
                front = self.cur[count:]
                self.got = fswap(front, self.left.pop(0))
                self.cur = self.cur[:count]
                return front
            return self.cur

        def sums(self):
            while self.got is not None or self.left:
                self.step()
            return self.cur[0]

    class Spread:
        def __init__(self, total):
            m = 4
            while m < dp:
                total = total + dswap(total, m)
                m *= 2
            self.total = total
            self.pair = dswap(total, 2)
            self.core = dswap(total, 1)

        def four(self, *tokens):
            pair = after(self.pair, *tokens)
            return [self.total, self.core, pair, dswap(pair, 1)]

    piece1 = lax.select_n(d4, query_weight, key_weight, value_weight, output_weight)
    g1 = Gather(piece1)
    for m in outer[:-1]:
        g1.far(m)
        g1.join()
    g1_first = g1.cur
    g1.near()
    vectors = after_all(
        (norm1_gain, norm1_bias, norm2_gain, norm2_bias, down_bias, up_bias, up_weight), piece1
    )
    tall = jnp.concatenate(vectors[:6]).reshape(9, R)
    lane = jnp.arange(width, dtype=jnp.int32) // R
    tall = jnp.where((lane == me_f)[None, :], jnp.tile(tall, (1, fsdp)), jnp.zeros((), BF))
    tall = jnp.pad(tall, ((0, SMALL - 9), (0, 0)))
    fronts = []
    for m in reversed(masks):
        if len(fronts) == 1:
            tall = after(tall, g1.got)
        fronts.append(tall)
        tall = tall + fswap(tall, m)
    small = tall.astype(F32)
    piece2 = lax.dynamic_index_in_dim(
        vectors[6].reshape(R, fsdp, 4, R), d4, axis=2, keepdims=False
    ).reshape(R, width)
    g2 = Gather(after(piece2, g1.got, *fronts[2:]))
    for m in outer[:-1]:
        g2.far(m)
        g2.join()
    g1.sides()
    g2.cur, g2.got = after_all((g2.cur, g2.got), *g1.ab)
    g2.near()
    g1.cross()
    early = outer[:-1]
    g3 = Gather(
        lax.dynamic_slice_in_dim(after(down_weight, g2.cur), d4 * R, R, axis=0)
    )
    for m in early[:-1]:
        g3.far(m)
        g3.join()
    g3.far(early[-1])
    g1.finish()
    g2.cur, g2.got = after_all((g2.cur, g2.got), *g1.got_ab1)
    g2.sides()
    g3.join()
    g3.near()

    layout = row_layout(after(lengths, g1_first)[0], row_count, slot_count)
    cosine, sine = rotary_tables(layout[3])
    bias = jnp.where(allowed_pairs(layout, layout, BLOCK, slot_count), 0.0, NEGATIVE)
    normed, three, first4 = qkv(
        idx, after(tokens, *g2.ab, g3.cur, bias), small, cosine, sine, g1.own + g1.other,
        maps_own + maps_core, fsdp, h,
    )
    first4 = first4.reshape(4, width, width)
    g2.got_ab = after_all(g2.got_ab, three)
    g2.cross()
    mixed, probs = attend(after(three, *g2.ab1), bias)
    g2.got_ab1 = after_all(g2.got_ab1, mixed)
    g2.finish()
    g3.cur, g3.got = after_all((g3.cur, g3.got), mixed)
    g3.sides()
    residual, hidden_in = branch(tokens, after(mixed, *g2.got_ab1, *g2.core, *g3.ab), first4, small)
    g3.got_ab = after_all(g3.got_ab, hidden_in)
    g3.cross()
    send_rs, keep_rs = (1, 3), (0, 2)
    act_s, slope_s, send3, up_s = up(
        idx, after(hidden_in, *g3.ab1), cotangent, small, g2.other, maps_core, send_rs, masks,
        fsdp, h,
    )
    act_k, slope_k, keep3, up_k = up(
        idx, after(hidden_in, send3), cotangent, small, g2.own, maps_own, keep_rs, masks, fsdp, h,
    )
    g3.got_ab1 = after_all(g3.got_ab1, keep3)
    g3.finish()

    class Scatter:
        def __init__(self, send):
            self.got = dswap(send, 1)

        def sides(self, keep):
            got = self.got
            a = keep[1, 0] + got[1, 0]
            b = keep[:, 1, half:] + got[:, 1, half:]
            self.keep = (keep[0, 0] + got[0, 0], keep[:, 1, :half] + got[:, 1, :half])
            self.mid = [dswap(a, 2), fswap(b, masks[-1])]
            self.done = (a, b) + self.keep

        def cross(self):
            (a, b), (x, y) = self.keep, self.mid
            self.last = (a[:half] + x[:half], b[0] + y[0])
            out = (a[half:] + x[half:], b[1] + y[1])
            self.got_last = [fswap(out[0], masks[-1]), dswap(out[1], 2)]
            self.done = out + self.last

        def rows(self):
            (a, b), (x, y) = self.last, self.got_last
            return jnp.stack([a + x, b + y], axis=1)

    s3 = Scatter(send3)
    s3.sides(keep3)
    hidden_s, sums_s, send2, down_s = act_grad(
        idx, after(cotangent, *s3.done), hidden_in, up_s, slope_s, g3.other, maps_core, send_rs,
        masks, fsdp, h,
    )
    s2 = Scatter(send2)
    s3.mid = after_all(s3.mid, send2)
    s3.cross()
    hidden_grad, sums_act, keep2, down_k = act_grad(
        idx, after(cotangent, send2, *s3.done), hidden_in, up_k, slope_k, g3.own, maps_own,
        keep_rs, masks, fsdp, h, (hidden_s, sums_s),
    )
    s2.sides(keep2)
    s3.got_last = after_all(s3.got_last, keep2)
    rows3 = Inner(s3.rows())
    front = rows3.step()
    residual_grad, branch_grad, mixed_grad, sums_mid = middle(
        cotangent, after(hidden_grad, *s2.done, front), residual, small, first4
    )
    front = rows3.step(mixed_grad)
    three_grad = attend_back(three, probs, after(mixed_grad, front), mixed, cosine, sine)
    s2.mid = after_all(s2.mid, three_grad)
    s2.cross()
    front = rows3.step(three_grad)
    send1 = first_grad(
        idx, after(normed, *s2.done, front), mixed, three_grad, branch_grad, send_rs, masks, fsdp,
        h,
    )
    s1 = Scatter(send1)
    keep1 = first_grad(
        idx, after(normed, send1), mixed, three_grad, branch_grad, keep_rs, masks, fsdp, h
    )
    s2.got_last = after_all(s2.got_last, keep1)
    rows2 = Inner(s2.rows())
    front = rows2.step()
    s1.sides(keep1)
    input_grad, sums_in = input_grads(
        after(tokens, *s1.done, front), three_grad, first4, small, residual_grad
    )
    front = rows2.step(input_grad)
    small_sum = sums_act + sums_mid + sums_in

    def small_step(swapper, m, *tokens):
        low = after(small_sum.astype(BF), *tokens)
        return low, swapper(low, m)

    low, small_got = small_step(dswap, 1)
    output = down_out(
        (act_s, act_k), (down_s, down_k), small, after(residual, front, low)
    )
    s1.mid = after_all(s1.mid, output)
    s1.cross()
    rest = [(fswap, m) for m in reversed(masks)]
    m = 2
    while m < dp:
        rest.append((dswap, m))
        m *= 2
    small_sum = small_sum + after(small_got, output).astype(F32)
    low, small_got = small_step(*rest.pop(), *s1.done)
    rows1 = Inner(s1.rows())
    rows2.got = after(rows2.got, rows1.cur)
    both = Spread(jnp.stack([rows2.sums(), rows3.sums()]))
    small_sum = small_sum + after(small_got, rows1.cur).astype(F32)
    front = rows1.step()
    low, small_got = small_step(*rest.pop(), front)
    both.pair = after(both.pair, rows1.cur)
    front = rows1.step(low)
    small_sum = small_sum + after(small_got, front).astype(F32)
    low, small_got = small_step(*rest.pop(), front)
    four23 = both.four(front)

    up_grad, down_grad = last_out(idx, four23, fsdp)
    if rows1.got is not None:
        rows1.got = after(rows1.got, up_grad)
    one = Spread(rows1.sums())
    small_sum = small_sum + after(small_got, one.total).astype(F32)
    while rest:
        low, small_got = small_step(*rest.pop(), one.total)
        small_sum = small_sum + small_got.astype(F32)
    four1 = jnp.stack(one.four())
    first_grads = [
        lax.dynamic_index_in_dim(four1, d4 ^ d, axis=0, keepdims=False)
        .reshape(R, width)
        .astype(F32)
        for d in range(4)
    ]
    own = lax.dynamic_slice_in_dim(small_sum, me_f * R, R, axis=1)
    return (
        output,
        input_grad,
        own[0],
        own[1],
        first_grads[0],
        first_grads[1],
        first_grads[2],
        first_grads[3],
        own[2],
        own[3],
        up_grad,
        own[5:9].reshape(4 * R),
        down_grad,
        own[4],
    )


def solution(mesh):
    rows = P(("dp", "fsdp"), None)
    flat = P("fsdp")
    tall = P("fsdp", None)
    in_specs = (
        rows, rows, flat, flat, tall, tall, tall, tall, flat, flat, tall, flat, tall, flat, rows,
    )
    out_specs = (
        rows, rows, flat, flat, tall, tall, tall, tall, flat, flat, tall, flat, tall, flat,
    )
    return jax.shard_map(
        partial(local, mesh.shape["dp"], mesh.shape["fsdp"]),
        mesh=mesh,
        in_specs=in_specs,
        out_specs=out_specs,
        check_vma=False,
    )
```
